128 devices in a mesh: dp: 1, cp: 128 (over z, y, x, core).
Axes of the slice: x: 4, y: 4, z: 4, core: 2. Of those that a mesh axis runs over, the one named last changes fastest.
Arguments:
- x_seq: bfloat16 [1, 32768, 1024], P('dp', 'cp')
- w_in: bfloat16 [1024, 3072], replicated
- w_out: bfloat16 [1024, 1024], replicated
- filt_taps: float32 [32768, 1024], replicated
- skip_gain: float32 [1024], replicated
- d_out: bfloat16 [1, 32768, 1024], P('dp', 'cp')
Outputs:
- output 1: bfloat16 [1, 32768, 1024], P('dp', 'cp')
- output 2: bfloat16 [1024, 3072], P(('dp', 'cp'))
- output 3: bfloat16 [1024, 1024], P(('dp', 'cp'))
- output 4: float32 [32768, 1024], P('dp', 'cp')
- output 5: float32 [1024], P(('dp', 'cp'))
All inputs are finite; a program needn't handle non-finite values.
Results may differ from the reference program's by a relative error of at most 0.0113872.
Values are sent between devices in bfloat16 or wider.
A program may use at most 1 GiB of HBM per device.

```python
import jax
import jax.numpy as jnp
from jax import lax

BATCH_PART = 1
SEQ_LEN = 32768
D_MODEL = 1024
CHAN_BLOCK = min(D_MODEL, 128)
NUM_BLOCKS = D_MODEL // CHAN_BLOCK


def setup_inputs(seed: int = 0, part: int = 0) -> dict:
    shared = jax.random.split(jax.random.key(seed), 5)
    local_keys = jax.random.split(jax.random.fold_in(jax.random.key(seed + 1), part), 2)
    act_shape = (BATCH_PART, SEQ_LEN, D_MODEL)
    x_seq = jax.random.normal(local_keys[0], act_shape, jnp.float32).astype(jnp.bfloat16)
    w_in = (jax.random.normal(shared[0], (D_MODEL, 3 * D_MODEL), jnp.float32) * D_MODEL ** -0.5).astype(jnp.bfloat16)
    w_out = (jax.random.normal(shared[1], (D_MODEL, D_MODEL), jnp.float32) * D_MODEL ** -0.5).astype(jnp.bfloat16)
    decay_rate = jax.random.uniform(shared[2], (D_MODEL,), jnp.float32, minval=0.5, maxval=3.0)
    tap_norm = jnp.sqrt(2.0 * decay_rate / (SEQ_LEN * (1.0 - jnp.exp(-2.0 * decay_rate))))
    lag_frac = jnp.arange(SEQ_LEN, dtype=jnp.float32)[:, None] / SEQ_LEN
    filt_taps = jax.random.normal(shared[3], (SEQ_LEN, D_MODEL), jnp.float32) * jnp.exp(-decay_rate * lag_frac) * tap_norm
    skip_gain = jax.random.uniform(shared[4], (D_MODEL,), jnp.float32, minval=-1.0, maxval=1.0)
    d_out = jax.random.normal(local_keys[1], act_shape, jnp.float32).astype(jnp.bfloat16)
    return {"x_seq": x_seq, "w_in": w_in, "w_out": w_out, "filt_taps": filt_taps, "skip_gain": skip_gain, "d_out": d_out}


def causal_conv(signal, tap_vals):
    fft_len = 2 * SEQ_LEN
    fft_spec = jnp.fft.rfft(signal, n=fft_len, axis=1) * jnp.fft.rfft(tap_vals, n=fft_len, axis=0)
    return jnp.fft.irfft(fft_spec, n=fft_len, axis=1)[:, :SEQ_LEN, :]


def blocked_conv(signal, tap_vals):
    sig_blocks = signal.reshape(BATCH_PART, SEQ_LEN, NUM_BLOCKS, CHAN_BLOCK).transpose(2, 0, 1, 3)
    tap_blocks = tap_vals.reshape(SEQ_LEN, NUM_BLOCKS, CHAN_BLOCK).transpose(1, 0, 2)
    conv_blocks = lax.map(lambda block_pair: causal_conv(block_pair[0], block_pair[1]), (sig_blocks, tap_blocks))
    return conv_blocks.transpose(1, 2, 0, 3).reshape(BATCH_PART, SEQ_LEN, D_MODEL)


def hyena_forward(x_seq, w_in, w_out, filt_taps, skip_gain):
    qkv_act = jnp.dot(x_seq, w_in, preferred_element_type=jnp.float32).astype(jnp.bfloat16)
    q_act = qkv_act[:, :, :D_MODEL]
    k_act = qkv_act[:, :, D_MODEL:2 * D_MODEL]
    v_act = qkv_act[:, :, 2 * D_MODEL:]
    gated_f32 = (k_act * v_act).astype(jnp.float32)
    conv_act = (blocked_conv(gated_f32, filt_taps) + skip_gain * gated_f32).astype(jnp.bfloat16)
    mixed_act = q_act * conv_act
    return jnp.dot(mixed_act, w_out, preferred_element_type=jnp.float32).astype(jnp.bfloat16)


def reference(x_seq, w_in, w_out, filt_taps, skip_gain, d_out):
    _, pullback = jax.vjp(hyena_forward, x_seq, w_in, w_out, filt_taps, skip_gain)
    grad_tuple = pullback(d_out)
    return (grad_tuple[0], grad_tuple[1], grad_tuple[2], grad_tuple[3], grad_tuple[4])
```

```python
import functools

import jax
import jax.numpy as jnp
import numpy as np
from jax import lax
from jax.experimental import pallas as pl
from jax.experimental.pallas import tpu as pltpu
from jax.sharding import PartitionSpec as P

F32, BF16 = jnp.float32, jnp.bfloat16


def split_const(mat):
    hi = mat.astype(np.float32).astype(jnp.bfloat16)
    lo = (mat - hi.astype(np.float64)).astype(np.float32).astype(jnp.bfloat16)
    return hi, lo


@functools.lru_cache(None)
def transform_tables(n_rows, n_lanes):
    n = n_rows * n_lanes
    t1 = np.concatenate([np.arange(0, n_rows, 2), np.arange(1, n_rows, 2)])
    k1 = np.arange(n_rows)
    ang = 2 * np.pi * np.outer(k1 + 0.25, t1) / n_rows
    f1 = np.concatenate([np.cos(ang), -np.sin(ang)], axis=0)
    g1 = f1.T / n
    t2 = np.arange(n_lanes)
    psi = 2 * np.pi * (np.outer(t2, t2) % n_lanes) / n_lanes
    cos2, sin2 = np.cos(psi), np.sin(psi)
    f2 = np.block([[cos2, -sin2], [sin2, cos2]])
    g2 = f2.T
    twist = 2 * np.pi * np.outer(k1 + 0.25, t2) / n
    twid = np.concatenate([np.cos(twist), -np.sin(twist)], axis=1).astype(np.float32)
    f1h, f1l = split_const(f1)
    g1h, g1l = split_const(g1)
    f2h, f2l = split_const(f2)
    g2h, g2l = split_const(g2)
    return (
        np.concatenate([f1h, f1l], axis=1),
        np.concatenate([f2h, f2l], axis=0),
        np.concatenate([g2h, g2l], axis=0),
        np.concatenate([g1h, g1l], axis=1),
        twid,
    )


def dot(a, b):
    return jnp.dot(a, b, preferred_element_type=F32)


def halves(val):
    hi = val.astype(BF16)
    lo = (val - hi.astype(F32)).astype(BF16)
    return hi, lo


def conv_kernel(n_chans, sig_ref, filt_ref, skip_ref, f1_ref, f2_ref, g2_ref, g1_ref, tw_ref,
                out_ref, gfilt_ref, gskip_ref, sig_f32, out_f32):
    n_src = sig_ref.shape[0]
    n_rows, n_lanes = 2 * n_src, sig_ref.shape[2] // 2
    for half in range(2):
        sig_f32[half] = sig_ref[:, :, half * n_lanes:(half + 1) * n_lanes].astype(F32).reshape(sig_f32.shape[1:])

    def rows_of(chan):
        val = jnp.concatenate([sig_f32[0, pl.ds(chan, n_src, stride=2 * n_chans), :],
                               sig_f32[1, pl.ds(chan, n_src, stride=2 * n_chans), :]], axis=0)
        return val

    def taps_of(chan):
        return jnp.concatenate([filt_ref[pl.ds(chan, n_src, stride=2 * n_chans), :],
                                filt_ref[pl.ds(n_chans + chan, n_src, stride=2 * n_chans), :]], axis=0)

    wr, wi = tw_ref[:, :n_lanes], tw_ref[:, n_lanes:]
    f1h, f1l = f1_ref[:, :n_rows], f1_ref[:, n_rows:]
    f2h, f2l = f2_ref[:2 * n_lanes], f2_ref[2 * n_lanes:]
    g2h, g2l = g2_ref[:2 * n_lanes], g2_ref[2 * n_lanes:]
    g1h, g1l = g1_ref[:, :2 * n_rows], g1_ref[:, 2 * n_rows:]

    def second(stage):
        parts = []
        for i in range(2):
            ar = stage[:n_rows, i * n_lanes:(i + 1) * n_lanes]
            ai = stage[n_rows:, i * n_lanes:(i + 1) * n_lanes]
            parts.append(jnp.concatenate([ar * wr - ai * wi, ar * wi + ai * wr], axis=1))
        bh, bl = halves(jnp.concatenate(parts, axis=0))
        spec = dot(bh, f2h) + (dot(bh, f2l) + dot(bl, f2h))
        return spec[:, :n_lanes], spec[:, n_lanes:]

    def inverse(pr, pi):
        ph, pll = halves(jnp.concatenate([pr, pi], axis=1))
        mid = dot(ph, g2h) + (dot(ph, g2l) + dot(pll, g2h))
        tr, ti = [], []
        for i in range(2):
            gr = mid[i * n_rows:(i + 1) * n_rows, :n_lanes]
            gi = mid[i * n_rows:(i + 1) * n_rows, n_lanes:]
            tr.append(gr * wr + gi * wi)
            ti.append(gi * wr - gr * wi)
        th, tl = halves(jnp.concatenate([jnp.concatenate(tr, axis=1), jnp.concatenate(ti, axis=1)], axis=0))
        return dot(g1h, th) + (dot(g1h, tl) + dot(g1l, th))

    def pair(step, carry):
        c0 = 2 * step
        u_val = jnp.concatenate([rows_of(c0), rows_of(c0 + 1)], axis=1)
        dy_val = jnp.concatenate([rows_of(n_chans + c0), rows_of(n_chans + c0 + 1)], axis=1)
        h_val = jnp.concatenate([taps_of(c0), taps_of(c0 + 1)], axis=1)
        u_bf, dy_bf = u_val.astype(BF16), dy_val.astype(BF16)
        h_hi, h_lo = halves(h_val)
        ur, ui = second(dot(f1h, u_bf) + dot(f1l, u_bf))
        dr, di = second(dot(f1h, dy_bf) + dot(f1l, dy_bf))
        hr, hi = second(dot(f1h, h_hi) + (dot(f1h, h_lo) + dot(f1l, h_hi)))
        y_lin = inverse(ur * hr - ui * hi, ur * hi + ui * hr)
        du_lin = inverse(dr * hr + di * hi, di * hr - dr * hi)
        gh_lin = inverse(dr * ur + di * ui, di * ur - dr * ui)
        for i in range(2):
            chan = c0 + i
            cols = slice(i * n_lanes, (i + 1) * n_lanes)
            skip = skip_ref[chan]
            y_out = (y_lin[:, cols] + skip * u_val[:, cols]).astype(BF16).astype(F32)
            du_out = (du_lin[:, cols] + skip * dy_val[:, cols]).astype(BF16).astype(F32)
            gskip_ref[pl.ds(chan, 1), :] = jnp.sum(u_val[:, cols] * dy_val[:, cols], axis=0, keepdims=True)
            for odd in range(2):
                rows = slice(odd * n_src, (odd + 1) * n_src)
                out_f32[odd, pl.ds(chan, n_src, stride=2 * n_chans), :] = y_out[rows]
                out_f32[odd, pl.ds(n_chans + chan, n_src, stride=2 * n_chans), :] = du_out[rows]
                gfilt_ref[pl.ds(odd * n_chans + chan, n_src, stride=2 * n_chans), :] = gh_lin[rows, cols]
        return carry

    lax.fori_loop(0, n_chans // 2, pair, 0)
    for half in range(2):
        out_ref[:, :, half * n_lanes:(half + 1) * n_lanes] = out_f32[half].astype(BF16).reshape(
            n_src, 2 * n_chans, n_lanes)


def channel_convs(sig, taps, skip):
    n_src, n_both, n_tok = sig.shape
    n_chans, n_lanes = n_both // 2, n_tok // 2
    n_rows = 2 * n_src
    tables = transform_tables(n_rows, n_lanes)
    vmem = pl.BlockSpec(memory_space=pltpu.VMEM)
    return pl.pallas_call(
        functools.partial(conv_kernel, n_chans),
        out_shape=(
            jax.ShapeDtypeStruct(sig.shape, BF16),
            jax.ShapeDtypeStruct((n_rows * n_chans, n_lanes), F32),
            jax.ShapeDtypeStruct((n_chans, n_lanes), F32),
        ),
        in_specs=[vmem, vmem, pl.BlockSpec(memory_space=pltpu.SMEM)] + [vmem] * 5,
        out_specs=(vmem, vmem, vmem),
        scratch_shapes=[
            pltpu.VMEM((2, n_src * n_both, n_lanes), F32),
            pltpu.VMEM((2, n_src * n_both, n_lanes), F32),
        ],
        compiler_params=pltpu.CompilerParams(vmem_limit_bytes=48 * 2 ** 20),
        cost_estimate=pl.CostEstimate(flops=10 ** 10, bytes_accessed=8 * 2 ** 20, transcendentals=0),
        name="channel_convs",
    )(sig, taps, skip, *[jnp.asarray(tab) for tab in tables])


def solution(mesh):
    ctx_size = mesh.shape["cp"]

    def local_step(x_seq, w_in, w_out, filt_taps, skip_gain, d_out):
        n_batch, n_tok, width = x_seq.shape
        n_chans = width // ctx_size
        seq_len = n_tok * ctx_size
        n_lanes = n_tok // 2
        rank = lax.axis_index("cp")
        x_tok, do_tok = x_seq[0], d_out[0]

        def mm(a, b, ca, cb):
            return lax.dot_general(a, b, (((ca,), (cb,)), ((), ())), preferred_element_type=F32)

        qkv = mm(w_in, x_tok, 0, 1).astype(BF16)
        q_act, k_act, v_act = qkv[:width], qkv[width:2 * width], qkv[2 * width:]
        u_act = k_act * v_act
        dz_act = mm(w_out, do_tok, 1, 1).astype(BF16)
        dy_act = dz_act * q_act
        sig = jnp.concatenate([u_act.reshape(ctx_size, n_chans, n_tok), dy_act.reshape(ctx_size, n_chans, n_tok)], axis=1)
        sig = lax.all_to_all(sig, "cp", 0, 0, tiled=True)

        taps = lax.dynamic_slice_in_dim(filt_taps, rank * n_chans, n_chans, axis=1)
        taps = taps.reshape(seq_len // n_lanes, n_lanes, n_chans).transpose(0, 2, 1).reshape(-1, n_lanes)
        skip = lax.dynamic_slice_in_dim(skip_gain, rank * n_chans, n_chans, axis=0)
        res, gfilt, gskip = channel_convs(sig, taps, skip)
        grad_filt = gfilt.reshape(seq_len // n_lanes, n_chans, n_lanes).transpose(0, 2, 1).reshape(seq_len, n_chans)
        grad_skip = jnp.sum(gskip, axis=1)

        res = lax.all_to_all(res, "cp", 0, 0, tiled=True)
        y_act = res[:, :n_chans].reshape(width, n_tok)
        du_act = res[:, n_chans:].reshape(width, n_tok)
        z_act = q_act * y_act
        d_qkv = jnp.concatenate([dz_act * y_act, du_act * v_act, du_act * k_act], axis=0)
        grad_x = mm(d_qkv, w_in, 0, 1).astype(BF16)[None]
        dw_in = mm(x_tok, d_qkv, 0, 1)
        dw_out = mm(z_act, do_tok, 1, 0)
        parts = jnp.concatenate([dw_in, dw_out], axis=1).reshape(ctx_size, n_chans, 4 * width)
        parts = lax.all_to_all(parts, "cp", 0, 0, tiled=True)
        sums = jnp.sum(parts, axis=0).astype(BF16)
        return grad_x, sums[:, :3 * width], sums[:, 3 * width:], grad_filt, grad_skip

    seq_spec = P("dp", "cp", None)
    row_spec = P(("dp", "cp"), None)
    return jax.shard_map(
        local_step,
        mesh=mesh,
        in_specs=(seq_spec, P(), P(), P(), P(), seq_spec),
        out_specs=(seq_spec, row_spec, row_spec, P("dp", "cp"), P(("dp", "cp"))),
        check_vma=False,
    )
```

```python
import functools

import jax
import jax.numpy as jnp
import numpy as np
from jax import lax
from jax.experimental import pallas as pl
from jax.experimental.pallas import tpu as pltpu
from jax.sharding import PartitionSpec as P

F32, BF16 = jnp.float32, jnp.bfloat16


def split_const(mat):
    hi = mat.astype(np.float32).astype(jnp.bfloat16)
    lo = (mat - hi.astype(np.float64)).astype(np.float32).astype(jnp.bfloat16)
    return hi, lo


@functools.lru_cache(None)
def transform_tables(n_rows, n_lanes):
    n = n_rows * n_lanes
    t1 = np.concatenate([np.arange(0, n_rows, 2), np.arange(1, n_rows, 2)])
    k1 = np.arange(n_rows)
    ang = 2 * np.pi * np.outer(k1 + 0.25, t1) / n_rows
    f1 = np.concatenate([np.cos(ang), -np.sin(ang)], axis=0)
    g1 = f1.T / n
    t2 = np.arange(n_lanes)
    psi = 2 * np.pi * (np.outer(t2, t2) % n_lanes) / n_lanes
    cos2, sin2 = np.cos(psi), np.sin(psi)
    f2 = np.block([[cos2, -sin2], [sin2, cos2]])
    g2 = f2.T
    twist = 2 * np.pi * np.outer(k1 + 0.25, t2) / n
    twid = np.concatenate([np.cos(twist), -np.sin(twist)], axis=1).astype(np.float32)
    f1h, f1l = split_const(f1)
    g1h, g1l = split_const(g1)
    f2h, f2l = split_const(f2)
    g2h, g2l = split_const(g2)
    return (
        np.concatenate([f1h, f1l], axis=1),
        np.concatenate([f2h, f2l], axis=0),
        np.concatenate([g2h, g2l], axis=0),
        np.concatenate([g1h, g1l], axis=1),
        twid,
    )


def dot(a, b):
    return jnp.dot(a, b, preferred_element_type=F32)


def halves(val):
    hi = val.astype(BF16)
    lo = (val - hi.astype(F32)).astype(BF16)
    return hi, lo


def conv_kernel(n_chans, sig_ref, filt_ref, skip_ref, f1_ref, f2_ref, g2_ref, g1_ref, tw_ref,
                out_ref, gfilt_ref, gskip_ref, sig_f32, out_f32):
    n_src = sig_ref.shape[0]
    n_rows, n_lanes = 2 * n_src, sig_ref.shape[2] // 2
    for half in range(2):
        sig_f32[half] = sig_ref[:, :, half * n_lanes:(half + 1) * n_lanes].astype(F32).reshape(sig_f32.shape[1:])

    def rows_of(chan):
        val = jnp.concatenate([sig_f32[0, pl.ds(chan, n_src, stride=2 * n_chans), :],
                               sig_f32[1, pl.ds(chan, n_src, stride=2 * n_chans), :]], axis=0)
        return val

    def taps_of(chan):
        return jnp.concatenate([filt_ref[pl.ds(chan, n_src, stride=2 * n_chans), :],
                                filt_ref[pl.ds(n_chans + chan, n_src, stride=2 * n_chans), :]], axis=0)

    wr, wi = tw_ref[:, :n_lanes], tw_ref[:, n_lanes:]
    f1h, f1l = f1_ref[:, :n_rows], f1_ref[:, n_rows:]
    f2h, f2l = f2_ref[:2 * n_lanes], f2_ref[2 * n_lanes:]
    g2h, g2l = g2_ref[:2 * n_lanes], g2_ref[2 * n_lanes:]
    g1h, g1l = g1_ref[:, :2 * n_rows], g1_ref[:, 2 * n_rows:]

    def second(stage):
        parts = []
        for i in range(2):
            ar = stage[:n_rows, i * n_lanes:(i + 1) * n_lanes]
            ai = stage[n_rows:, i * n_lanes:(i + 1) * n_lanes]
            parts.append(jnp.concatenate([ar * wr - ai * wi, ar * wi + ai * wr], axis=1))
        bh, bl = halves(jnp.concatenate(parts, axis=0))
        spec = dot(bh, f2h) + (dot(bh, f2l) + dot(bl, f2h))
        return spec[:, :n_lanes], spec[:, n_lanes:]

    def inverse(pr, pi):
        ph, pll = halves(jnp.concatenate([pr, pi], axis=1))
        mid = dot(ph, g2h) + (dot(ph, g2l) + dot(pll, g2h))
        tr, ti = [], []
        for i in range(2):
            gr = mid[i * n_rows:(i + 1) * n_rows, :n_lanes]
            gi = mid[i * n_rows:(i + 1) * n_rows, n_lanes:]
            tr.append(gr * wr + gi * wi)
            ti.append(gi * wr - gr * wi)
        th, tl = halves(jnp.concatenate([jnp.concatenate(tr, axis=1), jnp.concatenate(ti, axis=1)], axis=0))
        return dot(g1h, th) + (dot(g1h, tl) + dot(g1l, th))

    def pair(step, carry):
        c0 = 2 * step
        u_val = jnp.concatenate([rows_of(c0), rows_of(c0 + 1)], axis=1)
        dy_val = jnp.concatenate([rows_of(n_chans + c0), rows_of(n_chans + c0 + 1)], axis=1)
        h_val = jnp.concatenate([taps_of(c0), taps_of(c0 + 1)], axis=1)
        u_bf, dy_bf = u_val.astype(BF16), dy_val.astype(BF16)
        h_hi, h_lo = halves(h_val)
        ur, ui = second(dot(f1h, u_bf) + dot(f1l, u_bf))
        dr, di = second(dot(f1h, dy_bf) + dot(f1l, dy_bf))
        hr, hi = second(dot(f1h, h_hi) + (dot(f1h, h_lo) + dot(f1l, h_hi)))
        y_lin = inverse(ur * hr - ui * hi, ur * hi + ui * hr)
        du_lin = inverse(dr * hr + di * hi, di * hr - dr * hi)
        gh_lin = inverse(dr * ur + di * ui, di * ur - dr * ui)
        for i in range(2):
            chan = c0 + i
            cols = slice(i * n_lanes, (i + 1) * n_lanes)
            skip = skip_ref[chan]
            y_out = (y_lin[:, cols] + skip * u_val[:, cols]).astype(BF16).astype(F32)
            du_out = (du_lin[:, cols] + skip * dy_val[:, cols]).astype(BF16).astype(F32)
            gskip_ref[pl.ds(chan, 1), :] = jnp.sum(u_val[:, cols] * dy_val[:, cols], axis=0, keepdims=True)
            for odd in range(2):
                rows = slice(odd * n_src, (odd + 1) * n_src)
                out_f32[odd, pl.ds(chan, n_src, stride=2 * n_chans), :] = y_out[rows]
                out_f32[odd, pl.ds(n_chans + chan, n_src, stride=2 * n_chans), :] = du_out[rows]
                gfilt_ref[pl.ds(odd * n_chans + chan, n_src, stride=2 * n_chans), :] = gh_lin[rows, cols]
        return carry

    lax.fori_loop(0, n_chans // 2, pair, 0)
    for half in range(2):
        out_ref[:, :, half * n_lanes:(half + 1) * n_lanes] = out_f32[half].astype(BF16).reshape(
            n_src, 2 * n_chans, n_lanes)


def channel_convs(sig, taps, skip):
    n_src, n_both, n_tok = sig.shape
    n_chans, n_lanes = n_both // 2, n_tok // 2
    n_rows = 2 * n_src
    tables = transform_tables(n_rows, n_lanes)
    vmem = pl.BlockSpec(memory_space=pltpu.VMEM)
    return pl.pallas_call(
        functools.partial(conv_kernel, n_chans),
        out_shape=(
            jax.ShapeDtypeStruct(sig.shape, BF16),
            jax.ShapeDtypeStruct((n_rows * n_chans, n_lanes), F32),
            jax.ShapeDtypeStruct((n_chans, n_lanes), F32),
        ),
        in_specs=[vmem, vmem, pl.BlockSpec(memory_space=pltpu.SMEM)] + [vmem] * 5,
        out_specs=(vmem, vmem, vmem),
        scratch_shapes=[
            pltpu.VMEM((2, n_src * n_both, n_lanes), F32),
            pltpu.VMEM((2, n_src * n_both, n_lanes), F32),
        ],
        compiler_params=pltpu.CompilerParams(vmem_limit_bytes=48 * 2 ** 20),
        cost_estimate=pl.CostEstimate(flops=10 ** 10, bytes_accessed=8 * 2 ** 20, transcendentals=0),
        name="channel_convs",
    )(sig, taps, skip, *[jnp.asarray(tab) for tab in tables])


RING = 4
PART_ORDERS = ((0, 1, 2), (1, 2, 0), (2, 0, 1))


def part_columns(total):
    tiles = total // 128
    ends = [0, (tiles + 2) // 3 * 128, ((tiles + 2) // 3 + (tiles + 1) // 3) * 128, total]
    return [(ends[i], ends[i + 1]) for i in range(3)]


def grad_kernel(n_in, x_ref, z_ref, d_ref, do_ref, win_ref, wout_ref, *scratch):
    (x_peer, z_peer, d_peer, do_peer, p0, p1, p2, via0, via1, via2, fin0, fin1, fin2, r10, r11, r12,
     via20, via21, via22, fin20, fin21, fin22, r20, r21, r22, via30, via31, via32, fin30, fin31, fin32,
     send_sem, recv_sem, swap_send, swap_recv) = scratch
    partial = (p0, p1, p2)
    vias = ((via0, via1, via2), (via20, via21, via22), (via30, via31, via32))
    fins = ((fin0, fin1, fin2), (fin20, fin21, fin22), (fin30, fin31, fin32))
    reds = ((r10, r11, r12), (r20, r21, r22))
    rank = lax.axis_index("cp")
    core = lax.rem(rank, 2)
    chip = lax.div(rank, 2)
    coords = (lax.div(chip, 16), lax.rem(lax.div(chip, 4), 4), lax.rem(chip, 4))
    strides = (32, 8, 2)
    peer = rank + 1 - 2 * core
    n_out = do_ref.shape[1]
    cols = part_columns(n_in + n_out)

    def at_offset(dim, step):
        pos = lax.rem(coords[dim] + step, RING)
        return pos, rank + (pos - coords[dim]) * strides[dim]

    nxt = [at_offset(dim, 1) for dim in range(3)]
    opp = [at_offset(dim, 2) for dim in range(3)]
    prv = [at_offset(dim, 3) for dim in range(3)]

    barrier = pltpu.get_barrier_semaphore()
    for device in [peer] + [spot[1] for spot in nxt] + [spot[1] for spot in prv]:
        pl.semaphore_signal(barrier, inc=1, device_id={"cp": device}, device_id_type=pl.DeviceIdType.MESH)
    pl.semaphore_wait(barrier, 7)

    def remote(src, dst, send, recv, device):
        return pltpu.make_async_remote_copy(src_ref=src, dst_ref=dst, send_sem=send, recv_sem=recv,
                                            device_id={"cp": device}, device_id_type=pl.DeviceIdType.MESH)

    swaps = []

    def swap(src, dst):
        copy = remote(src, dst, swap_send.at[len(swaps)], swap_recv.at[len(swaps)], peer)
        copy.start()
        swaps.append(copy)

    swap(x_ref.at[:, 1 - core], x_peer)
    row_ranges = [(lo, min(hi, n_in)) for lo, hi in cols]
    for lo, hi in row_ranges:
        swap(d_ref.at[pl.ds(lo, hi - lo)], d_peer.at[pl.ds(lo, hi - lo)])
    swap(z_ref.at[:, 1 - core], z_peer)
    swap(do_ref, do_peer)

    n_tok = x_ref.shape[-1]
    n_rows = x_ref.shape[0] * x_ref.shape[2]

    def flat(val):
        return val.reshape(n_rows, n_tok)

    def mm(a, b, cb):
        return lax.dot_general(a, b, (((1,), (cb,)), ((), ())), preferred_element_type=F32)

    def put(part, col, val):
        partial[part][:, :, :, :, pl.ds(col, val.shape[1])] = val.reshape(
            RING, RING, RING, x_ref.shape[2], val.shape[1])

    def slab(ref, axis, pos, col=None):
        index = [slice(None)] * len(ref.shape)
        if axis is not None:
            index[axis] = pos
        if col is not None:
            index[-1] = pl.ds(*col)
        return ref.at[tuple(index)]

    copies = {}

    def send(part, phase, which, src, dst, device):
        slot = (phase * 3 + part) * 6 + which
        copy = remote(src, dst, send_sem.at[slot], recv_sem.at[slot], device)
        copy.start()
        copies[part, phase, which] = copy

    def source(part, phase):
        return partial[part] if phase == 0 else reds[phase - 1][part]

    def axis_of(part, phase):
        order = PART_ORDERS[part]
        left = sorted(order[phase:])
        return left.index(order[phase])

    def split(part):
        lo, hi = cols[part]
        first = ((hi - lo) // 128 + 1) // 2 * 128
        return (0, first), (first, hi - lo - first)

    def launch(part, phase):
        dim, axis, src = PART_ORDERS[part][phase], axis_of(part, phase), source(part, phase)
        a_cols, b_cols = split(part)
        via, fin = vias[phase][part], fins[phase][part]
        send(part, phase, 0, slab(src, axis, opp[dim][0], a_cols), slab(via, None, None, a_cols), nxt[dim][1])
        send(part, phase, 1, slab(src, axis, opp[dim][0], b_cols), slab(via, None, None, b_cols), prv[dim][1])
        send(part, phase, 2, slab(src, axis, nxt[dim][0], b_cols), slab(fin, 0, 0, b_cols), nxt[dim][1])
        send(part, phase, 3, slab(src, axis, prv[dim][0], a_cols), slab(fin, 0, 1, a_cols), prv[dim][1])

    def each_block(shape, body):
        lead = shape[:-2]
        count = int(np.prod(lead)) if lead else 1
        if count == 1:
            body(tuple(0 for _ in lead))
            return

        def step(i, carry):
            index = []
            for size in reversed(lead):
                index.insert(0, lax.rem(i, size))
                i = lax.div(i, size)
            body(tuple(index))
            return carry

        lax.fori_loop(0, count, step, 0, unroll=min(count, 4))

    def relay(part, phase):
        dim, axis, src = PART_ORDERS[part][phase], axis_of(part, phase), source(part, phase)
        a_cols, b_cols = split(part)
        via, fin = vias[phase][part], fins[phase][part]
        for which, col, spot, side in ((0, a_cols, nxt[dim], 0), (1, b_cols, prv[dim], 1)):
            copies[part, phase, which].wait_recv()
            span = pl.ds(*col)

            def add(index):
                at = index[:axis] + (spot[0],) + index[axis:]
                src[at + (slice(None), span)] = src[at + (slice(None), span)] + via[index + (slice(None), span)]

            each_block(via.shape, add)
            send(part, phase, 4 + which, slab(src, axis, spot[0], col), slab(fin, 0, side, col), spot[1])

    def finish(part, phase):
        dim, axis, src = PART_ORDERS[part][phase], axis_of(part, phase), source(part, phase)
        via, fin = vias[phase][part], fins[phase][part]
        for which in range(2, 6):
            copies[part, phase, which].wait_recv()

        def add(index):
            at = index[:axis] + (coords[dim],) + index[axis:]
            total = src[at] + fin[(0,) + index] + fin[(1,) + index]
            if phase < 2:
                reds[phase][part][index] = total
            else:
                lo, hi = cols[part]
                mid = min(max(n_in, lo), hi)
                if mid > lo:
                    win_ref[:, lo:mid] = total[:, :mid - lo].astype(win_ref.dtype)
                if hi > mid:
                    wout_ref[:, mid - n_in:hi - n_in] = total[:, mid - lo:].astype(wout_ref.dtype)

        each_block(via.shape, add)

    x_own = flat(x_ref[:, core])
    swaps[0].wait_recv()
    x_other = flat(x_peer[...])
    for part in range(3):
        lo, hi = cols[part]
        swaps[1 + part].wait_recv()
        for start in range(lo, min(hi, n_in), 512):
            size = min(512, min(hi, n_in) - start)
            put(part, start - lo, mm(x_own, d_ref[pl.ds(start, size), :], 1)
                + mm(x_other, d_peer[pl.ds(start, size), :], 1))
        if hi > n_in:
            swaps[4].wait_recv()
            swaps[5].wait_recv()
            z_own, z_other = flat(z_ref[:, core]), flat(z_peer[...])
            for start in range(max(lo, n_in), hi, 512):
                size = min(512, hi - start)
                put(part, start - lo, mm(z_own, do_ref[:, pl.ds(start - n_in, size)], 0)
                    + mm(z_other, do_peer[:, pl.ds(start - n_in, size)], 0))
        launch(part, 0)
    for phase in range(3):
        for part in range(3):
            relay(part, phase)
        for part in range(3):
            finish(part, phase)
            if phase < 2:
                launch(part, phase + 1)
    for copy in copies.values():
        copy.wait_send()
    for copy in swaps:
        copy.wait_send()


def weight_grads(x_cm, z_cm, d_cm, d_out):
    n_chip, n_core, n_row, n_tok = x_cm.shape
    n_in, n_out = d_cm.shape[0], d_out.shape[1]
    widths = [hi - lo for lo, hi in part_columns(n_in + n_out)]
    vmem = pl.BlockSpec(memory_space=pltpu.VMEM)
    scratch = [pltpu.VMEM((n_chip, n_row, n_tok), BF16), pltpu.VMEM((n_chip, n_row, n_tok), BF16),
               pltpu.VMEM(d_cm.shape, BF16), pltpu.VMEM(d_out.shape, BF16)]
    scratch += [pltpu.VMEM((RING,) * 3 + (n_row, w), F32) for w in widths]
    for n_lead in (2, 1, 0):
        lead = (RING,) * n_lead
        scratch += [pltpu.VMEM(lead + (n_row, w), F32) for w in widths]
        scratch += [pltpu.VMEM((2,) + lead + (n_row, w), F32) for w in widths]
        if n_lead:
            scratch += [pltpu.VMEM(lead + (n_row, w), F32) for w in widths]
    scratch += [pltpu.SemaphoreType.DMA((54,)), pltpu.SemaphoreType.DMA((54,)),
                pltpu.SemaphoreType.DMA((6,)), pltpu.SemaphoreType.DMA((6,))]
    return pl.pallas_call(
        functools.partial(grad_kernel, n_in),
        out_shape=(jax.ShapeDtypeStruct((n_row, n_in), BF16), jax.ShapeDtypeStruct((n_row, n_out), BF16)),
        in_specs=[vmem] * 4,
        out_specs=(vmem, vmem),
        scratch_shapes=scratch,
        compiler_params=pltpu.CompilerParams(vmem_limit_bytes=56 * 2 ** 20, collective_id=0, has_side_effects=True),
        cost_estimate=pl.CostEstimate(flops=5 * 10 ** 9, bytes_accessed=8 * 2 ** 20, transcendentals=0),
        name="weight_grads",
    )(x_cm, z_cm, d_cm, d_out)


def solution(mesh):
    ctx_size = mesh.shape["cp"]

    def local_step(x_seq, w_in, w_out, filt_taps, skip_gain, d_out):
        n_batch, n_tok, width = x_seq.shape
        n_chans = width // ctx_size
        seq_len = n_tok * ctx_size
        n_lanes = n_tok // 2
        rank = lax.axis_index("cp")
        x_tok, do_tok = x_seq[0], d_out[0]

        def mm(a, b, ca, cb):
            return lax.dot_general(a, b, (((ca,), (cb,)), ((), ())), preferred_element_type=F32)

        qkv = mm(w_in, x_tok, 0, 1).astype(BF16)
        q_act, k_act, v_act = qkv[:width], qkv[width:2 * width], qkv[2 * width:]
        u_act = k_act * v_act
        dz_act = mm(w_out, do_tok, 1, 1).astype(BF16)
        dy_act = dz_act * q_act
        sig = jnp.concatenate([u_act.reshape(ctx_size, n_chans, n_tok), dy_act.reshape(ctx_size, n_chans, n_tok)], axis=1)
        sig = lax.all_to_all(sig, "cp", 0, 0, tiled=True)

        taps = lax.dynamic_slice_in_dim(filt_taps, rank * n_chans, n_chans, axis=1)
        taps = taps.reshape(seq_len // n_lanes, n_lanes, n_chans).transpose(0, 2, 1).reshape(-1, n_lanes)
        skip = lax.dynamic_slice_in_dim(skip_gain, rank * n_chans, n_chans, axis=0)
        res, gfilt, gskip = channel_convs(sig, taps, skip)
        grad_filt = gfilt.reshape(seq_len // n_lanes, n_chans, n_lanes).transpose(0, 2, 1).reshape(seq_len, n_chans)
        grad_skip = jnp.sum(gskip, axis=1)

        res = lax.all_to_all(res, "cp", 0, 0, tiled=True)
        y_act = res[:, :n_chans].reshape(width, n_tok)
        du_act = res[:, n_chans:].reshape(width, n_tok)
        z_act = q_act * y_act
        d_qkv = jnp.concatenate([dz_act * y_act, du_act * v_act, du_act * k_act], axis=0)
        grad_x = mm(d_qkv, w_in, 0, 1).astype(BF16)[None]
        by_core = (ctx_size // 2, 2, n_chans, n_tok)
        grad_w_in, grad_w_out = weight_grads(
            x_tok.T.reshape(by_core), z_act.reshape(by_core), d_qkv, do_tok)
        return grad_x, grad_w_in, grad_w_out, grad_filt, grad_skip

    seq_spec = P("dp", "cp", None)
    row_spec = P(("dp", "cp"), None)
    return jax.shard_map(
        local_step,
        mesh=mesh,
        in_specs=(seq_spec, P(), P(), P(), P(), seq_spec),
        out_specs=(seq_spec, row_spec, row_spec, P("dp", "cp"), P(("dp", "cp"))),
        check_vma=False,
    )
```

```python
import functools

import jax
import jax.numpy as jnp
import numpy as np
from jax import lax
from jax.experimental import pallas as pl
from jax.experimental.pallas import tpu as pltpu
from jax.sharding import PartitionSpec as P

F32, BF16 = jnp.float32, jnp.bfloat16


def split_const(mat):
    hi = mat.astype(np.float32).astype(jnp.bfloat16)
    lo = (mat - hi.astype(np.float64)).astype(np.float32).astype(jnp.bfloat16)
    return hi, lo


@functools.lru_cache(None)
def transform_tables(n_rows, n_lanes):
    n = n_rows * n_lanes
    t1 = np.concatenate([np.arange(0, n_rows, 2), np.arange(1, n_rows, 2)])
    k1 = np.arange(n_rows)
    ang = 2 * np.pi * np.outer(k1 + 0.25, t1) / n_rows
    f1 = np.concatenate([np.cos(ang), -np.sin(ang)], axis=0)
    g1 = f1.T / n
    t2 = np.arange(n_lanes)
    psi = 2 * np.pi * (np.outer(t2, t2) % n_lanes) / n_lanes
    cos2, sin2 = np.cos(psi), np.sin(psi)
    f2 = np.block([[cos2, -sin2], [sin2, cos2]])
    g2 = f2.T
    twist = 2 * np.pi * np.outer(k1 + 0.25, t2) / n
    twid = np.concatenate([np.cos(twist), -np.sin(twist)], axis=1).astype(np.float32)
    f1h, f1l = split_const(f1)
    g1h, g1l = split_const(g1)
    f2h, f2l = split_const(f2)
    g2h, g2l = split_const(g2)
    return (
        np.concatenate([f1h, f1l], axis=1),
        np.concatenate([f2h, f2l], axis=0),
        np.concatenate([g2h, g2l], axis=0),
        np.concatenate([g1h, g1l], axis=1),
        twid,
    )


def dot(a, b):
    return jnp.dot(a, b, preferred_element_type=F32)


def halves(val):
    hi = val.astype(BF16)
    lo = (val - hi.astype(F32)).astype(BF16)
    return hi, lo


def mix_kernel(u_ref, dy_ref, filt_ref, skip_ref, f1_hbm, f2_hbm, g2_hbm, g1_hbm, tw_hbm,
               y_ref, du_ref, gfilt_ref, gskip_ref,
               u_in, dy_in, y_out, du_out, u_f32, dy_f32, out_f32, wide, flip, taps, u_spec, h_spec, d_spec,
               f1_ref, f2_ref, g2_ref, g1_ref, tw_ref, load_sem, wide_sem, send_sem, recv_sem):
    n_dev, n_chans, n_tok = u_ref.shape
    n_lanes = n_tok // 2
    n_rows = 2 * n_dev
    n_pairs = n_chans // 2
    rank = lax.axis_index("cp")

    loads = [pltpu.make_async_copy(src, dst, load_sem.at[i]) for i, (src, dst) in enumerate(
        ((f1_hbm, f1_ref), (f2_hbm, f2_ref), (g2_hbm, g2_ref), (g1_hbm, g1_ref), (tw_hbm, tw_ref)))]
    n_wide = wide.shape[0]
    first_lane = pl.multiple_of(lax.div(rank * n_chans, 128) * 128, 128)
    wides = [pltpu.make_async_copy(
        filt_ref.at[pl.ds(i * wide.shape[1], wide.shape[1]), pl.ds(first_lane, 128)], wide.at[i], wide_sem.at[i])
        for i in range(n_wide)]

    def others(body):
        def step(i, carry):
            body(lax.rem(rank + i, n_dev))
            return carry

        lax.fori_loop(1, n_dev, step, 0)

    barrier = pltpu.get_barrier_semaphore()
    others(lambda dev: pl.semaphore_signal(barrier, inc=1, device_id={"cp": dev}, device_id_type=pl.DeviceIdType.MESH))
    for copy in wides + loads:
        copy.start()
    pl.semaphore_wait(barrier, n_dev - 1)

    def exchange(which, src, dst):
        def send(dev):
            pltpu.make_async_remote_copy(
                src_ref=src.at[dev], dst_ref=dst.at[rank], send_sem=send_sem.at[which], recv_sem=recv_sem.at[which],
                device_id={"cp": dev}, device_id_type=pl.DeviceIdType.MESH).start()

        others(send)
        dst[rank] = src[rank]

    def wait_all(sem, which, ref):
        part = ref.at[pl.ds(0, n_dev - 1)]
        pltpu.make_async_copy(part, part, sem.at[which]).wait()

    exchange(0, u_ref, u_in)
    exchange(1, dy_ref, dy_in)

    own_row = pl.multiple_of(lax.rem(rank * n_chans, 128), n_chans)
    per_wide = wide.shape[1] // n_lanes

    for i in range(n_wide):
        wides[i].wait()

        def turn(j, carry):
            for k in range(4):
                tile = 4 * j + k
                flip[k] = wide[i, pl.ds(pl.multiple_of(tile * n_lanes, n_lanes), n_lanes), :].T
                at = pl.multiple_of((i * per_wide + tile) * n_chans, n_chans)
                taps[pl.ds(at, n_chans), :] = flip[k, pl.ds(own_row, n_chans), :]
            return carry

        lax.fori_loop(0, per_wide // 4, turn, 0)
    for copy in loads:
        copy.wait()

    def f1(i):
        return f1_ref[:, i * n_rows:(i + 1) * n_rows]

    def g1(i):
        return g1_ref[:, 2 * i * n_rows:2 * (i + 1) * n_rows]

    def f2(i):
        return f2_ref[2 * i * n_lanes:2 * (i + 1) * n_lanes]

    def g2(i):
        return g2_ref[2 * i * n_lanes:2 * (i + 1) * n_lanes]

    def twist():
        return tw_ref[:, :n_lanes], tw_ref[:, n_lanes:]

    def second(stage):
        wr, wi = twist()
        parts = []
        for i in range(2):
            ar = stage[:n_rows, i * n_lanes:(i + 1) * n_lanes]
            ai = stage[n_rows:, i * n_lanes:(i + 1) * n_lanes]
            parts.append(jnp.concatenate([ar * wr - ai * wi, ar * wi + ai * wr], axis=1))
        bh, bl = halves(jnp.concatenate(parts, axis=0))
        return dot(bh, f2(0)) + (dot(bh, f2(1)) + dot(bl, f2(0)))

    def inverse(pr, pi):
        wr, wi = twist()
        ph, pll = halves(jnp.concatenate([pr, pi], axis=1))
        mid = dot(ph, g2(0)) + (dot(ph, g2(1)) + dot(pll, g2(0)))
        tr, ti = [], []
        for i in range(2):
            gr = mid[i * n_rows:(i + 1) * n_rows, :n_lanes]
            gi = mid[i * n_rows:(i + 1) * n_rows, n_lanes:]
            tr.append(gr * wr + gi * wi)
            ti.append(gi * wr - gr * wi)
        th, tl = halves(jnp.concatenate([jnp.concatenate(tr, axis=1), jnp.concatenate(ti, axis=1)], axis=0))
        return dot(g1(0), th) + (dot(g1(0), tl) + dot(g1(1), th))

    def pairs(body):
        def step(p, carry):
            body(p)
            return carry

        lax.fori_loop(0, n_pairs, step, 0)

    def rows_of(ref, chan):
        return jnp.concatenate([ref[0, pl.ds(chan, n_dev, stride=n_chans), :],
                                ref[1, pl.ds(chan, n_dev, stride=n_chans), :]], axis=0)

    def both(ref, p):
        return jnp.concatenate([rows_of(ref, 2 * p), rows_of(ref, 2 * p + 1)], axis=1)

    def widen(src, dst):
        for half in range(2):
            dst[half] = src[:, :, half * n_lanes:(half + 1) * n_lanes].astype(F32).reshape(dst.shape[1:])

    def parts_of(ref, p):
        return ref[p, :, :n_lanes], ref[p, :, n_lanes:]

    def taps_spec(p):
        def one(chan):
            return jnp.concatenate([taps[pl.ds(chan, n_dev, stride=2 * n_chans), :],
                                    taps[pl.ds(n_chans + chan, n_dev, stride=2 * n_chans), :]], axis=0)

        h_hi, h_lo = halves(jnp.concatenate([one(2 * p), one(2 * p + 1)], axis=1))
        h_spec[p] = second(dot(f1(0), h_hi) + (dot(f1(0), h_lo) + dot(f1(1), h_hi)))

    pairs(taps_spec)

    def filtered(sig, spec, sign):
        def one(p):
            val = both(sig, p)
            low = val.astype(BF16)
            spec[p] = second(dot(f1(0), low) + dot(f1(1), low))
            sr, si = parts_of(spec, p)
            hr, hi = parts_of(h_spec, p)
            if sign > 0:
                lin = inverse(sr * hr - si * hi, sr * hi + si * hr)
            else:
                lin = inverse(sr * hr + si * hi, si * hr - sr * hi)
            for i in range(2):
                chan = 2 * p + i
                cols = slice(i * n_lanes, (i + 1) * n_lanes)
                res = lin[:, cols] + skip_ref[rank * n_chans + chan] * val[:, cols]
                for odd in range(2):
                    out_f32[odd, pl.ds(chan, n_dev, stride=n_chans), :] = res[odd * n_dev:(odd + 1) * n_dev]

        pairs(one)

    def narrow(dst):
        for half in range(2):
            dst[:, :, half * n_lanes:(half + 1) * n_lanes] = out_f32[half].astype(BF16).reshape(
                n_dev, n_chans, n_lanes)

    wait_all(recv_sem, 0, u_in)
    widen(u_in, u_f32)
    filtered(u_f32, u_spec, 1)
    narrow(y_out)
    exchange(2, y_out, y_ref)
    wait_all(recv_sem, 1, dy_in)
    widen(dy_in, dy_f32)
    filtered(dy_f32, d_spec, -1)
    narrow(du_out)
    exchange(3, du_out, du_ref)

    def taps_grad(p):
        ur, ui = parts_of(u_spec, p)
        dr, di = parts_of(d_spec, p)
        lin = inverse(dr * ur + di * ui, di * ur - dr * ui)
        prod = both(u_f32, p) * both(dy_f32, p)
        for i in range(2):
            chan = 2 * p + i
            cols = slice(i * n_lanes, (i + 1) * n_lanes)
            gskip_ref[pl.ds(chan, 1), :] = jnp.sum(prod[:, cols], axis=0, keepdims=True)
            for odd in range(2):
                gfilt_ref[pl.ds(odd * n_chans + chan, n_dev, stride=2 * n_chans), :] = lin[
                    odd * n_dev:(odd + 1) * n_dev, cols]

    pairs(taps_grad)
    wait_all(recv_sem, 2, y_ref)
    wait_all(recv_sem, 3, du_ref)
    for which, ref in enumerate((u_ref, dy_ref, y_out, du_out)):
        wait_all(send_sem, which, ref)


def mix_channels(u_cm, dy_cm, filt_taps, skip_gain):
    n_dev, n_chans, n_tok = u_cm.shape
    n_lanes = n_tok // 2
    n_rows = 2 * n_dev
    n_wide = 8
    tables = [jnp.asarray(tab) for tab in transform_tables(n_rows, n_lanes)]
    vmem = pl.BlockSpec(memory_space=pltpu.VMEM)
    hbm = pl.BlockSpec(memory_space=pl.ANY)
    block = pltpu.VMEM(u_cm.shape, BF16)
    flat = pltpu.VMEM((2, n_dev * n_chans, n_lanes), F32)
    spec = pltpu.VMEM((n_chans // 2, 2 * n_rows, 2 * n_lanes), F32)
    return pl.pallas_call(
        mix_kernel,
        out_shape=(
            jax.ShapeDtypeStruct(u_cm.shape, BF16),
            jax.ShapeDtypeStruct(u_cm.shape, BF16),
            jax.ShapeDtypeStruct((n_rows * n_chans, n_lanes), F32),
            jax.ShapeDtypeStruct((n_chans, n_lanes), F32),
        ),
        in_specs=[vmem, vmem, hbm, pl.BlockSpec(memory_space=pltpu.SMEM)] + [hbm] * 5,
        out_specs=(vmem,) * 4,
        scratch_shapes=[block] * 4 + [flat] * 3 + [
            pltpu.VMEM((n_wide, n_rows * n_lanes // n_wide, 128), F32),
            pltpu.VMEM((4, 128, n_lanes), F32),
            pltpu.VMEM((n_rows * n_chans, n_lanes), F32),
        ] + [spec] * 3 + [pltpu.VMEM(tab.shape, tab.dtype) for tab in tables] + [
            pltpu.SemaphoreType.DMA((len(tables),)),
            pltpu.SemaphoreType.DMA((n_wide,)),
            pltpu.SemaphoreType.DMA((4,)),
            pltpu.SemaphoreType.DMA((4,)),
        ],
        compiler_params=pltpu.CompilerParams(vmem_limit_bytes=60 * 2 ** 20, collective_id=1, has_side_effects=True),
        cost_estimate=pl.CostEstimate(flops=10 ** 10, bytes_accessed=24 * 2 ** 20, transcendentals=0),
        name="mix_channels",
    )(u_cm, dy_cm, filt_taps, skip_gain, *tables)


RING = 4
PART_ORDERS = ((0, 1, 2), (1, 2, 0), (2, 0, 1))


def part_columns(total):
    tiles = total // 128
    ends = [0, (tiles + 2) // 3 * 128, ((tiles + 2) // 3 + (tiles + 1) // 3) * 128, total]
    return [(ends[i], ends[i + 1]) for i in range(3)]


def grad_kernel(n_in, x_ref, z_ref, d_ref, do_ref, win_ref, wout_ref, *scratch):
    (x_peer, z_peer, d_peer, do_peer, p0, p1, p2, via0, via1, via2, fin0, fin1, fin2, r10, r11, r12,
     via20, via21, via22, fin20, fin21, fin22, r20, r21, r22, via30, via31, via32, fin30, fin31, fin32,
     send_sem, recv_sem, swap_send, swap_recv) = scratch
    partial = (p0, p1, p2)
    vias = ((via0, via1, via2), (via20, via21, via22), (via30, via31, via32))
    fins = ((fin0, fin1, fin2), (fin20, fin21, fin22), (fin30, fin31, fin32))
    reds = ((r10, r11, r12), (r20, r21, r22))
    rank = lax.axis_index("cp")
    core = lax.rem(rank, 2)
    chip = lax.div(rank, 2)
    coords = (lax.div(chip, 16), lax.rem(lax.div(chip, 4), 4), lax.rem(chip, 4))
    strides = (32, 8, 2)
    peer = rank + 1 - 2 * core
    n_out = do_ref.shape[1]
    cols = part_columns(n_in + n_out)

    def at_offset(dim, step):
        pos = lax.rem(coords[dim] + step, RING)
        return pos, rank + (pos - coords[dim]) * strides[dim]

    nxt = [at_offset(dim, 1) for dim in range(3)]
    opp = [at_offset(dim, 2) for dim in range(3)]
    prv = [at_offset(dim, 3) for dim in range(3)]

    barrier = pltpu.get_barrier_semaphore()
    for device in [peer] + [spot[1] for spot in nxt] + [spot[1] for spot in prv]:
        pl.semaphore_signal(barrier, inc=1, device_id={"cp": device}, device_id_type=pl.DeviceIdType.MESH)
    pl.semaphore_wait(barrier, 7)

    def remote(src, dst, send, recv, device):
        return pltpu.make_async_remote_copy(src_ref=src, dst_ref=dst, send_sem=send, recv_sem=recv,
                                            device_id={"cp": device}, device_id_type=pl.DeviceIdType.MESH)

    swaps = []

    def swap(src, dst):
        copy = remote(src, dst, swap_send.at[len(swaps)], swap_recv.at[len(swaps)], peer)
        copy.start()
        swaps.append(copy)

    swap(x_ref.at[:, 1 - core], x_peer)
    row_ranges = [(lo, min(hi, n_in)) for lo, hi in cols]
    for lo, hi in row_ranges:
        swap(d_ref.at[pl.ds(lo, hi - lo)], d_peer.at[pl.ds(lo, hi - lo)])
    swap(z_ref.at[:, 1 - core], z_peer)
    swap(do_ref, do_peer)

    n_tok = x_ref.shape[-1]
    n_rows = x_ref.shape[0] * x_ref.shape[2]

    def flat(val):
        return val.reshape(n_rows, n_tok)

    def mm(a, b, cb):
        return lax.dot_general(a, b, (((1,), (cb,)), ((), ())), preferred_element_type=F32)

    def put(part, col, val):
        partial[part][:, :, :, :, pl.ds(col, val.shape[1])] = val.reshape(
            RING, RING, RING, x_ref.shape[2], val.shape[1])

    def slab(ref, axis, pos, col=None):
        index = [slice(None)] * len(ref.shape)
        if axis is not None:
            index[axis] = pos
        if col is not None:
            index[-1] = pl.ds(*col)
        return ref.at[tuple(index)]

    copies = {}

    def send(part, phase, which, src, dst, device):
        slot = (phase * 3 + part) * 6 + which
        copy = remote(src, dst, send_sem.at[slot], recv_sem.at[slot], device)
        copy.start()
        copies[part, phase, which] = copy

    def source(part, phase):
        return partial[part] if phase == 0 else reds[phase - 1][part]

    def axis_of(part, phase):
        order = PART_ORDERS[part]
        left = sorted(order[phase:])
        return left.index(order[phase])

    def split(part):
        lo, hi = cols[part]
        first = ((hi - lo) // 128 + 1) // 2 * 128
        return (0, first), (first, hi - lo - first)

    def launch(part, phase):
        dim, axis, src = PART_ORDERS[part][phase], axis_of(part, phase), source(part, phase)
        a_cols, b_cols = split(part)
        via, fin = vias[phase][part], fins[phase][part]
        send(part, phase, 0, slab(src, axis, opp[dim][0], a_cols), slab(via, None, None, a_cols), nxt[dim][1])
        send(part, phase, 1, slab(src, axis, opp[dim][0], b_cols), slab(via, None, None, b_cols), prv[dim][1])
        send(part, phase, 2, slab(src, axis, nxt[dim][0], b_cols), slab(fin, 0, 0, b_cols), nxt[dim][1])
        send(part, phase, 3, slab(src, axis, prv[dim][0], a_cols), slab(fin, 0, 1, a_cols), prv[dim][1])

    def each_block(shape, body):
        lead = shape[:-2]
        count = int(np.prod(lead)) if lead else 1
        if count == 1:
            body(tuple(0 for _ in lead))
            return

        def step(i, carry):
            index = []
            for size in reversed(lead):
                index.insert(0, lax.rem(i, size))
                i = lax.div(i, size)
            body(tuple(index))
            return carry

        lax.fori_loop(0, count, step, 0, unroll=min(count, 4))

    def relay(part, phase):
        dim, axis, src = PART_ORDERS[part][phase], axis_of(part, phase), source(part, phase)
        a_cols, b_cols = split(part)
        via, fin = vias[phase][part], fins[phase][part]
        for which, col, spot, side in ((0, a_cols, nxt[dim], 0), (1, b_cols, prv[dim], 1)):
            copies[part, phase, which].wait_recv()
            span = pl.ds(*col)

            def add(index):
                at = index[:axis] + (spot[0],) + index[axis:]
                src[at + (slice(None), span)] = src[at + (slice(None), span)] + via[index + (slice(None), span)]

            each_block(via.shape, add)
            send(part, phase, 4 + which, slab(src, axis, spot[0], col), slab(fin, 0, side, col), spot[1])

    def finish(part, phase):
        dim, axis, src = PART_ORDERS[part][phase], axis_of(part, phase), source(part, phase)
        via, fin = vias[phase][part], fins[phase][part]
        for which in range(2, 6):
            copies[part, phase, which].wait_recv()

        def add(index):
            at = index[:axis] + (coords[dim],) + index[axis:]
            total = src[at] + fin[(0,) + index] + fin[(1,) + index]
            if phase < 2:
                reds[phase][part][index] = total
            else:
                lo, hi = cols[part]
                mid = min(max(n_in, lo), hi)
                if mid > lo:
                    win_ref[:, lo:mid] = total[:, :mid - lo].astype(win_ref.dtype)
                if hi > mid:
                    wout_ref[:, mid - n_in:hi - n_in] = total[:, mid - lo:].astype(wout_ref.dtype)

        each_block(via.shape, add)

    x_own = flat(x_ref[:, core])
    swaps[0].wait_recv()
    x_other = flat(x_peer[...])
    for part in range(3):
        lo, hi = cols[part]
        swaps[1 + part].wait_recv()
        for start in range(lo, min(hi, n_in), 512):
            size = min(512, min(hi, n_in) - start)
            put(part, start - lo, mm(x_own, d_ref[pl.ds(start, size), :], 1)
                + mm(x_other, d_peer[pl.ds(start, size), :], 1))
        if hi > n_in:
            swaps[4].wait_recv()
            swaps[5].wait_recv()
            z_own, z_other = flat(z_ref[:, core]), flat(z_peer[...])
            for start in range(max(lo, n_in), hi, 512):
                size = min(512, hi - start)
                put(part, start - lo, mm(z_own, do_ref[:, pl.ds(start - n_in, size)], 0)
                    + mm(z_other, do_peer[:, pl.ds(start - n_in, size)], 0))
        launch(part, 0)
    for phase in range(3):
        for part in range(3):
            relay(part, phase)
        for part in range(3):
            finish(part, phase)
            if phase < 2:
                launch(part, phase + 1)
    for copy in copies.values():
        copy.wait_send()
    for copy in swaps:
        copy.wait_send()


def weight_grads(x_cm, z_cm, d_cm, d_out):
    n_chip, n_core, n_row, n_tok = x_cm.shape
    n_in, n_out = d_cm.shape[0], d_out.shape[1]
    widths = [hi - lo for lo, hi in part_columns(n_in + n_out)]
    vmem = pl.BlockSpec(memory_space=pltpu.VMEM)
    scratch = [pltpu.VMEM((n_chip, n_row, n_tok), BF16), pltpu.VMEM((n_chip, n_row, n_tok), BF16),
               pltpu.VMEM(d_cm.shape, BF16), pltpu.VMEM(d_out.shape, BF16)]
    scratch += [pltpu.VMEM((RING,) * 3 + (n_row, w), F32) for w in widths]
    for n_lead in (2, 1, 0):
        lead = (RING,) * n_lead
        scratch += [pltpu.VMEM(lead + (n_row, w), F32) for w in widths]
        scratch += [pltpu.VMEM((2,) + lead + (n_row, w), F32) for w in widths]
        if n_lead:
            scratch += [pltpu.VMEM(lead + (n_row, w), F32) for w in widths]
    scratch += [pltpu.SemaphoreType.DMA((54,)), pltpu.SemaphoreType.DMA((54,)),
                pltpu.SemaphoreType.DMA((6,)), pltpu.SemaphoreType.DMA((6,))]
    return pl.pallas_call(
        functools.partial(grad_kernel, n_in),
        out_shape=(jax.ShapeDtypeStruct((n_row, n_in), BF16), jax.ShapeDtypeStruct((n_row, n_out), BF16)),
        in_specs=[vmem] * 4,
        out_specs=(vmem, vmem),
        scratch_shapes=scratch,
        compiler_params=pltpu.CompilerParams(vmem_limit_bytes=56 * 2 ** 20, collective_id=0, has_side_effects=True),
        cost_estimate=pl.CostEstimate(flops=5 * 10 ** 9, bytes_accessed=8 * 2 ** 20, transcendentals=0),
        name="weight_grads",
    )(x_cm, z_cm, d_cm, d_out)


def solution(mesh):
    ctx_size = mesh.shape["cp"]

    def local_step(x_seq, w_in, w_out, filt_taps, skip_gain, d_out):
        n_batch, n_tok, width = x_seq.shape
        n_chans = width // ctx_size
        seq_len = n_tok * ctx_size
        n_lanes = n_tok // 2
        x_tok, do_tok = x_seq[0], d_out[0]

        def mm(a, b, ca, cb):
            return lax.dot_general(a, b, (((ca,), (cb,)), ((), ())), preferred_element_type=F32)

        qkv = mm(w_in, x_tok, 0, 1).astype(BF16)
        q_act, k_act, v_act = qkv[:width], qkv[width:2 * width], qkv[2 * width:]
        u_act = k_act * v_act
        dz_act = mm(w_out, do_tok, 1, 1).astype(BF16)
        dy_act = dz_act * q_act
        by_dev = (ctx_size, n_chans, n_tok)
        y_dev, du_dev, gfilt, gskip = mix_channels(u_act.reshape(by_dev), dy_act.reshape(by_dev), filt_taps, skip_gain)
        grad_filt = gfilt.reshape(seq_len // n_lanes, n_chans, n_lanes).transpose(0, 2, 1).reshape(seq_len, n_chans)
        grad_skip = jnp.sum(gskip, axis=1)
        y_act, du_act = y_dev.reshape(width, n_tok), du_dev.reshape(width, n_tok)
        z_act = q_act * y_act
        d_qkv = jnp.concatenate([dz_act * y_act, du_act * v_act, du_act * k_act], axis=0)
        grad_x = mm(d_qkv, w_in, 0, 1).astype(BF16)[None]
        by_core = (ctx_size // 2, 2, n_chans, n_tok)
        grad_w_in, grad_w_out = weight_grads(
            x_tok.T.reshape(by_core), z_act.reshape(by_core), d_qkv, do_tok)
        return grad_x, grad_w_in, grad_w_out, grad_filt, grad_skip

    seq_spec = P("dp", "cp", None)
    row_spec = P(("dp", "cp"), None)
    return jax.shard_map(
        local_step,
        mesh=mesh,
        in_specs=(seq_spec, P(), P(), P(), P(), seq_spec),
        out_specs=(seq_spec, row_spec, row_spec, P("dp", "cp"), P(("dp", "cp"))),
        check_vma=False,
    )
```

```python
import functools

import jax
import jax.numpy as jnp
import numpy as np
from jax import lax
from jax.experimental import pallas as pl
from jax.experimental.pallas import tpu as pltpu
from jax.sharding import PartitionSpec as P

F32, BF16 = jnp.float32, jnp.bfloat16


def split_const(mat):
    hi = mat.astype(np.float32).astype(jnp.bfloat16)
    lo = (mat - hi.astype(np.float64)).astype(np.float32).astype(jnp.bfloat16)
    return hi, lo


@functools.lru_cache(None)
def transform_tables(n_rows, n_lanes):
    n = n_rows * n_lanes
    t1 = np.concatenate([np.arange(0, n_rows, 2), np.arange(1, n_rows, 2)])
    k1 = np.arange(n_rows)
    ang = 2 * np.pi * np.outer(k1 + 0.25, t1) / n_rows
    f1 = np.concatenate([np.cos(ang), -np.sin(ang)], axis=0)
    g1 = f1.T / n
    t2 = np.arange(n_lanes)
    psi = 2 * np.pi * (np.outer(t2, t2) % n_lanes) / n_lanes
    cos2, sin2 = np.cos(psi), np.sin(psi)
    f2 = np.block([[cos2, -sin2], [sin2, cos2]])
    g2 = f2.T
    twist = 2 * np.pi * np.outer(k1 + 0.25, t2) / n
    twid = np.concatenate([np.cos(twist), -np.sin(twist)], axis=1).astype(np.float32)
    f1h, f1l = split_const(f1)
    g1h, g1l = split_const(g1)
    f2h, f2l = split_const(f2)
    g2h, g2l = split_const(g2)
    return (
        np.concatenate([f1h, f1l], axis=1),
        np.concatenate([f2h, f2l], axis=0),
        np.concatenate([g2h, g2l], axis=0),
        np.concatenate([g1h, g1l], axis=1),
        twid,
    )


def dot(a, b):
    return jnp.dot(a, b, preferred_element_type=F32)


def halves(val):
    hi = val.astype(BF16)
    lo = (val - hi.astype(F32)).astype(BF16)
    return hi, lo


RING = 4
PART_ORDERS = ((0, 1, 2), (1, 2, 0), (2, 0, 1))


def part_columns(total):
    tiles = total // 128
    ends = [0, (tiles + 2) // 3 * 128, ((tiles + 2) // 3 + (tiles + 1) // 3) * 128, total]
    return [(ends[i], ends[i + 1]) for i in range(3)]


def hyena_kernel(qkv_ref, dz_ref, x_ref, do_ref, filt_ref, skip_ref, win_hbm, f1_hbm, f2_hbm, g2_hbm, g1_hbm, tw_hbm,
                 gx_ref, gwin_ref, gwout_ref, gfilt_ref, gskip_ref, *scratch):
    names = iter(scratch)

    def take(count):
        return [next(names) for _ in range(count)]

    u_out, dy_out, y_out, du_out, u_in, dy_in, y_in, du_in = take(8)
    u_f32, dy_f32, out_f32 = take(3)
    wide, flip, taps = take(3)
    u_spec, h_spec, d_spec = take(3)
    f1_ref, f2_ref, g2_ref, g1_ref, tw_ref, win_ref = take(6)
    z_own, d_own, x_peer, z_peer, d_peer, do_peer = take(6)
    partial = take(6)
    vias, fins, reds = [], [], []
    for phase in range(3):
        vias.append(take(6))
        fins.append(take(6))
        if phase < 2:
            reds.append(take(6))
    load_sem, wide_sem, ex_send, ex_recv, swap_send, swap_recv, ring_send, ring_recv = take(8)

    n_dev, n_chans, n_tok = u_out.shape
    n_lanes = n_tok // 2
    n_rows = 2 * n_dev
    n_pairs = n_chans // 2
    width = n_dev * n_chans
    rank = lax.axis_index("cp")
    core = lax.rem(rank, 2)
    chip = lax.div(rank, 2)
    coords = (lax.div(chip, 16), lax.rem(lax.div(chip, 4), 4), lax.rem(chip, 4))
    strides = (32, 8, 2)
    peer = rank + 1 - 2 * core

    def remote(src, dst, send, recv, device):
        return pltpu.make_async_remote_copy(src_ref=src, dst_ref=dst, send_sem=send, recv_sem=recv,
                                            device_id={"cp": device}, device_id_type=pl.DeviceIdType.MESH)

    def others(body):
        def step(i, carry):
            body(lax.rem(rank + i, n_dev))
            return carry

        lax.fori_loop(1, n_dev, step, 0)

    barrier = pltpu.get_barrier_semaphore()
    others(lambda dev: pl.semaphore_signal(barrier, inc=1, device_id={"cp": dev}, device_id_type=pl.DeviceIdType.MESH))

    n_slot, per_slot = wide.shape[0], wide.shape[1]
    n_wide = filt_ref.shape[0] // per_slot
    first_lane = pl.multiple_of(lax.div(rank * n_chans, 128) * 128, 128)
    wides = [pltpu.make_async_copy(
        filt_ref.at[pl.ds(i * per_slot, per_slot), pl.ds(first_lane, 128)], wide.at[i % n_slot], wide_sem.at[i])
        for i in range(n_wide)]
    loads = [pltpu.make_async_copy(src, dst, load_sem.at[i]) for i, (src, dst) in enumerate(
        ((f1_hbm, f1_ref), (f2_hbm, f2_ref), (g2_hbm, g2_ref), (g1_hbm, g1_ref), (tw_hbm, tw_ref), (win_hbm, win_ref)))]
    for copy in wides[:n_slot] + loads:
        copy.start()

    def act(i):
        return qkv_ref[i * width:(i + 1) * width]

    u_out[...] = (act(1) * act(2)).reshape(u_out.shape)
    dy_out[...] = (dz_ref[...] * act(0)).reshape(dy_out.shape)
    pl.semaphore_wait(barrier, n_dev - 1)

    def exchange(which, src, dst):
        others(lambda dev: remote(src.at[dev], dst.at[rank], ex_send.at[which], ex_recv.at[which], dev).start())
        dst[rank] = src[rank]

    def wait_all(sem, which, ref):
        part = ref.at[pl.ds(0, n_dev - 1)]
        pltpu.make_async_copy(part, part, sem.at[which]).wait()

    exchange(0, u_out, u_in)
    exchange(1, dy_out, dy_in)

    swaps = []

    def swap(src, dst):
        copy = remote(src, dst, swap_send.at[len(swaps)], swap_recv.at[len(swaps)], peer)
        copy.start()
        swaps.append(copy)
        return copy

    x_swap = swap(x_ref.at[:, 1 - core], x_peer)
    do_swap = swap(do_ref, do_peer)

    own_row = pl.multiple_of(lax.rem(rank * n_chans, 128), n_chans)
    per_wide = per_slot // n_lanes

    for i in range(n_wide):
        wides[i].wait()

        def turn(j, carry):
            for k in range(4):
                tile = 4 * j + k
                flip[k] = wide[i % n_slot, pl.ds(pl.multiple_of(tile * n_lanes, n_lanes), n_lanes), :].T
                at = pl.multiple_of((i * per_wide + tile) * n_chans, n_chans)
                taps[pl.ds(at, n_chans), :] = flip[k, pl.ds(own_row, n_chans), :]
            return carry

        lax.fori_loop(0, per_wide // 4, turn, 0)
        if i + n_slot < n_wide:
            wides[i + n_slot].start()
    for copy in loads[:5]:
        copy.wait()

    def f1(i):
        return f1_ref[:, i * n_rows:(i + 1) * n_rows]

    def g1(i):
        return g1_ref[:, 2 * i * n_rows:2 * (i + 1) * n_rows]

    def f2(i):
        return f2_ref[2 * i * n_lanes:2 * (i + 1) * n_lanes]

    def g2(i):
        return g2_ref[2 * i * n_lanes:2 * (i + 1) * n_lanes]

    def twist():
        return tw_ref[:, :n_lanes], tw_ref[:, n_lanes:]

    def second(stage):
        wr, wi = twist()
        parts = []
        for i in range(2):
            ar = stage[:n_rows, i * n_lanes:(i + 1) * n_lanes]
            ai = stage[n_rows:, i * n_lanes:(i + 1) * n_lanes]
            parts.append(jnp.concatenate([ar * wr - ai * wi, ar * wi + ai * wr], axis=1))
        bh, bl = halves(jnp.concatenate(parts, axis=0))
        return dot(bh, f2(0)) + (dot(bh, f2(1)) + dot(bl, f2(0)))

    def inverse(pr, pi):
        wr, wi = twist()
        ph, pll = halves(jnp.concatenate([pr, pi], axis=1))
        mid = dot(ph, g2(0)) + (dot(ph, g2(1)) + dot(pll, g2(0)))
        tr, ti = [], []
        for i in range(2):
            gr = mid[i * n_rows:(i + 1) * n_rows, :n_lanes]
            gi = mid[i * n_rows:(i + 1) * n_rows, n_lanes:]
            tr.append(gr * wr + gi * wi)
            ti.append(gi * wr - gr * wi)
        th, tl = halves(jnp.concatenate([jnp.concatenate(tr, axis=1), jnp.concatenate(ti, axis=1)], axis=0))
        return dot(g1(0), th) + (dot(g1(0), tl) + dot(g1(1), th))

    def pairs(body):
        def step(p, carry):
            body(p)
            return carry

        lax.fori_loop(0, n_pairs, step, 0)

    def rows_of(ref, chan):
        return jnp.concatenate([ref[0, pl.ds(chan, n_dev, stride=n_chans), :],
                                ref[1, pl.ds(chan, n_dev, stride=n_chans), :]], axis=0)

    def both(ref, p):
        return jnp.concatenate([rows_of(ref, 2 * p), rows_of(ref, 2 * p + 1)], axis=1)

    def widen(src, dst):
        for half in range(2):
            dst[half] = src[:, :, half * n_lanes:(half + 1) * n_lanes].astype(F32).reshape(dst.shape[1:])

    def parts_of(ref, p):
        return ref[p, :, :n_lanes], ref[p, :, n_lanes:]

    def taps_spec(p):
        def one(chan):
            return jnp.concatenate([taps[pl.ds(chan, n_dev, stride=2 * n_chans), :],
                                    taps[pl.ds(n_chans + chan, n_dev, stride=2 * n_chans), :]], axis=0)

        h_hi, h_lo = halves(jnp.concatenate([one(2 * p), one(2 * p + 1)], axis=1))
        h_spec[p] = second(dot(f1(0), h_hi) + (dot(f1(0), h_lo) + dot(f1(1), h_hi)))

    pairs(taps_spec)

    def filtered(sig, spec, sign):
        def one(p):
            val = both(sig, p)
            low = val.astype(BF16)
            spec[p] = second(dot(f1(0), low) + dot(f1(1), low))
            sr, si = parts_of(spec, p)
            hr, hi = parts_of(h_spec, p)
            if sign > 0:
                lin = inverse(sr * hr - si * hi, sr * hi + si * hr)
            else:
                lin = inverse(sr * hr + si * hi, si * hr - sr * hi)
            for i in range(2):
                chan = 2 * p + i
                cols = slice(i * n_lanes, (i + 1) * n_lanes)
                res = lin[:, cols] + skip_ref[rank * n_chans + chan] * val[:, cols]
                for odd in range(2):
                    out_f32[odd, pl.ds(chan, n_dev, stride=n_chans), :] = res[odd * n_dev:(odd + 1) * n_dev]

        pairs(one)

    def narrow(dst):
        for half in range(2):
            dst[:, :, half * n_lanes:(half + 1) * n_lanes] = out_f32[half].astype(BF16).reshape(
                n_dev, n_chans, n_lanes)

    wait_all(ex_recv, 0, u_in)
    widen(u_in, u_f32)
    filtered(u_f32, u_spec, 1)
    narrow(y_out)
    exchange(2, y_out, y_in)
    wait_all(ex_recv, 1, dy_in)
    widen(dy_in, dy_f32)
    filtered(dy_f32, d_spec, -1)
    narrow(du_out)
    exchange(3, du_out, du_in)

    wait_all(ex_recv, 2, y_in)
    y_act = y_in[...].reshape(width, n_tok)
    z_own[...] = (act(0) * y_act).reshape(z_own.shape)
    d_own[0:width] = dz_ref[...] * y_act
    z_swap = swap(z_own.at[:, 1 - core], z_peer)
    d_swaps = [swap(d_own.at[pl.ds(0, width)], d_peer.at[pl.ds(0, width)])]

    def taps_grad(p):
        ur, ui = parts_of(u_spec, p)
        dr, di = parts_of(d_spec, p)
        lin = inverse(dr * ur + di * ui, di * ur - dr * ui)
        prod = both(u_f32, p) * both(dy_f32, p)
        for i in range(2):
            chan = 2 * p + i
            cols = slice(i * n_lanes, (i + 1) * n_lanes)
            gskip_ref[pl.ds(chan, 1), :] = jnp.sum(prod[:, cols], axis=0, keepdims=True)
            for odd in range(2):
                gfilt_ref[pl.ds(odd * n_chans + chan, n_dev, stride=2 * n_chans), :] = lin[
                    odd * n_dev:(odd + 1) * n_dev, cols]

    pairs(taps_grad)

    def at_offset(dim, step):
        pos = lax.rem(coords[dim] + step, RING)
        return pos, rank + (pos - coords[dim]) * strides[dim]

    nxt = [at_offset(dim, 1) for dim in range(3)]
    opp = [at_offset(dim, 2) for dim in range(3)]
    prv = [at_offset(dim, 3) for dim in range(3)]
    cols = part_columns(2 * width)
    half_rows = width // 2

    def mm(a, b, cb):
        return lax.dot_general(a, b, (((1,), (cb,)), ((), ())), preferred_element_type=F32)

    def flat(val):
        return val.reshape(half_rows, n_tok)

    def segments(part):
        lo, hi = cols[part % 3]
        runs = []
        for first, is_out, base in (((0, False, 0), (width, True, 0)) if part < 3 else ((0, False, width),)):
            last = first + width if part < 3 else 2 * width
            a, b = max(lo, first), min(hi, last)
            if a < b:
                runs.append((is_out, base + a - first, a - lo, b - a))
        return runs

    def products(part):
        for is_out, first, place, size in segments(part):
            for off in range(0, size, 512):
                step = min(512, size - off)
                at = first + off
                if is_out:
                    val = (mm(flat(z_own[:, core]), do_ref[:, at:at + step], 0)
                           + mm(flat(z_peer[...]), do_peer[:, at:at + step], 0))
                else:
                    val = (mm(flat(x_ref[:, core]), d_own[at:at + step], 1)
                           + mm(flat(x_peer[...]), d_peer[at:at + step], 1))
                partial[part][:, :, :, :, place + off:place + off + step] = val.reshape(
                    RING, RING, RING, n_chans, step)

    def slab(ref, axis, pos, col=None):
        index = [slice(None)] * len(ref.shape)
        if axis is not None:
            index[axis] = pos
        if col is not None:
            index[-1] = pl.ds(*col)
        return ref.at[tuple(index)]

    copies = {}

    def send(part, phase, which, src, dst, device):
        slot = (phase * 6 + part) * 6 + which
        copy = remote(src, dst, ring_send.at[slot], ring_recv.at[slot], device)
        copy.start()
        copies[part, phase, which] = copy

    def setting(part, phase):
        order = PART_ORDERS[(part + part // 3) % 3]
        dim = order[phase]
        axis = sorted(order[phase:]).index(dim)
        src = partial[part] if phase == 0 else reds[phase - 1][part]
        size = src.shape[-1]
        first = (size // 128 + 1) // 2 * 128
        return dim, axis, src, vias[phase][part], fins[phase][part], (0, first), (first, size - first)

    def launch(part, phase):
        dim, axis, src, via, fin, a_cols, b_cols = setting(part, phase)
        send(part, phase, 0, slab(src, axis, opp[dim][0], a_cols), slab(via, None, None, a_cols), nxt[dim][1])
        send(part, phase, 1, slab(src, axis, opp[dim][0], b_cols), slab(via, None, None, b_cols), prv[dim][1])
        send(part, phase, 2, slab(src, axis, nxt[dim][0], b_cols), slab(fin, 0, 0, b_cols), nxt[dim][1])
        send(part, phase, 3, slab(src, axis, prv[dim][0], a_cols), slab(fin, 0, 1, a_cols), prv[dim][1])

    def each_block(shape, body):
        lead = shape[:-2]
        count = int(np.prod(lead)) if lead else 1
        if count == 1:
            body(tuple(0 for _ in lead))
            return

        def step(i, carry):
            index = []
            for size in reversed(lead):
                index.insert(0, lax.rem(i, size))
                i = lax.div(i, size)
            body(tuple(index))
            return carry

        lax.fori_loop(0, count, step, 0, unroll=min(count, 4))

    def relay(part, phase):
        dim, axis, src, via, fin, a_cols, b_cols = setting(part, phase)
        for which, col, spot, side in ((0, a_cols, nxt[dim], 0), (1, b_cols, prv[dim], 1)):
            copies[part, phase, which].wait_recv()
            span = pl.ds(*col)

            def add(index):
                at = index[:axis] + (spot[0],) + index[axis:]
                src[at + (slice(None), span)] = src[at + (slice(None), span)] + via[index + (slice(None), span)]

            each_block(via.shape, add)
            send(part, phase, 4 + which, slab(src, axis, spot[0], col), slab(fin, 0, side, col), spot[1])

    def finish(part, phase):
        dim, axis, src, via, fin, _, _ = setting(part, phase)
        for which in range(2, 6):
            copies[part, phase, which].wait_recv()

        def add(index):
            at = index[:axis] + (coords[dim],) + index[axis:]
            total = src[at] + fin[(0,) + index] + fin[(1,) + index]
            if phase < 2:
                reds[phase][part][index] = total
                return
            for is_out, first, place, size in segments(part):
                dst = gwout_ref if is_out else gwin_ref
                dst[:, first:first + size] = total[:, place:place + size].astype(dst.dtype)

        each_block(via.shape, add)
        if phase < 2:
            launch(part, phase + 1)

    early, late = (0, 1, 2), (3, 4, 5)
    for copy in (x_swap, do_swap, z_swap, d_swaps[0]):
        copy.wait_recv()
    for part in early:
        products(part)
        launch(part, 0)

    wait_all(ex_recv, 3, du_in)
    du_act = du_in[...].reshape(width, n_tok)
    for i in (1, 2):
        d_own[i * width:(i + 1) * width] = du_act * act(3 - i)
        span = pl.ds(i * width, width)
        d_swaps.append(swap(d_own.at[span], d_peer.at[span]))

    def run(step, parts, phase):
        for part in parts:
            step(part, phase)

    run(relay, early, 0)
    for copy in d_swaps[1:]:
        copy.wait_recv()
    for part in late:
        products(part)
        launch(part, 0)

    loads[5].wait()
    for first in range(0, width, 256):
        gx_ref[:, first:first + 256] = dot(win_ref[first:first + 256], d_own[...]).T.astype(gx_ref.dtype)

    run(finish, early, 0)
    run(relay, late, 0)
    run(relay, early, 1)
    run(finish, early, 1)
    run(finish, late, 0)
    run(relay, early, 2)
    run(finish, early, 2)
    run(relay, late, 1)
    run(finish, late, 1)
    run(relay, late, 2)
    run(finish, late, 2)
    for which, ref in enumerate((u_out, dy_out, y_out, du_out)):
        wait_all(ex_send, which, ref)
    for copy in list(copies.values()) + swaps:
        copy.wait_send()


def hyena_grads(qkv, dz, x_cm, d_out, filt_taps, skip_gain, w_in, n_dev):
    n_chip, n_core, n_chans, n_tok = x_cm.shape
    width = dz.shape[0]
    n_lanes, n_rows = n_tok // 2, 2 * n_dev
    n_taps = filt_taps.shape[0]
    n_wide, n_slot = 8, 4
    tables = [jnp.asarray(tab) for tab in transform_tables(n_rows, n_lanes)]
    vmem = pl.BlockSpec(memory_space=pltpu.VMEM)
    hbm = pl.BlockSpec(memory_space=pl.ANY)
    widths = [hi - lo for lo, hi in part_columns(2 * width)] * 2
    scratch = [pltpu.VMEM((n_dev, n_chans, n_tok), BF16)] * 8
    scratch += [pltpu.VMEM((2, width, n_lanes), F32)] * 3
    scratch += [pltpu.VMEM((n_slot, n_taps // n_wide, 128), F32), pltpu.VMEM((4, 128, n_lanes), F32),
                pltpu.VMEM((n_rows * n_chans, n_lanes), F32)]
    scratch += [pltpu.VMEM((n_chans // 2, 2 * n_rows, 2 * n_lanes), F32)] * 3
    scratch += [pltpu.VMEM(arr.shape, arr.dtype) for arr in tables + [w_in]]
    scratch += [pltpu.VMEM(x_cm.shape, BF16), pltpu.VMEM(qkv.shape, BF16), pltpu.VMEM((n_chip, n_chans, n_tok), BF16),
                pltpu.VMEM((n_chip, n_chans, n_tok), BF16), pltpu.VMEM(qkv.shape, BF16), pltpu.VMEM(d_out.shape, BF16)]
    scratch += [pltpu.VMEM((RING,) * 3 + (n_chans, w), F32) for w in widths]
    for n_lead in (2, 1, 0):
        lead = (RING,) * n_lead
        scratch += [pltpu.VMEM(lead + (n_chans, w), F32) for w in widths]
        scratch += [pltpu.VMEM((2,) + lead + (n_chans, w), F32) for w in widths]
        if n_lead:
            scratch += [pltpu.VMEM(lead + (n_chans, w), F32) for w in widths]
    scratch += [pltpu.SemaphoreType.DMA((n,)) for n in (len(tables) + 1, n_wide, 4, 4, 6, 6, 108, 108)]
    return pl.pallas_call(
        hyena_kernel,
        out_shape=(
            jax.ShapeDtypeStruct((n_tok, width), BF16),
            jax.ShapeDtypeStruct((n_chans, 3 * width), BF16),
            jax.ShapeDtypeStruct((n_chans, width), BF16),
            jax.ShapeDtypeStruct((n_rows * n_chans, n_lanes), F32),
            jax.ShapeDtypeStruct((n_chans, n_lanes), F32),
        ),
        in_specs=[vmem] * 4 + [hbm, pl.BlockSpec(memory_space=pltpu.SMEM)] + [hbm] * 6,
        out_specs=(vmem,) * 5,
        scratch_shapes=scratch,
        compiler_params=pltpu.CompilerParams(vmem_limit_bytes=63 * 2 ** 20, collective_id=0, has_side_effects=True),
        cost_estimate=pl.CostEstimate(flops=2 * 10 ** 10, bytes_accessed=32 * 2 ** 20, transcendentals=0),
        name="hyena_grads",
    )(qkv, dz, x_cm, d_out, filt_taps, skip_gain, w_in, *tables)


def solution(mesh):
    ctx_size = mesh.shape["cp"]

    def local_step(x_seq, w_in, w_out, filt_taps, skip_gain, d_out):
        n_batch, n_tok, width = x_seq.shape
        n_chans = width // ctx_size
        seq_len = n_tok * ctx_size
        n_lanes = n_tok // 2
        x_tok, do_tok = x_seq[0], d_out[0]

        def mm(a, b, ca, cb):
            return lax.dot_general(a, b, (((ca,), (cb,)), ((), ())), preferred_element_type=F32)

        qkv = mm(w_in, x_tok, 0, 1).astype(BF16)
        dz = mm(w_out, do_tok, 1, 1).astype(BF16)
        x_cm = x_tok.T.reshape(ctx_size // 2, 2, n_chans, n_tok)
        grad_x, grad_w_in, grad_w_out, gfilt, gskip = hyena_grads(
            qkv, dz, x_cm, do_tok, filt_taps, skip_gain, w_in, ctx_size)
        grad_filt = gfilt.reshape(seq_len // n_lanes, n_chans, n_lanes).transpose(0, 2, 1).reshape(seq_len, n_chans)
        return grad_x[None], grad_w_in, grad_w_out, grad_filt, jnp.sum(gskip, axis=1)

    seq_spec = P("dp", "cp", None)
    row_spec = P(("dp", "cp"), None)
    return jax.shard_map(
        local_step,
        mesh=mesh,
        in_specs=(seq_spec, P(), P(), P(), P(), seq_spec),
        out_specs=(seq_spec, row_spec, row_spec, P("dp", "cp"), P(("dp", "cp"))),
        check_vma=False,
    )
```

```python
import functools

import jax
import jax.numpy as jnp
import numpy as np
from jax import lax
from jax.experimental import pallas as pl
from jax.experimental.pallas import tpu as pltpu
from jax.sharding import PartitionSpec as P

F32, BF16 = jnp.float32, jnp.bfloat16


def split_const(mat):
    hi = mat.astype(np.float32).astype(jnp.bfloat16)
    lo = (mat - hi.astype(np.float64)).astype(np.float32).astype(jnp.bfloat16)
    return hi, lo


@functools.lru_cache(None)
def transform_tables(n_rows, n_lanes):
    n = n_rows * n_lanes
    t1 = np.concatenate([np.arange(0, n_rows, 2), np.arange(1, n_rows, 2)])
    k1 = np.arange(n_rows)
    ang = 2 * np.pi * np.outer(k1 + 0.25, t1) / n_rows
    f1 = np.concatenate([np.cos(ang), -np.sin(ang)], axis=0)
    g1 = f1.T / n
    t2 = np.arange(n_lanes)
    psi = 2 * np.pi * (np.outer(t2, t2) % n_lanes) / n_lanes
    cos2, sin2 = np.cos(psi), np.sin(psi)
    f2 = np.block([[cos2, -sin2], [sin2, cos2]])
    g2 = f2.T
    twist = 2 * np.pi * np.outer(k1 + 0.25, t2) / n
    twid = np.concatenate([np.cos(twist), -np.sin(twist)], axis=1).astype(np.float32)
    f1h, f1l = split_const(f1)
    g1h, g1l = split_const(g1)
    f2h, f2l = split_const(f2)
    g2h, g2l = split_const(g2)
    return (
        np.concatenate([f1h, f1l], axis=1),
        np.concatenate([f2h, f2l], axis=0),
        np.concatenate([g2h, g2l], axis=0),
        np.concatenate([g1h, g1l], axis=1),
        twid,
    )


def dot(a, b):
    return jnp.dot(a, b, preferred_element_type=F32)


def halves(val):
    hi = val.astype(BF16)
    lo = (val - hi.astype(F32)).astype(BF16)
    return hi, lo


RING = 4
PART_ORDERS = ((0, 1, 2), (1, 2, 0), (2, 0, 1))


def part_columns(total):
    tiles = total // 128
    ends = [0, (tiles + 2) // 3 * 128, ((tiles + 2) // 3 + (tiles + 1) // 3) * 128, total]
    return [(ends[i], ends[i + 1]) for i in range(3)]


def hyena_kernel(x_ref, do_ref, filt_ref, skip_ref, win_hbm, wout_hbm, f1_hbm, f2_hbm, g2_hbm, g1_hbm, tw_hbm,
                 gx_ref, gwin_ref, gwout_ref, gfilt_ref, gskip_ref, *scratch):
    names = iter(scratch)

    def take(count):
        return [next(names) for _ in range(count)]

    u_out, dy_out, u_in, dy_in, y_in, du_in = take(6)
    y_out, du_out = u_in, dy_in
    u_f32, dy_f32, out_f32 = take(3)
    wide, flip, taps = take(3)
    u_spec, h_spec, d_spec = take(3)
    f1_ref, f2_ref, g2_ref, g1_ref, tw_ref, win_ref, wout_ref = take(7)
    qkv_ref, dz_ref = take(2)
    x_own, z_own, d_own, x_peer, z_peer, d_peer, do_peer = take(7)
    partial = take(6)
    vias, fins, reds = [], [], []
    for phase in range(3):
        vias.append(take(6))
        fins.append(take(6))
        if phase < 2:
            reds.append(take(6))
    load_sem, wide_sem, ex_send, ex_recv, swap_send, swap_recv, ring_send, ring_recv = take(8)

    n_dev, n_chans, n_tok = u_out.shape
    n_lanes = n_tok // 2
    n_rows = 2 * n_dev
    n_pairs = n_chans // 2
    width = n_dev * n_chans
    rank = lax.axis_index("cp")
    core = lax.rem(rank, 2)
    chip = lax.div(rank, 2)
    coords = (lax.div(chip, 16), lax.rem(lax.div(chip, 4), 4), lax.rem(chip, 4))
    strides = (32, 8, 2)
    peer = rank + 1 - 2 * core

    def remote(src, dst, send, recv, device):
        return pltpu.make_async_remote_copy(src_ref=src, dst_ref=dst, send_sem=send, recv_sem=recv,
                                            device_id={"cp": device}, device_id_type=pl.DeviceIdType.MESH)

    def others(body):
        def step(i, carry):
            body(lax.rem(rank + i, n_dev))
            return carry

        lax.fori_loop(1, n_dev, step, 0)

    barrier = pltpu.get_barrier_semaphore()
    others(lambda dev: pl.semaphore_signal(barrier, inc=1, device_id={"cp": dev}, device_id_type=pl.DeviceIdType.MESH))

    n_slot, per_slot = wide.shape[0], wide.shape[1]
    n_wide = filt_ref.shape[0] // per_slot
    first_lane = pl.multiple_of(lax.div(rank * n_chans, 128) * 128, 128)
    wides = [pltpu.make_async_copy(
        filt_ref.at[pl.ds(i * per_slot, per_slot), pl.ds(first_lane, 128)], wide.at[i % n_slot], wide_sem.at[i])
        for i in range(n_wide)]
    loads = [pltpu.make_async_copy(src, dst, load_sem.at[i]) for i, (src, dst) in enumerate(
        [(win_hbm.at[:, pl.ds(j * width, width)], win_ref.at[:, pl.ds(j * width, width)]) for j in range(3)]
        + [(wout_hbm, wout_ref), (f1_hbm, f1_ref), (f2_hbm, f2_ref), (g2_hbm, g2_ref), (g1_hbm, g1_ref), (tw_hbm, tw_ref)])]
    for copy in [loads[1], loads[2], loads[0]] + loads[3:] + wides[:n_slot]:
        copy.start()

    def act(i):
        return qkv_ref[i * width:(i + 1) * width]

    def project(i):
        loads[i].wait()
        for first in range(i * width, (i + 1) * width, 256):
            qkv_ref[first:first + 256] = dot(x_ref[...], win_ref[:, first:first + 256]).T.astype(BF16)

    project(1)
    project(2)
    u_out[...] = (act(1) * act(2)).reshape(u_out.shape)
    pl.semaphore_wait(barrier, n_dev - 1)

    def exchange(which, src, dst):
        others(lambda dev: remote(src.at[dev], dst.at[rank], ex_send.at[which], ex_recv.at[which], dev).start())
        dst[rank] = src[rank]

    def wait_all(sem, which, ref):
        part = ref.at[pl.ds(0, n_dev - 1)]
        pltpu.make_async_copy(part, part, sem.at[which]).wait()

    exchange(0, u_out, u_in)
    project(0)
    loads[3].wait()
    for first in range(0, width, 256):
        dz_ref[first:first + 256] = lax.dot_general(
            do_ref[...], wout_ref[first:first + 256], (((1,), (1,)), ((), ())), preferred_element_type=F32).T.astype(BF16)
    dy_out[...] = (dz_ref[...] * act(0)).reshape(dy_out.shape)
    exchange(1, dy_out, dy_in)
    n_group = 256 // (2 * n_chans)
    for i in range(width // 256):
        x_own[i * n_group:(i + 1) * n_group] = x_ref[:, i * 256:(i + 1) * 256].astype(F32).T.astype(BF16).reshape(
            n_group, 2, n_chans, n_tok)

    swaps = []

    def swap(src, dst):
        copy = remote(src, dst, swap_send.at[len(swaps)], swap_recv.at[len(swaps)], peer)
        copy.start()
        swaps.append(copy)
        return copy

    x_swap = swap(x_own.at[:, 1 - core], x_peer)
    do_swap = swap(do_ref, do_peer)

    own_row = pl.multiple_of(lax.rem(rank * n_chans, 128), n_chans)
    per_wide = per_slot // n_lanes

    for i in range(n_wide):
        wides[i].wait()

        def turn(j, carry):
            for k in range(4):
                tile = 4 * j + k
                flip[k] = wide[i % n_slot, pl.ds(pl.multiple_of(tile * n_lanes, n_lanes), n_lanes), :].T
                at = pl.multiple_of((i * per_wide + tile) * n_chans, n_chans)
                taps[pl.ds(at, n_chans), :] = flip[k, pl.ds(own_row, n_chans), :]
            return carry

        lax.fori_loop(0, per_wide // 4, turn, 0)
        if i + n_slot < n_wide:
            wides[i + n_slot].start()
    for copy in loads[4:]:
        copy.wait()

    def f1(i):
        return f1_ref[:, i * n_rows:(i + 1) * n_rows]

    def g1(i):
        return g1_ref[:, 2 * i * n_rows:2 * (i + 1) * n_rows]

    def f2(i):
        return f2_ref[2 * i * n_lanes:2 * (i + 1) * n_lanes]

    def g2(i):
        return g2_ref[2 * i * n_lanes:2 * (i + 1) * n_lanes]

    def twist():
        return tw_ref[:, :n_lanes], tw_ref[:, n_lanes:]

    def second(stage):
        wr, wi = twist()
        parts = []
        for i in range(2):
            ar = stage[:n_rows, i * n_lanes:(i + 1) * n_lanes]
            ai = stage[n_rows:, i * n_lanes:(i + 1) * n_lanes]
            parts.append(jnp.concatenate([ar * wr - ai * wi, ar * wi + ai * wr], axis=1))
        bh, bl = halves(jnp.concatenate(parts, axis=0))
        return dot(bh, f2(0)) + (dot(bh, f2(1)) + dot(bl, f2(0)))

    def inverse(pr, pi):
        wr, wi = twist()
        ph, pll = halves(jnp.concatenate([pr, pi], axis=1))
        mid = dot(ph, g2(0)) + (dot(ph, g2(1)) + dot(pll, g2(0)))
        tr, ti = [], []
        for i in range(2):
            gr = mid[i * n_rows:(i + 1) * n_rows, :n_lanes]
            gi = mid[i * n_rows:(i + 1) * n_rows, n_lanes:]
            tr.append(gr * wr + gi * wi)
            ti.append(gi * wr - gr * wi)
        th, tl = halves(jnp.concatenate([jnp.concatenate(tr, axis=1), jnp.concatenate(ti, axis=1)], axis=0))
        return dot(g1(0), th) + (dot(g1(0), tl) + dot(g1(1), th))

    def pairs(body, first=0, last=n_pairs):
        def step(p, carry):
            body(p)
            return carry

        lax.fori_loop(first, last, step, 0)

    def rows_of(ref, chan):
        return jnp.concatenate([ref[0, pl.ds(chan, n_dev, stride=n_chans), :],
                                ref[1, pl.ds(chan, n_dev, stride=n_chans), :]], axis=0)

    def both(ref, p):
        return jnp.concatenate([rows_of(ref, 2 * p), rows_of(ref, 2 * p + 1)], axis=1)

    def widen(src, dst):
        for half in range(2):
            dst[half] = src[:, :, half * n_lanes:(half + 1) * n_lanes].astype(F32).reshape(dst.shape[1:])

    def parts_of(ref, p):
        return ref[p, :, :n_lanes], ref[p, :, n_lanes:]

    def taps_spec(p):
        def one(chan):
            return jnp.concatenate([taps[pl.ds(chan, n_dev, stride=2 * n_chans), :],
                                    taps[pl.ds(n_chans + chan, n_dev, stride=2 * n_chans), :]], axis=0)

        h_hi, h_lo = halves(jnp.concatenate([one(2 * p), one(2 * p + 1)], axis=1))
        h_spec[p] = second(dot(f1(0), h_hi) + (dot(f1(0), h_lo) + dot(f1(1), h_hi)))

    pairs(taps_spec)

    def filtered(sig, spec, sign):
        def one(p):
            val = both(sig, p)
            low = val.astype(BF16)
            spec[p] = second(dot(f1(0), low) + dot(f1(1), low))
            sr, si = parts_of(spec, p)
            hr, hi = parts_of(h_spec, p)
            if sign > 0:
                lin = inverse(sr * hr - si * hi, sr * hi + si * hr)
            else:
                lin = inverse(sr * hr + si * hi, si * hr - sr * hi)
            for i in range(2):
                chan = 2 * p + i
                cols = slice(i * n_lanes, (i + 1) * n_lanes)
                res = lin[:, cols] + skip_ref[rank * n_chans + chan] * val[:, cols]
                for odd in range(2):
                    out_f32[odd, pl.ds(chan, n_dev, stride=n_chans), :] = res[odd * n_dev:(odd + 1) * n_dev]

        pairs(one)

    def narrow(dst):
        for half in range(2):
            dst[:, :, half * n_lanes:(half + 1) * n_lanes] = out_f32[half].astype(BF16).reshape(
                n_dev, n_chans, n_lanes)

    wait_all(ex_recv, 0, u_in)
    widen(u_in, u_f32)
    filtered(u_f32, u_spec, 1)
    narrow(y_out)
    exchange(2, y_out, y_in)
    wait_all(ex_recv, 1, dy_in)
    widen(dy_in, dy_f32)
    filtered(dy_f32, d_spec, -1)
    narrow(du_out)
    exchange(3, du_out, du_in)

    wait_all(ex_recv, 2, y_in)
    y_act = y_in[...].reshape(width, n_tok)
    z_own[...] = (act(0) * y_act).reshape(z_own.shape)
    d_own[0:width] = dz_ref[...] * y_act
    z_swap = swap(z_own.at[:, 1 - core], z_peer)
    d_swaps = [swap(d_own.at[pl.ds(0, width)], d_peer.at[pl.ds(0, width)])]

    def taps_grad(p):
        ur, ui = parts_of(u_spec, p)
        dr, di = parts_of(d_spec, p)
        lin = inverse(dr * ur + di * ui, di * ur - dr * ui)
        prod = both(u_f32, p) * both(dy_f32, p)
        for i in range(2):
            chan = 2 * p + i
            cols = slice(i * n_lanes, (i + 1) * n_lanes)
            gskip_ref[pl.ds(chan, 1), :] = jnp.sum(prod[:, cols], axis=0, keepdims=True)
            for odd in range(2):
                gfilt_ref[pl.ds(odd * n_chans + chan, n_dev, stride=2 * n_chans), :] = lin[
                    odd * n_dev:(odd + 1) * n_dev, cols]

    pairs(taps_grad, 0, n_pairs // 2)

    def at_offset(dim, step):
        pos = lax.rem(coords[dim] + step, RING)
        return pos, rank + (pos - coords[dim]) * strides[dim]

    nxt = [at_offset(dim, 1) for dim in range(3)]
    opp = [at_offset(dim, 2) for dim in range(3)]
    prv = [at_offset(dim, 3) for dim in range(3)]
    cols = part_columns(2 * width)
    half_rows = width // 2

    def mm(a, b, cb):
        return lax.dot_general(a, b, (((1,), (cb,)), ((), ())), preferred_element_type=F32)

    def flat(val):
        return val.reshape(half_rows, n_tok)

    def segments(part):
        lo, hi = cols[part % 3]
        runs = []
        for first, is_out, base in (((0, False, 0), (width, True, 0)) if part < 3 else ((0, False, width),)):
            last = first + width if part < 3 else 2 * width
            a, b = max(lo, first), min(hi, last)
            if a < b:
                runs.append((is_out, base + a - first, a - lo, b - a))
        return runs

    def products(part):
        for is_out, first, place, size in segments(part):
            for off in range(0, size, 512):
                step = min(512, size - off)
                at = first + off
                if is_out:
                    val = (mm(flat(z_own[:, core]), do_ref[:, at:at + step], 0)
                           + mm(flat(z_peer[...]), do_peer[:, at:at + step], 0))
                else:
                    val = (mm(flat(x_own[:, core]), d_own[at:at + step], 1)
                           + mm(flat(x_peer[...]), d_peer[at:at + step], 1))
                partial[part][:, :, :, :, place + off:place + off + step] = val.reshape(
                    RING, RING, RING, n_chans, step)

    def slab(ref, axis, pos, col=None):
        index = [slice(None)] * len(ref.shape)
        if axis is not None:
            index[axis] = pos
        if col is not None:
            index[-1] = pl.ds(*col)
        return ref.at[tuple(index)]

    copies = {}

    def send(part, phase, which, src, dst, device):
        slot = (phase * 6 + part) * 6 + which
        copy = remote(src, dst, ring_send.at[slot], ring_recv.at[slot], device)
        copy.start()
        copies[part, phase, which] = copy

    def setting(part, phase):
        order = PART_ORDERS[(part + part // 3) % 3]
        dim = order[phase]
        axis = sorted(order[phase:]).index(dim)
        src = partial[part] if phase == 0 else reds[phase - 1][part]
        size = src.shape[-1]
        first = (size // 128 + 1) // 2 * 128
        return dim, axis, src, vias[phase][part], fins[phase][part], (0, first), (first, size - first)

    def launch(part, phase):
        dim, axis, src, via, fin, a_cols, b_cols = setting(part, phase)
        send(part, phase, 0, slab(src, axis, opp[dim][0], a_cols), slab(via, None, None, a_cols), nxt[dim][1])
        send(part, phase, 1, slab(src, axis, opp[dim][0], b_cols), slab(via, None, None, b_cols), prv[dim][1])
        send(part, phase, 2, slab(src, axis, nxt[dim][0], b_cols), slab(fin, 0, 0, b_cols), nxt[dim][1])
        send(part, phase, 3, slab(src, axis, prv[dim][0], a_cols), slab(fin, 0, 1, a_cols), prv[dim][1])

    def each_block(shape, body):
        lead = shape[:-2]
        count = int(np.prod(lead)) if lead else 1
        if count == 1:
            body(tuple(0 for _ in lead))
            return

        def step(i, carry):
            index = []
            for size in reversed(lead):
                index.insert(0, lax.rem(i, size))
                i = lax.div(i, size)
            body(tuple(index))
            return carry

        lax.fori_loop(0, count, step, 0, unroll=min(count, 4))

    def relay(part, phase):
        dim, axis, src, via, fin, a_cols, b_cols = setting(part, phase)
        for which, col, spot, side in ((0, a_cols, nxt[dim], 0), (1, b_cols, prv[dim], 1)):
            copies[part, phase, which].wait_recv()
            span = pl.ds(*col)

            def add(index):
                at = index[:axis] + (spot[0],) + index[axis:]
                src[at + (slice(None), span)] = src[at + (slice(None), span)] + via[index + (slice(None), span)]

            each_block(via.shape, add)
            send(part, phase, 4 + which, slab(src, axis, spot[0], col), slab(fin, 0, side, col), spot[1])

    def finish(part, phase):
        dim, axis, src, via, fin, _, _ = setting(part, phase)
        for which in range(2, 6):
            copies[part, phase, which].wait_recv()

        def add(index):
            at = index[:axis] + (coords[dim],) + index[axis:]
            total = src[at] + fin[(0,) + index] + fin[(1,) + index]
            if phase < 2:
                reds[phase][part][index] = total
                return
            for is_out, first, place, size in segments(part):
                dst = gwout_ref if is_out else gwin_ref
                dst[:, first:first + size] = total[:, place:place + size].astype(dst.dtype)

        each_block(via.shape, add)
        if phase < 2:
            launch(part, phase + 1)

    early, late = (0, 1, 2), (3, 4, 5)
    for copy in (x_swap, do_swap, z_swap, d_swaps[0]):
        copy.wait_recv()
    for part in early:
        products(part)
        launch(part, 0)

    pairs(taps_grad, n_pairs // 2, n_pairs)
    wait_all(ex_recv, 3, du_in)
    du_act = du_in[...].reshape(width, n_tok)
    for i in (1, 2):
        d_own[i * width:(i + 1) * width] = du_act * act(3 - i)
        span = pl.ds(i * width, width)
        d_swaps.append(swap(d_own.at[span], d_peer.at[span]))

    def run(step, parts, phase):
        for part in parts:
            step(part, phase)

    run(relay, early, 0)
    for copy in d_swaps[1:]:
        copy.wait_recv()
    for part in late:
        products(part)
        launch(part, 0)

    for first in range(0, width, 256):
        gx_ref[:, first:first + 256] = dot(win_ref[first:first + 256], d_own[...]).T.astype(gx_ref.dtype)

    run(finish, early, 0)
    run(relay, late, 0)
    run(relay, early, 1)
    run(finish, early, 1)
    run(finish, late, 0)
    run(relay, early, 2)
    run(finish, early, 2)
    run(relay, late, 1)
    run(finish, late, 1)
    run(relay, late, 2)
    run(finish, late, 2)
    for which, ref in enumerate((u_out, dy_out, y_out, du_out)):
        wait_all(ex_send, which, ref)
    for copy in list(copies.values()) + swaps:
        copy.wait_send()


def hyena_grads(x_tok, d_out, filt_taps, skip_gain, w_in, w_out, n_dev):
    n_tok, width = x_tok.shape
    n_chans, n_chip = width // n_dev, n_dev // 2
    n_lanes, n_rows = n_tok // 2, 2 * n_dev
    n_taps = filt_taps.shape[0]
    n_wide, n_slot = 16, 3
    tables = [jnp.asarray(tab) for tab in transform_tables(n_rows, n_lanes)]
    vmem = pl.BlockSpec(memory_space=pltpu.VMEM)
    hbm = pl.BlockSpec(memory_space=pl.ANY)
    widths = [hi - lo for lo, hi in part_columns(2 * width)] * 2
    pairs = pltpu.VMEM((n_chip, 2, n_chans, n_tok), BF16)
    single = pltpu.VMEM((n_chip, n_chans, n_tok), BF16)
    stack = pltpu.VMEM((3 * width, n_tok), BF16)
    scratch = [pltpu.VMEM((n_dev, n_chans, n_tok), BF16)] * 6
    scratch += [pltpu.VMEM((2, width, n_lanes), F32)] * 3
    scratch += [pltpu.VMEM((n_slot, n_taps // n_wide, 128), F32), pltpu.VMEM((4, 128, n_lanes), F32),
                pltpu.VMEM((n_rows * n_chans, n_lanes), F32)]
    scratch += [pltpu.VMEM((n_chans // 2, 2 * n_rows, 2 * n_lanes), F32)] * 3
    scratch += [pltpu.VMEM(arr.shape, arr.dtype) for arr in tables + [w_in, w_out]]
    scratch += [stack, pltpu.VMEM((width, n_tok), BF16)]
    scratch += [pairs, pairs, stack, single, single, stack, pltpu.VMEM(d_out.shape, BF16)]
    scratch += [pltpu.VMEM((RING,) * 3 + (n_chans, w), F32) for w in widths]
    for n_lead in (2, 1, 0):
        lead = (RING,) * n_lead
        scratch += [pltpu.VMEM(lead + (n_chans, w), F32) for w in widths]
        scratch += [pltpu.VMEM((2,) + lead + (n_chans, w), F32) for w in widths]
        if n_lead:
            scratch += [pltpu.VMEM(lead + (n_chans, w), F32) for w in widths]
    scratch += [pltpu.SemaphoreType.DMA((n,)) for n in (len(tables) + 4, n_wide, 4, 4, 6, 6, 108, 108)]
    return pl.pallas_call(
        hyena_kernel,
        out_shape=(
            jax.ShapeDtypeStruct((n_tok, width), BF16),
            jax.ShapeDtypeStruct((n_chans, 3 * width), BF16),
            jax.ShapeDtypeStruct((n_chans, width), BF16),
            jax.ShapeDtypeStruct((n_rows * n_chans, n_lanes), F32),
            jax.ShapeDtypeStruct((n_chans, n_lanes), F32),
        ),
        in_specs=[vmem] * 2 + [hbm, pl.BlockSpec(memory_space=pltpu.SMEM)] + [hbm] * 7,
        out_specs=(vmem,) * 5,
        scratch_shapes=scratch,
        compiler_params=pltpu.CompilerParams(vmem_limit_bytes=56 * 2 ** 20, collective_id=0, has_side_effects=True),
        cost_estimate=pl.CostEstimate(flops=2 * 10 ** 10, bytes_accessed=32 * 2 ** 20, transcendentals=0),
        name="hyena_grads",
    )(x_tok, d_out, filt_taps, skip_gain, w_in, w_out, *tables)


def solution(mesh):
    ctx_size = mesh.shape["cp"]

    def local_step(x_seq, w_in, w_out, filt_taps, skip_gain, d_out):
        n_batch, n_tok, width = x_seq.shape
        n_chans = width // ctx_size
        seq_len = n_tok * ctx_size
        n_lanes = n_tok // 2
        x_tok, do_tok = x_seq[0], d_out[0]

        grad_x, grad_w_in, grad_w_out, gfilt, gskip = hyena_grads(
            x_tok, do_tok, filt_taps, skip_gain, w_in, w_out, ctx_size)
        grad_filt = gfilt.reshape(seq_len // n_lanes, n_chans, n_lanes).transpose(0, 2, 1).reshape(seq_len, n_chans)
        return grad_x[None], grad_w_in, grad_w_out, grad_filt, jnp.sum(gskip, axis=1)

    seq_spec = P("dp", "cp", None)
    row_spec = P(("dp", "cp"), None)
    return jax.shard_map(
        local_step,
        mesh=mesh,
        in_specs=(seq_spec, P(), P(), P(), P(), seq_spec),
        out_specs=(seq_spec, row_spec, row_spec, P("dp", "cp"), P(("dp", "cp"))),
        check_vma=False,
    )
```

```python
import functools

import jax
import jax.numpy as jnp
import numpy as np
from jax import lax
from jax.experimental import pallas as pl
from jax.experimental.pallas import tpu as pltpu
from jax.sharding import PartitionSpec as P

F32, BF16 = jnp.float32, jnp.bfloat16


def split_const(mat):
    hi = mat.astype(np.float32).astype(jnp.bfloat16)
    lo = (mat - hi.astype(np.float64)).astype(np.float32).astype(jnp.bfloat16)
    return hi, lo


@functools.lru_cache(None)
def transform_tables(n_rows, n_lanes):
    n = n_rows * n_lanes
    t1 = np.concatenate([np.arange(0, n_rows, 2), np.arange(1, n_rows, 2)])
    k1 = np.arange(n_rows)
    ang = 2 * np.pi * np.outer(k1 + 0.25, t1) / n_rows
    f1 = np.concatenate([np.cos(ang), -np.sin(ang)], axis=0)
    g1 = f1.T / n
    t2 = np.arange(n_lanes)
    psi = 2 * np.pi * (np.outer(t2, t2) % n_lanes) / n_lanes
    cos2, sin2 = np.cos(psi), np.sin(psi)
    f2 = np.block([[cos2, -sin2], [sin2, cos2]])
    g2 = f2.T
    twist = 2 * np.pi * np.outer(k1 + 0.25, t2) / n
    twid = np.concatenate([np.cos(twist), -np.sin(twist)], axis=1).astype(np.float32)
    f1h, f1l = split_const(f1)
    g1h, g1l = split_const(g1)
    f2h, f2l = split_const(f2)
    g2h, g2l = split_const(g2)
    return (
        np.concatenate([f1h, f1l], axis=1),
        np.concatenate([f2h, f2l], axis=0),
        np.concatenate([g2h, g2l], axis=0),
        np.concatenate([g1h, g1l], axis=1),
        twid,
    )


def dot(a, b):
    return jnp.dot(a, b, preferred_element_type=F32)


def halves(val):
    hi = val.astype(BF16)
    lo = (val - hi.astype(F32)).astype(BF16)
    return hi, lo


RING = 4
PART_ORDERS = ((0, 1, 2), (1, 2, 0), (2, 0, 1))


def part_columns(total):
    tiles = total // 128
    ends = [0, (tiles + 2) // 3 * 128, ((tiles + 2) // 3 + (tiles + 1) // 3) * 128, total]
    return [(ends[i], ends[i + 1]) for i in range(3)]


def all_columns(width):
    cut = (2 * width // 128 * 5 + 7) // 8 * 128
    return (part_columns(2 * width) + part_columns(cut)
            + [(cut + lo, cut + hi) for lo, hi in part_columns(2 * width - cut)])


def result_kernel(*refs):
    for src, dst in zip(refs[:4], refs[5:9]):
        dst[...] = src[...]
    refs[9][...] = jnp.sum(refs[4][...].T, axis=0)


def results(*vals):
    vmem = pl.BlockSpec(memory_space=pltpu.VMEM)
    n_chans = vals[4].shape[0]
    return pl.pallas_call(
        result_kernel,
        out_shape=tuple(jax.ShapeDtypeStruct(val.shape, val.dtype) for val in vals[:4])
        + (jax.ShapeDtypeStruct((n_chans,), F32),),
        in_specs=[vmem] * 5,
        out_specs=(vmem,) * 5,
        cost_estimate=pl.CostEstimate(flops=10 ** 6, bytes_accessed=4 * 2 ** 20, transcendentals=0),
        name="results",
    )(*vals)


def hyena_kernel(x_ref, do_ref, filt_ref, skip_ref, win_hbm, wout_hbm, f1_hbm, f2_hbm, g2_hbm, g1_hbm, tw_hbm,
                 gx_ref, gwin_ref, gwout_ref, gfilt_ref, gskip_ref, *scratch):
    names = iter(scratch)

    def take(count):
        return [next(names) for _ in range(count)]

    u_out, dy_out, u_in, dy_in, y_in, du_in = take(6)
    y_out, du_out = u_in, dy_in
    u_f32, dy_f32, out_f32 = take(3)
    wide, flip, taps = take(3)
    u_spec, h_spec, d_spec = take(3)
    f1_ref, f2_ref, g2_ref, g1_ref, tw_ref, win_ref, wout_ref = take(7)
    qkv_ref, dz_ref = take(2)
    x_own, z_own, d_own, x_peer, z_peer, d_peer, do_peer = take(7)
    partial = take(9)
    vias, fins, reds = [], [], []
    for phase in range(3):
        vias.append(take(9))
        fins.append(take(9))
        if phase < 2:
            reds.append(take(9))
    load_sem, wide_sem, ex_send, ex_recv, swap_send, swap_recv, ring_send, ring_recv = take(8)

    n_dev, n_chans, n_tok = u_out.shape
    n_lanes = n_tok // 2
    n_rows = 2 * n_dev
    n_pairs = n_chans // 2
    width = n_dev * n_chans
    rank = lax.axis_index("cp")
    core = lax.rem(rank, 2)
    chip = lax.div(rank, 2)
    coords = (lax.div(chip, 16), lax.rem(lax.div(chip, 4), 4), lax.rem(chip, 4))
    strides = (32, 8, 2)
    peer = rank + 1 - 2 * core

    def remote(src, dst, send, recv, device):
        return pltpu.make_async_remote_copy(src_ref=src, dst_ref=dst, send_sem=send, recv_sem=recv,
                                            device_id={"cp": device}, device_id_type=pl.DeviceIdType.MESH)

    def others(body):
        body(lax.rem(rank + 1, n_dev))

        def step(i, carry):
            for k in range(7):
                body(lax.rem(rank + 2 + 7 * i + k, n_dev))
            return carry

        lax.fori_loop(0, (n_dev - 2) // 7, step, 0)

    barrier = pltpu.get_barrier_semaphore()
    others(lambda dev: pl.semaphore_signal(barrier, inc=1, device_id={"cp": dev}, device_id_type=pl.DeviceIdType.MESH))

    n_slot, per_slot = wide.shape[0], wide.shape[1]
    n_wide = filt_ref.shape[0] // per_slot
    first_lane = pl.multiple_of(lax.div(rank * n_chans, 128) * 128, 128)
    wides = [pltpu.make_async_copy(
        filt_ref.at[pl.ds(i * per_slot, per_slot), pl.ds(first_lane, 128)], wide.at[i % n_slot], wide_sem.at[i])
        for i in range(n_wide)]
    loads = [pltpu.make_async_copy(src, dst, load_sem.at[i]) for i, (src, dst) in enumerate(
        [(win_hbm.at[:, pl.ds(j * width, width)], win_ref.at[:, pl.ds(j * width, width)]) for j in range(3)]
        + [(wout_hbm, wout_ref), (f1_hbm, f1_ref), (f2_hbm, f2_ref), (g2_hbm, g2_ref), (g1_hbm, g1_ref), (tw_hbm, tw_ref)])]
    for copy in [loads[1], loads[2], loads[0]] + loads[3:] + wides[:n_slot]:
        copy.start()

    def act(i):
        return qkv_ref[i * width:(i + 1) * width]

    def project(i):
        loads[i].wait()
        for first in range(i * width, (i + 1) * width, 256):
            qkv_ref[first:first + 256] = dot(x_ref[...], win_ref[:, first:first + 256]).T.astype(BF16)

    project(1)
    project(2)
    u_out[...] = (act(1) * act(2)).reshape(u_out.shape)
    pl.semaphore_wait(barrier, n_dev - 1)

    def exchange(which, src, dst):
        others(lambda dev: remote(src.at[dev], dst.at[rank], ex_send.at[which], ex_recv.at[which], dev).start())
        dst[rank] = src[rank]

    def wait_all(sem, which, ref):
        part = ref.at[pl.ds(0, n_dev - 1)]
        pltpu.make_async_copy(part, part, sem.at[which]).wait()

    exchange(0, u_out, u_in)
    project(0)
    loads[3].wait()
    for first in range(0, width, 256):
        dz_ref[first:first + 256] = lax.dot_general(
            do_ref[...], wout_ref[first:first + 256], (((1,), (1,)), ((), ())), preferred_element_type=F32).T.astype(BF16)
    dy_out[...] = (dz_ref[...] * act(0)).reshape(dy_out.shape)
    exchange(1, dy_out, dy_in)
    n_group = 256 // (2 * n_chans)
    for i in range(width // 256):
        x_own[i * n_group:(i + 1) * n_group] = x_ref[:, i * 256:(i + 1) * 256].astype(F32).T.astype(BF16).reshape(
            n_group, 2, n_chans, n_tok)

    swaps = []

    def swap(src, dst):
        copy = remote(src, dst, swap_send.at[len(swaps)], swap_recv.at[len(swaps)], peer)
        copy.start()
        swaps.append(copy)
        return copy

    x_swap = swap(x_own.at[:, 1 - core], x_peer)
    do_swap = swap(do_ref, do_peer)

    own_row = pl.multiple_of(lax.rem(rank * n_chans, 128), n_chans)
    per_wide = per_slot // n_lanes

    for i in range(n_wide):
        wides[i].wait()

        def turn(j, carry):
            for k in range(4):
                tile = 4 * j + k
                flip[k] = wide[i % n_slot, pl.ds(pl.multiple_of(tile * n_lanes, n_lanes), n_lanes), :].T
                at = pl.multiple_of((i * per_wide + tile) * n_chans, n_chans)
                taps[pl.ds(at, n_chans), :] = flip[k, pl.ds(own_row, n_chans), :]
            return carry

        lax.fori_loop(0, per_wide // 4, turn, 0)
        if i + n_slot < n_wide:
            wides[i + n_slot].start()
    for copy in loads[4:]:
        copy.wait()

    def f1(i):
        return f1_ref[:, i * n_rows:(i + 1) * n_rows]

    def g1(i):
        return g1_ref[:, 2 * i * n_rows:2 * (i + 1) * n_rows]

    def f2(i):
        return f2_ref[2 * i * n_lanes:2 * (i + 1) * n_lanes]

    def g2(i):
        return g2_ref[2 * i * n_lanes:2 * (i + 1) * n_lanes]

    def twist():
        return tw_ref[:, :n_lanes], tw_ref[:, n_lanes:]

    def second(stage):
        wr, wi = twist()
        parts = []
        for i in range(2):
            ar = stage[:n_rows, i * n_lanes:(i + 1) * n_lanes]
            ai = stage[n_rows:, i * n_lanes:(i + 1) * n_lanes]
            parts.append(jnp.concatenate([ar * wr - ai * wi, ar * wi + ai * wr], axis=1))
        bh, bl = halves(jnp.concatenate(parts, axis=0))
        return dot(bh, f2(0)) + (dot(bh, f2(1)) + dot(bl, f2(0)))

    def inverse(pr, pi):
        wr, wi = twist()
        ph, pll = halves(jnp.concatenate([pr, pi], axis=1))
        mid = dot(ph, g2(0)) + (dot(ph, g2(1)) + dot(pll, g2(0)))
        tr, ti = [], []
        for i in range(2):
            gr = mid[i * n_rows:(i + 1) * n_rows, :n_lanes]
            gi = mid[i * n_rows:(i + 1) * n_rows, n_lanes:]
            tr.append(gr * wr + gi * wi)
            ti.append(gi * wr - gr * wi)
        th, tl = halves(jnp.concatenate([jnp.concatenate(tr, axis=1), jnp.concatenate(ti, axis=1)], axis=0))
        return dot(g1(0), th) + (dot(g1(0), tl) + dot(g1(1), th))

    def pairs(body, first=0, last=n_pairs):
        def step(p, carry):
            body(p)
            return carry

        lax.fori_loop(first, last, step, 0)

    def rows_of(ref, chan):
        return jnp.concatenate([ref[0, pl.ds(chan, n_dev, stride=n_chans), :],
                                ref[1, pl.ds(chan, n_dev, stride=n_chans), :]], axis=0)

    def both(ref, p):
        return jnp.concatenate([rows_of(ref, 2 * p), rows_of(ref, 2 * p + 1)], axis=1)

    def widen(src, dst):
        for half in range(2):
            dst[half] = src[:, :, half * n_lanes:(half + 1) * n_lanes].astype(F32).reshape(dst.shape[1:])

    def parts_of(ref, p):
        return ref[p, :, :n_lanes], ref[p, :, n_lanes:]

    def taps_spec(p):
        def one(chan):
            return jnp.concatenate([taps[pl.ds(chan, n_dev, stride=2 * n_chans), :],
                                    taps[pl.ds(n_chans + chan, n_dev, stride=2 * n_chans), :]], axis=0)

        h_hi, h_lo = halves(jnp.concatenate([one(2 * p), one(2 * p + 1)], axis=1))
        h_spec[p] = second(dot(f1(0), h_hi) + (dot(f1(0), h_lo) + dot(f1(1), h_hi)))

    pairs(taps_spec)

    def filtered(sig, spec, sign):
        def one(p):
            val = both(sig, p)
            low = val.astype(BF16)
            spec[p] = second(dot(f1(0), low) + dot(f1(1), low))
            sr, si = parts_of(spec, p)
            hr, hi = parts_of(h_spec, p)
            if sign > 0:
                lin = inverse(sr * hr - si * hi, sr * hi + si * hr)
            else:
                lin = inverse(sr * hr + si * hi, si * hr - sr * hi)
            for i in range(2):
                chan = 2 * p + i
                cols = slice(i * n_lanes, (i + 1) * n_lanes)
                res = lin[:, cols] + skip_ref[rank * n_chans + chan] * val[:, cols]
                for odd in range(2):
                    out_f32[odd, pl.ds(chan, n_dev, stride=n_chans), :] = res[odd * n_dev:(odd + 1) * n_dev]

        pairs(one)

    def narrow(dst):
        for half in range(2):
            dst[:, :, half * n_lanes:(half + 1) * n_lanes] = out_f32[half].astype(BF16).reshape(
                n_dev, n_chans, n_lanes)

    wait_all(ex_recv, 0, u_in)
    widen(u_in, u_f32)
    filtered(u_f32, u_spec, 1)
    narrow(y_out)
    exchange(2, y_out, y_in)
    wait_all(ex_recv, 1, dy_in)
    widen(dy_in, dy_f32)
    filtered(dy_f32, d_spec, -1)
    narrow(du_out)
    exchange(3, du_out, du_in)

    wait_all(ex_recv, 2, y_in)
    y_act = y_in[...].reshape(width, n_tok)
    z_own[...] = (act(0) * y_act).reshape(z_own.shape)
    d_own[0:width] = dz_ref[...] * y_act
    z_swap = swap(z_own.at[:, 1 - core], z_peer)
    d_swaps = [swap(d_own.at[pl.ds(0, width)], d_peer.at[pl.ds(0, width)])]

    def taps_grad(p):
        ur, ui = parts_of(u_spec, p)
        dr, di = parts_of(d_spec, p)
        lin = inverse(dr * ur + di * ui, di * ur - dr * ui)
        prod = both(u_f32, p) * both(dy_f32, p)
        for i in range(2):
            chan = 2 * p + i
            cols = slice(i * n_lanes, (i + 1) * n_lanes)
            gskip_ref[pl.ds(chan, 1), :] = jnp.sum(prod[:, cols], axis=0, keepdims=True)
            for odd in range(2):
                gfilt_ref[pl.ds(odd * n_chans + chan, n_dev, stride=2 * n_chans), :] = lin[
                    odd * n_dev:(odd + 1) * n_dev, cols]

    pairs(taps_grad, 0, n_pairs // 2)

    def at_offset(dim, step):
        pos = lax.rem(coords[dim] + step, RING)
        return pos, rank + (pos - coords[dim]) * strides[dim]

    nxt = [at_offset(dim, 1) for dim in range(3)]
    opp = [at_offset(dim, 2) for dim in range(3)]
    prv = [at_offset(dim, 3) for dim in range(3)]
    cols = all_columns(width)
    half_rows = width // 2

    def mm(a, b, cb):
        return lax.dot_general(a, b, (((1,), (cb,)), ((), ())), preferred_element_type=F32)

    def flat(val):
        return val.reshape(half_rows, n_tok)

    def segments(part):
        lo, hi = cols[part]
        runs = []
        for first, is_out, base in (((0, False, 0), (width, True, 0)) if part < 3 else ((0, False, width),)):
            last = first + width if part < 3 else 2 * width
            a, b = max(lo, first), min(hi, last)
            if a < b:
                runs.append((is_out, base + a - first, a - lo, b - a))
        return runs

    def products(part):
        for is_out, first, place, size in segments(part):
            for off in range(0, size, 512):
                step = min(512, size - off)
                at = first + off
                if is_out:
                    val = (mm(flat(z_own[:, core]), do_ref[:, at:at + step], 0)
                           + mm(flat(z_peer[...]), do_peer[:, at:at + step], 0))
                else:
                    val = (mm(flat(x_own[:, core]), d_own[at:at + step], 1)
                           + mm(flat(x_peer[...]), d_peer[at:at + step], 1))
                partial[part][:, :, :, :, place + off:place + off + step] = val.reshape(
                    RING, RING, RING, n_chans, step)

    def slab(ref, axis, pos, col=None):
        index = [slice(None)] * len(ref.shape)
        if axis is not None:
            index[axis] = pos
        if col is not None:
            index[-1] = pl.ds(*col)
        return ref.at[tuple(index)]

    copies = {}

    def send(part, phase, which, src, dst, device):
        slot = (phase * 9 + part) * 6 + which
        copy = remote(src, dst, ring_send.at[slot], ring_recv.at[slot], device)
        copy.start()
        copies[part, phase, which] = copy

    def setting(part, phase):
        order = PART_ORDERS[(part + part // 3) % 3]
        dim = order[phase]
        axis = sorted(order[phase:]).index(dim)
        src = partial[part] if phase == 0 else reds[phase - 1][part]
        size = src.shape[-1]
        first = (size // 128 + 1) // 2 * 128
        return dim, axis, src, vias[phase][part], fins[phase][part], (0, first), (first, size - first)

    def launch(part, phase):
        dim, axis, src, via, fin, a_cols, b_cols = setting(part, phase)
        send(part, phase, 0, slab(src, axis, opp[dim][0], a_cols), slab(via, None, None, a_cols), nxt[dim][1])
        send(part, phase, 1, slab(src, axis, opp[dim][0], b_cols), slab(via, None, None, b_cols), prv[dim][1])
        send(part, phase, 2, slab(src, axis, nxt[dim][0], b_cols), slab(fin, 0, 0, b_cols), nxt[dim][1])
        send(part, phase, 3, slab(src, axis, prv[dim][0], a_cols), slab(fin, 0, 1, a_cols), prv[dim][1])

    def each_block(shape, body):
        lead = shape[:-2]
        count = int(np.prod(lead)) if lead else 1
        if count == 1:
            body(tuple(0 for _ in lead))
            return

        def step(i, carry):
            index = []
            for size in reversed(lead):
                index.insert(0, lax.rem(i, size))
                i = lax.div(i, size)
            body(tuple(index))
            return carry

        lax.fori_loop(0, count, step, 0, unroll=min(count, 4))

    def relay(part, phase):
        dim, axis, src, via, fin, a_cols, b_cols = setting(part, phase)
        for which, col, spot, side in ((0, a_cols, nxt[dim], 0), (1, b_cols, prv[dim], 1)):
            copies[part, phase, which].wait_recv()
            span = pl.ds(*col)

            def add(index):
                at = index[:axis] + (spot[0],) + index[axis:]
                src[at + (slice(None), span)] = src[at + (slice(None), span)] + via[index + (slice(None), span)]

            each_block(via.shape, add)
            send(part, phase, 4 + which, slab(src, axis, spot[0], col), slab(fin, 0, side, col), spot[1])

    def finish(part, phase):
        dim, axis, src, via, fin, _, _ = setting(part, phase)
        for which in range(2, 6):
            copies[part, phase, which].wait_recv()

        def add(index):
            at = index[:axis] + (coords[dim],) + index[axis:]
            total = src[at] + fin[(0,) + index] + fin[(1,) + index]
            if phase < 2:
                reds[phase][part][index] = total
                return
            for is_out, first, place, size in segments(part):
                dst = gwout_ref if is_out else gwin_ref
                dst[:, first:first + size] = total[:, place:place + size].astype(dst.dtype)

        each_block(via.shape, add)
        if phase < 2:
            launch(part, phase + 1)

    early, late, last = (0, 1, 2), (3, 4, 5), (6, 7, 8)
    for copy in (x_swap, do_swap, z_swap, d_swaps[0]):
        copy.wait_recv()
    for part in early:
        products(part)
        launch(part, 0)

    pairs(taps_grad, n_pairs // 2, n_pairs)
    wait_all(ex_recv, 3, du_in)
    du_act = du_in[...].reshape(width, n_tok)
    for i in (1, 2):
        d_own[i * width:(i + 1) * width] = du_act * act(3 - i)
        span = pl.ds(i * width, width)
        d_swaps.append(swap(d_own.at[span], d_peer.at[span]))

    def run(step, parts, phase):
        for part in parts:
            step(part, phase)

    run(relay, early, 0)
    for copy in d_swaps[1:]:
        copy.wait_recv()
    for part in late:
        products(part)
        launch(part, 0)
    for part in last:
        products(part)

    for first in range(0, width, 256):
        gx_ref[:, first:first + 256] = dot(win_ref[first:first + 256], d_own[...]).T.astype(gx_ref.dtype)

    run(finish, early, 0)
    run(relay, late, 0)
    run(launch, last, 0)
    run(relay, early, 1)
    run(finish, early, 1)
    run(finish, late, 0)
    run(relay, last, 0)
    run(relay, early, 2)
    run(finish, early, 2)
    run(relay, late, 1)
    run(finish, late, 1)
    run(finish, last, 0)
    run(relay, late, 2)
    run(finish, late, 2)
    run(relay, last, 1)
    run(finish, last, 1)
    run(relay, last, 2)
    run(finish, last, 2)
    for which, ref in enumerate((u_out, dy_out, y_out, du_out)):
        wait_all(ex_send, which, ref)
    for copy in list(copies.values()) + swaps:
        copy.wait_send()


def hyena_grads(x_tok, d_out, filt_taps, skip_gain, w_in, w_out, n_dev):
    n_tok, width = x_tok.shape
    n_chans, n_chip = width // n_dev, n_dev // 2
    n_lanes, n_rows = n_tok // 2, 2 * n_dev
    n_taps = filt_taps.shape[0]
    n_wide, n_slot = 16, 3
    tables = [jnp.asarray(tab) for tab in transform_tables(n_rows, n_lanes)]
    vmem = pl.BlockSpec(memory_space=pltpu.VMEM)
    hbm = pl.BlockSpec(memory_space=pl.ANY)
    widths = [hi - lo for lo, hi in all_columns(width)]
    pairs = pltpu.VMEM((n_chip, 2, n_chans, n_tok), BF16)
    single = pltpu.VMEM((n_chip, n_chans, n_tok), BF16)
    stack = pltpu.VMEM((3 * width, n_tok), BF16)
    scratch = [pltpu.VMEM((n_dev, n_chans, n_tok), BF16)] * 6
    scratch += [pltpu.VMEM((2, width, n_lanes), F32)] * 3
    scratch += [pltpu.VMEM((n_slot, n_taps // n_wide, 128), F32), pltpu.VMEM((4, 128, n_lanes), F32),
                pltpu.VMEM((n_rows * n_chans, n_lanes), F32)]
    scratch += [pltpu.VMEM((n_chans // 2, 2 * n_rows, 2 * n_lanes), F32)] * 3
    scratch += [pltpu.VMEM(arr.shape, arr.dtype) for arr in tables + [w_in, w_out]]
    scratch += [stack, pltpu.VMEM((width, n_tok), BF16)]
    scratch += [pairs, pairs, stack, single, single, stack, pltpu.VMEM(d_out.shape, BF16)]
    scratch += [pltpu.VMEM((RING,) * 3 + (n_chans, w), F32) for w in widths]
    for n_lead in (2, 1, 0):
        lead = (RING,) * n_lead
        scratch += [pltpu.VMEM(lead + (n_chans, w), F32) for w in widths]
        scratch += [pltpu.VMEM((2,) + lead + (n_chans, w), F32) for w in widths]
        if n_lead:
            scratch += [pltpu.VMEM(lead + (n_chans, w), F32) for w in widths]
    scratch += [pltpu.SemaphoreType.DMA((n,)) for n in (len(tables) + 4, n_wide, 4, 4, 6, 6, 162, 162)]
    return pl.pallas_call(
        hyena_kernel,
        out_shape=(
            jax.ShapeDtypeStruct((n_tok, width), BF16),
            jax.ShapeDtypeStruct((n_chans, 3 * width), BF16),
            jax.ShapeDtypeStruct((n_chans, width), BF16),
            jax.ShapeDtypeStruct((n_rows * n_chans, n_lanes), F32),
            jax.ShapeDtypeStruct((n_chans, n_lanes), F32),
        ),
        in_specs=[vmem] * 2 + [hbm, pl.BlockSpec(memory_space=pltpu.SMEM)] + [hbm] * 7,
        out_specs=(vmem,) * 5,
        scratch_shapes=scratch,
        compiler_params=pltpu.CompilerParams(vmem_limit_bytes=57 * 2 ** 20, collective_id=0, has_side_effects=True),
        cost_estimate=pl.CostEstimate(flops=2 * 10 ** 10, bytes_accessed=32 * 2 ** 20, transcendentals=0),
        name="hyena_grads",
    )(x_tok, d_out, filt_taps, skip_gain, w_in, w_out, *tables)


def solution(mesh):
    ctx_size = mesh.shape["cp"]

    def local_step(x_seq, w_in, w_out, filt_taps, skip_gain, d_out):
        n_batch, n_tok, width = x_seq.shape
        n_chans = width // ctx_size
        seq_len = n_tok * ctx_size
        n_lanes = n_tok // 2
        x_tok, do_tok = x_seq[0], d_out[0]

        grad_x, grad_w_in, grad_w_out, gfilt, grad_skip = results(*hyena_grads(
            x_tok, do_tok, filt_taps, skip_gain, w_in, w_out, ctx_size))
        grad_filt = gfilt.reshape(seq_len // n_lanes, n_chans, n_lanes).transpose(0, 2, 1).reshape(seq_len, n_chans)
        return grad_x[None], grad_w_in, grad_w_out, grad_filt, grad_skip

    seq_spec = P("dp", "cp", None)
    row_spec = P(("dp", "cp"), None)
    return jax.shard_map(
        local_step,
        mesh=mesh,
        in_specs=(seq_spec, P(), P(), P(), P(), seq_spec),
        out_specs=(seq_spec, row_spec, row_spec, P("dp", "cp"), P(("dp", "cp"))),
        check_vma=False,
    )
```

```python
import functools

import jax
import jax.numpy as jnp
import numpy as np
from jax import lax
from jax.experimental import pallas as pl
from jax.experimental.pallas import tpu as pltpu
from jax.sharding import PartitionSpec as P

F32, BF16 = jnp.float32, jnp.bfloat16


def split_const(mat):
    hi = mat.astype(np.float32).astype(jnp.bfloat16)
    lo = (mat - hi.astype(np.float64)).astype(np.float32).astype(jnp.bfloat16)
    return hi, lo


@functools.lru_cache(None)
def transform_tables(n_rows, n_lanes):
    n = n_rows * n_lanes
    t1 = np.concatenate([np.arange(0, n_rows, 2), np.arange(1, n_rows, 2)])
    k1 = np.arange(n_rows)
    ang = 2 * np.pi * np.outer(k1 + 0.25, t1) / n_rows
    f1 = np.concatenate([np.cos(ang), -np.sin(ang)], axis=0)
    g1 = f1.T / n
    t2 = np.arange(n_lanes)
    psi = 2 * np.pi * (np.outer(t2, t2) % n_lanes) / n_lanes
    cos2, sin2 = np.cos(psi), np.sin(psi)
    f2 = np.block([[cos2, -sin2], [sin2, cos2]])
    g2 = f2.T
    twist = 2 * np.pi * np.outer(k1 + 0.25, t2) / n
    twid = np.concatenate([np.cos(twist), -np.sin(twist)], axis=1).astype(np.float32)
    f1h, f1l = split_const(f1)
    g1h, g1l = split_const(g1)
    f2h, f2l = split_const(f2)
    g2h, g2l = split_const(g2)
    return (
        np.concatenate([f1h, f1l], axis=1),
        np.concatenate([f2h, f2l], axis=0),
        np.concatenate([g2h, g2l], axis=0),
        np.concatenate([g1h, g1l], axis=1),
        twid,
    )


def dot(a, b):
    return jnp.dot(a, b, preferred_element_type=F32)


def halves(val):
    hi = val.astype(BF16)
    lo = (val - hi.astype(F32)).astype(BF16)
    return hi, lo


RING = 4
PART_ORDERS = ((0, 1, 2), (1, 2, 0), (2, 0, 1))


def part_columns(total):
    tiles = total // 128
    ends = [0, (tiles + 2) // 3 * 128, ((tiles + 2) // 3 + (tiles + 1) // 3) * 128, total]
    return [(ends[i], ends[i + 1]) for i in range(3)]


def all_columns(width):
    return part_columns(2 * width) * 2


def result_kernel(*refs):
    for src, dst in zip(refs[:4], refs[5:9]):
        dst[...] = src[...]
    refs[9][...] = jnp.sum(refs[4][...].T, axis=0)


def results(*vals):
    vmem = pl.BlockSpec(memory_space=pltpu.VMEM)
    n_chans = vals[4].shape[0]
    return pl.pallas_call(
        result_kernel,
        out_shape=tuple(jax.ShapeDtypeStruct(val.shape, val.dtype) for val in vals[:4])
        + (jax.ShapeDtypeStruct((n_chans,), F32),),
        in_specs=[vmem] * 5,
        out_specs=(vmem,) * 5,
        cost_estimate=pl.CostEstimate(flops=10 ** 6, bytes_accessed=4 * 2 ** 20, transcendentals=0),
        name="results",
    )(*vals)


def hyena_kernel(x_ref, do_ref, filt_ref, skip_ref, win_hbm, wout_hbm, f1_hbm, f2_hbm, g2_hbm, g1_hbm, tw_hbm,
                 gx_ref, gwin_ref, gwout_ref, gfilt_ref, gskip_ref, *scratch):
    names = iter(scratch)

    def take(count):
        return [next(names) for _ in range(count)]

    u_out, dy_out, u_in, dy_in, y_in, du_in = take(6)
    y_out, du_out = u_in, dy_in
    u_f32, dy_f32, out_f32 = take(3)
    wide, flip, taps = take(3)
    u_spec, h_spec, d_spec = take(3)
    f1_ref, f2_ref, g2_ref, g1_ref, tw_ref, win_ref, wout_ref = take(7)
    qkv_ref, dz_ref = take(2)
    x_own, z_own, d_own, x_peer, z_peer, d_peer, do_peer = take(7)
    partial = take(6)
    vias, fins, reds = [], [], []
    for phase in range(3):
        vias.append(take(6))
        fins.append(take(6))
        if phase < 2:
            reds.append(take(6))
    load_sem, wide_sem, ex_send, ex_recv, swap_send, swap_recv, ring_send, ring_recv = take(8)

    n_dev, n_chans, n_tok = u_out.shape
    n_lanes = n_tok // 2
    n_rows = 2 * n_dev
    n_pairs = n_chans // 2
    width = n_dev * n_chans
    rank = lax.axis_index("cp")
    core = lax.rem(rank, 2)
    chip = lax.div(rank, 2)
    coords = (lax.div(chip, 16), lax.rem(lax.div(chip, 4), 4), lax.rem(chip, 4))
    strides = (32, 8, 2)
    peer = rank + 1 - 2 * core

    def remote(src, dst, send, recv, device):
        return pltpu.make_async_remote_copy(src_ref=src, dst_ref=dst, send_sem=send, recv_sem=recv,
                                            device_id={"cp": device}, device_id_type=pl.DeviceIdType.MESH)

    def others(body):
        body(lax.rem(rank + 1, n_dev))

        def step(i, carry):
            for k in range(7):
                body(lax.rem(rank + 2 + 7 * i + k, n_dev))
            return carry

        lax.fori_loop(0, (n_dev - 2) // 7, step, 0)

    barrier = pltpu.get_barrier_semaphore()
    others(lambda dev: pl.semaphore_signal(barrier, inc=1, device_id={"cp": dev}, device_id_type=pl.DeviceIdType.MESH))

    n_slot, per_slot = wide.shape[0], wide.shape[1]
    n_wide = filt_ref.shape[0] // per_slot
    first_lane = pl.multiple_of(lax.div(rank * n_chans, 128) * 128, 128)
    wides = [pltpu.make_async_copy(
        filt_ref.at[pl.ds(i * per_slot, per_slot), pl.ds(first_lane, 128)], wide.at[i % n_slot], wide_sem.at[i])
        for i in range(n_wide)]
    loads = [pltpu.make_async_copy(src, dst, load_sem.at[i]) for i, (src, dst) in enumerate(
        [(win_hbm.at[:, pl.ds(j * width, width)], win_ref.at[:, pl.ds(j * width, width)]) for j in range(3)]
        + [(wout_hbm, wout_ref), (f1_hbm, f1_ref), (f2_hbm, f2_ref), (g2_hbm, g2_ref), (g1_hbm, g1_ref), (tw_hbm, tw_ref)])]
    for copy in [loads[1], loads[2], loads[0]] + loads[3:] + wides[:n_slot]:
        copy.start()

    def act(i):
        return qkv_ref[i * width:(i + 1) * width]

    def project(i):
        loads[i].wait()
        for first in range(i * width, (i + 1) * width, 256):
            qkv_ref[first:first + 256] = dot(x_ref[...], win_ref[:, first:first + 256]).T.astype(BF16)

    project(1)
    project(2)
    u_out[...] = (act(1) * act(2)).reshape(u_out.shape)
    pl.semaphore_wait(barrier, n_dev - 1)

    def exchange(which, src, dst):
        others(lambda dev: remote(src.at[dev], dst.at[rank], ex_send.at[which], ex_recv.at[which], dev).start())
        dst[rank] = src[rank]

    def wait_all(sem, which, ref):
        part = ref.at[pl.ds(0, n_dev - 1)]
        pltpu.make_async_copy(part, part, sem.at[which]).wait()

    exchange(0, u_out, u_in)
    project(0)
    loads[3].wait()
    for first in range(0, width, 256):
        dz_ref[first:first + 256] = lax.dot_general(
            do_ref[...], wout_ref[first:first + 256], (((1,), (1,)), ((), ())), preferred_element_type=F32).T.astype(BF16)
    dy_out[...] = (dz_ref[...] * act(0)).reshape(dy_out.shape)
    exchange(1, dy_out, dy_in)
    n_group = 256 // (2 * n_chans)
    for i in range(width // 256):
        x_own[i * n_group:(i + 1) * n_group] = x_ref[:, i * 256:(i + 1) * 256].astype(F32).T.astype(BF16).reshape(
            n_group, 2, n_chans, n_tok)

    swaps = []

    def swap(src, dst):
        copy = remote(src, dst, swap_send.at[len(swaps)], swap_recv.at[len(swaps)], peer)
        copy.start()
        swaps.append(copy)
        return copy

    x_swap = swap(x_own.at[:, 1 - core], x_peer)
    do_swap = swap(do_ref, do_peer)

    own_row = pl.multiple_of(lax.rem(rank * n_chans, 128), n_chans)
    per_wide = per_slot // n_lanes

    for i in range(n_wide):
        wides[i].wait()

        def turn(j, carry):
            for k in range(4):
                tile = 4 * j + k
                flip[k] = wide[i % n_slot, pl.ds(pl.multiple_of(tile * n_lanes, n_lanes), n_lanes), :].T
                at = pl.multiple_of((i * per_wide + tile) * n_chans, n_chans)
                taps[pl.ds(at, n_chans), :] = flip[k, pl.ds(own_row, n_chans), :]
            return carry

        lax.fori_loop(0, per_wide // 4, turn, 0)
        if i + n_slot < n_wide:
            wides[i + n_slot].start()
    for copy in loads[4:]:
        copy.wait()

    def f1(i):
        return f1_ref[:, i * n_rows:(i + 1) * n_rows]

    def g1(i):
        return g1_ref[:, 2 * i * n_rows:2 * (i + 1) * n_rows]

    def f2(i):
        return f2_ref[2 * i * n_lanes:2 * (i + 1) * n_lanes]

    def g2(i):
        return g2_ref[2 * i * n_lanes:2 * (i + 1) * n_lanes]

    def twist():
        return tw_ref[:, :n_lanes], tw_ref[:, n_lanes:]

    def second(stage):
        wr, wi = twist()
        parts = []
        for i in range(2):
            ar = stage[:n_rows, i * n_lanes:(i + 1) * n_lanes]
            ai = stage[n_rows:, i * n_lanes:(i + 1) * n_lanes]
            parts.append(jnp.concatenate([ar * wr - ai * wi, ar * wi + ai * wr], axis=1))
        bh, bl = halves(jnp.concatenate(parts, axis=0))
        return dot(bh, f2(0)) + (dot(bh, f2(1)) + dot(bl, f2(0)))

    def inverse(pr, pi):
        wr, wi = twist()
        ph, pll = halves(jnp.concatenate([pr, pi], axis=1))
        mid = dot(ph, g2(0)) + (dot(ph, g2(1)) + dot(pll, g2(0)))
        tr, ti = [], []
        for i in range(2):
            gr = mid[i * n_rows:(i + 1) * n_rows, :n_lanes]
            gi = mid[i * n_rows:(i + 1) * n_rows, n_lanes:]
            tr.append(gr * wr + gi * wi)
            ti.append(gi * wr - gr * wi)
        th, tl = halves(jnp.concatenate([jnp.concatenate(tr, axis=1), jnp.concatenate(ti, axis=1)], axis=0))
        return dot(g1(0), th) + (dot(g1(0), tl) + dot(g1(1), th))

    def pairs(body, first=0, last=n_pairs):
        def step(p, carry):
            body(p)
            return carry

        lax.fori_loop(first, last, step, 0)

    def rows_of(ref, chan):
        return jnp.concatenate([ref[0, pl.ds(chan, n_dev, stride=n_chans), :],
                                ref[1, pl.ds(chan, n_dev, stride=n_chans), :]], axis=0)

    def both(ref, p):
        return jnp.concatenate([rows_of(ref, 2 * p), rows_of(ref, 2 * p + 1)], axis=1)

    def widen(src, dst):
        for half in range(2):
            dst[half] = src[:, :, half * n_lanes:(half + 1) * n_lanes].astype(F32).reshape(dst.shape[1:])

    def parts_of(ref, p):
        return ref[p, :, :n_lanes], ref[p, :, n_lanes:]

    def taps_spec(p):
        def one(chan):
            return jnp.concatenate([taps[pl.ds(chan, n_dev, stride=2 * n_chans), :],
                                    taps[pl.ds(n_chans + chan, n_dev, stride=2 * n_chans), :]], axis=0)

        h_hi, h_lo = halves(jnp.concatenate([one(2 * p), one(2 * p + 1)], axis=1))
        h_spec[p] = second(dot(f1(0), h_hi) + (dot(f1(0), h_lo) + dot(f1(1), h_hi)))

    pairs(taps_spec)

    def filtered(sig, spec, sign):
        def one(p):
            val = both(sig, p)
            low = val.astype(BF16)
            spec[p] = second(dot(f1(0), low) + dot(f1(1), low))
            sr, si = parts_of(spec, p)
            hr, hi = parts_of(h_spec, p)
            if sign > 0:
                lin = inverse(sr * hr - si * hi, sr * hi + si * hr)
            else:
                lin = inverse(sr * hr + si * hi, si * hr - sr * hi)
            for i in range(2):
                chan = 2 * p + i
                cols = slice(i * n_lanes, (i + 1) * n_lanes)
                res = lin[:, cols] + skip_ref[rank * n_chans + chan] * val[:, cols]
                for odd in range(2):
                    out_f32[odd, pl.ds(chan, n_dev, stride=n_chans), :] = res[odd * n_dev:(odd + 1) * n_dev]

        pairs(one)

    def narrow(dst):
        for half in range(2):
            dst[:, :, half * n_lanes:(half + 1) * n_lanes] = out_f32[half].astype(BF16).reshape(
                n_dev, n_chans, n_lanes)

    wait_all(ex_recv, 0, u_in)
    widen(u_in, u_f32)
    filtered(u_f32, u_spec, 1)
    narrow(y_out)
    exchange(2, y_out, y_in)
    wait_all(ex_recv, 1, dy_in)
    widen(dy_in, dy_f32)
    filtered(dy_f32, d_spec, -1)
    narrow(du_out)
    exchange(3, du_out, du_in)

    wait_all(ex_recv, 2, y_in)
    y_act = y_in[...].reshape(width, n_tok)
    z_own[...] = (act(0) * y_act).reshape(z_own.shape)
    d_own[0:width] = dz_ref[...] * y_act
    z_swap = swap(z_own.at[:, 1 - core], z_peer)
    d_swaps = [swap(d_own.at[pl.ds(0, width)], d_peer.at[pl.ds(0, width)])]

    def taps_grad(p):
        ur, ui = parts_of(u_spec, p)
        dr, di = parts_of(d_spec, p)
        lin = inverse(dr * ur + di * ui, di * ur - dr * ui)
        prod = both(u_f32, p) * both(dy_f32, p)
        for i in range(2):
            chan = 2 * p + i
            cols = slice(i * n_lanes, (i + 1) * n_lanes)
            gskip_ref[pl.ds(chan, 1), :] = jnp.sum(prod[:, cols], axis=0, keepdims=True)
            for odd in range(2):
                gfilt_ref[pl.ds(odd * n_chans + chan, n_dev, stride=2 * n_chans), :] = lin[
                    odd * n_dev:(odd + 1) * n_dev, cols]

    pairs(taps_grad, 0, n_pairs // 2)

    def at_offset(dim, step):
        pos = lax.rem(coords[dim] + step, RING)
        return pos, rank + (pos - coords[dim]) * strides[dim]

    nxt = [at_offset(dim, 1) for dim in range(3)]
    opp = [at_offset(dim, 2) for dim in range(3)]
    prv = [at_offset(dim, 3) for dim in range(3)]
    cols = all_columns(width)
    half_rows = width // 2

    def mm(a, b, cb):
        return lax.dot_general(a, b, (((1,), (cb,)), ((), ())), preferred_element_type=F32)

    def flat(val):
        return val.reshape(half_rows, n_tok)

    def segments(part):
        lo, hi = cols[part]
        runs = []
        for first, is_out, base in (((0, False, 0), (width, True, 0)) if part < 3 else ((0, False, width),)):
            last = first + width if part < 3 else 2 * width
            a, b = max(lo, first), min(hi, last)
            if a < b:
                runs.append((is_out, base + a - first, a - lo, b - a))
        return runs

    def products(part):
        for is_out, first, place, size in segments(part):
            for off in range(0, size, 512):
                step = min(512, size - off)
                at = first + off
                if is_out:
                    val = (mm(flat(z_own[:, core]), do_ref[:, at:at + step], 0)
                           + mm(flat(z_peer[...]), do_peer[:, at:at + step], 0))
                else:
                    val = (mm(flat(x_own[:, core]), d_own[at:at + step], 1)
                           + mm(flat(x_peer[...]), d_peer[at:at + step], 1))
                partial[part][:, :, :, :, place + off:place + off + step] = val.reshape(
                    RING, RING, RING, n_chans, step)

    def slab(ref, axis, pos, col=None):
        index = [slice(None)] * len(ref.shape)
        if axis is not None:
            index[axis] = pos
        if col is not None:
            index[-1] = pl.ds(*col)
        return ref.at[tuple(index)]

    copies = {}

    def send(part, phase, which, src, dst, device):
        slot = (phase * 6 + part) * 6 + which
        copy = remote(src, dst, ring_send.at[slot], ring_recv.at[slot], device)
        copy.start()
        copies[part, phase, which] = copy

    def setting(part, phase):
        order = PART_ORDERS[(part + part // 3) % 3]
        dim = order[phase]
        axis = sorted(order[phase:]).index(dim)
        src = partial[part] if phase == 0 else reds[phase - 1][part]
        size = src.shape[-1]
        first = (size // 128 + 1) // 2 * 128
        return dim, axis, src, vias[phase][part], fins[phase][part], (0, first), (first, size - first)

    def launch(part, phase):
        dim, axis, src, via, fin, a_cols, b_cols = setting(part, phase)
        send(part, phase, 0, slab(src, axis, opp[dim][0], a_cols), slab(via, None, None, a_cols), nxt[dim][1])
        send(part, phase, 1, slab(src, axis, opp[dim][0], b_cols), slab(via, None, None, b_cols), prv[dim][1])
        send(part, phase, 2, slab(src, axis, nxt[dim][0], b_cols), slab(fin, 0, 0, b_cols), nxt[dim][1])
        send(part, phase, 3, slab(src, axis, prv[dim][0], a_cols), slab(fin, 0, 1, a_cols), prv[dim][1])

    def each_block(shape, body):
        lead = shape[:-2]
        count = int(np.prod(lead)) if lead else 1
        if count == 1:
            body(tuple(0 for _ in lead))
            return

        def step(i, carry):
            index = []
            for size in reversed(lead):
                index.insert(0, lax.rem(i, size))
                i = lax.div(i, size)
            body(tuple(index))
            return carry

        lax.fori_loop(0, count, step, 0, unroll=min(count, 4))

    def relay(part, phase):
        dim, axis, src, via, fin, a_cols, b_cols = setting(part, phase)
        for which, col, spot, side in ((0, a_cols, nxt[dim], 0), (1, b_cols, prv[dim], 1)):
            copies[part, phase, which].wait_recv()
            span = pl.ds(*col)

            def add(index):
                at = index[:axis] + (spot[0],) + index[axis:]
                src[at + (slice(None), span)] = src[at + (slice(None), span)] + via[index + (slice(None), span)]

            each_block(via.shape, add)
            send(part, phase, 4 + which, slab(src, axis, spot[0], col), slab(fin, 0, side, col), spot[1])

    def finish(part, phase):
        dim, axis, src, via, fin, _, _ = setting(part, phase)
        for which in range(2, 6):
            copies[part, phase, which].wait_recv()

        def add(index):
            at = index[:axis] + (coords[dim],) + index[axis:]
            total = src[at] + fin[(0,) + index] + fin[(1,) + index]
            if phase < 2:
                reds[phase][part][index] = total
                return
            for is_out, first, place, size in segments(part):
                dst = gwout_ref if is_out else gwin_ref
                dst[:, first:first + size] = total[:, place:place + size].astype(dst.dtype)

        each_block(via.shape, add)
        if phase < 2:
            launch(part, phase + 1)

    early, late = (0, 1, 2), (3, 4, 5)
    for copy in (x_swap, do_swap, z_swap, d_swaps[0]):
        copy.wait_recv()
    for part in early:
        products(part)
        launch(part, 0)

    wait_all(ex_recv, 3, du_in)
    du_act = du_in[...].reshape(width, n_tok)
    for i in (1, 2):
        d_own[i * width:(i + 1) * width] = du_act * act(3 - i)
        span = pl.ds(i * width, width)
        d_swaps.append(swap(d_own.at[span], d_peer.at[span]))

    def run(step, parts, phase):
        for part in parts:
            step(part, phase)

    run(relay, early, 0)
    for copy in d_swaps[1:]:
        copy.wait_recv()
    for part in late:
        products(part)
        launch(part, 0)
    pairs(taps_grad, n_pairs // 2, n_pairs)

    def input_grad(first):
        gx_ref[:, first:first + 256] = dot(win_ref[first:first + 256], d_own[...]).T.astype(gx_ref.dtype)

    run(finish, early, 0)
    run(relay, late, 0)
    run(relay, early, 1)
    run(finish, early, 1)
    run(finish, late, 0)
    input_grad(0)
    input_grad(256)
    run(relay, early, 2)
    run(finish, early, 2)
    run(relay, late, 1)
    input_grad(512)
    run(finish, late, 1)
    input_grad(768)
    run(relay, late, 2)
    run(finish, late, 2)
    for which, ref in enumerate((u_out, dy_out, y_out, du_out)):
        wait_all(ex_send, which, ref)
    for copy in list(copies.values()) + swaps:
        copy.wait_send()


def hyena_grads(x_tok, d_out, filt_taps, skip_gain, w_in, w_out, n_dev):
    n_tok, width = x_tok.shape
    n_chans, n_chip = width // n_dev, n_dev // 2
    n_lanes, n_rows = n_tok // 2, 2 * n_dev
    n_taps = filt_taps.shape[0]
    n_wide, n_slot = 16, 3
    tables = [jnp.asarray(tab) for tab in transform_tables(n_rows, n_lanes)]
    vmem = pl.BlockSpec(memory_space=pltpu.VMEM)
    hbm = pl.BlockSpec(memory_space=pl.ANY)
    widths = [hi - lo for lo, hi in all_columns(width)]
    pairs = pltpu.VMEM((n_chip, 2, n_chans, n_tok), BF16)
    single = pltpu.VMEM((n_chip, n_chans, n_tok), BF16)
    stack = pltpu.VMEM((3 * width, n_tok), BF16)
    scratch = [pltpu.VMEM((n_dev, n_chans, n_tok), BF16)] * 6
    scratch += [pltpu.VMEM((2, width, n_lanes), F32)] * 3
    scratch += [pltpu.VMEM((n_slot, n_taps // n_wide, 128), F32), pltpu.VMEM((4, 128, n_lanes), F32),
                pltpu.VMEM((n_rows * n_chans, n_lanes), F32)]
    scratch += [pltpu.VMEM((n_chans // 2, 2 * n_rows, 2 * n_lanes), F32)] * 3
    scratch += [pltpu.VMEM(arr.shape, arr.dtype) for arr in tables + [w_in, w_out]]
    scratch += [stack, pltpu.VMEM((width, n_tok), BF16)]
    scratch += [pairs, pairs, stack, single, single, stack, pltpu.VMEM(d_out.shape, BF16)]
    scratch += [pltpu.VMEM((RING,) * 3 + (n_chans, w), F32) for w in widths]
    for n_lead in (2, 1, 0):
        lead = (RING,) * n_lead
        scratch += [pltpu.VMEM(lead + (n_chans, w), F32) for w in widths]
        scratch += [pltpu.VMEM((2,) + lead + (n_chans, w), F32) for w in widths]
        if n_lead:
            scratch += [pltpu.VMEM(lead + (n_chans, w), F32) for w in widths]
    scratch += [pltpu.SemaphoreType.DMA((n,)) for n in (len(tables) + 4, n_wide, 4, 4, 6, 6, 108, 108)]
    return pl.pallas_call(
        hyena_kernel,
        out_shape=(
            jax.ShapeDtypeStruct((n_tok, width), BF16),
            jax.ShapeDtypeStruct((n_chans, 3 * width), BF16),
            jax.ShapeDtypeStruct((n_chans, width), BF16),
            jax.ShapeDtypeStruct((n_rows * n_chans, n_lanes), F32),
            jax.ShapeDtypeStruct((n_chans, n_lanes), F32),
        ),
        in_specs=[vmem] * 2 + [hbm, pl.BlockSpec(memory_space=pltpu.SMEM)] + [hbm] * 7,
        out_specs=(vmem,) * 5,
        scratch_shapes=scratch,
        compiler_params=pltpu.CompilerParams(vmem_limit_bytes=57 * 2 ** 20, collective_id=0, has_side_effects=True),
        cost_estimate=pl.CostEstimate(flops=2 * 10 ** 10, bytes_accessed=32 * 2 ** 20, transcendentals=0),
        name="hyena_grads",
    )(x_tok, d_out, filt_taps, skip_gain, w_in, w_out, *tables)


def solution(mesh):
    ctx_size = mesh.shape["cp"]

    def local_step(x_seq, w_in, w_out, filt_taps, skip_gain, d_out):
        n_batch, n_tok, width = x_seq.shape
        n_chans = width // ctx_size
        seq_len = n_tok * ctx_size
        n_lanes = n_tok // 2
        x_tok, do_tok = x_seq[0], d_out[0]

        grad_x, grad_w_in, grad_w_out, gfilt, grad_skip = results(*hyena_grads(
            x_tok, do_tok, filt_taps, skip_gain, w_in, w_out, ctx_size))
        grad_filt = gfilt.reshape(seq_len // n_lanes, n_chans, n_lanes).transpose(0, 2, 1).reshape(seq_len, n_chans)
        return grad_x[None], grad_w_in, grad_w_out, grad_filt, grad_skip

    seq_spec = P("dp", "cp", None)
    row_spec = P(("dp", "cp"), None)
    return jax.shard_map(
        local_step,
        mesh=mesh,
        in_specs=(seq_spec, P(), P(), P(), P(), seq_spec),
        out_specs=(seq_spec, row_spec, row_spec, P("dp", "cp"), P(("dp", "cp"))),
        check_vma=False,
    )
```

```python
import functools

import jax
import jax.numpy as jnp
import numpy as np
from jax import lax
from jax.experimental import pallas as pl
from jax.experimental.pallas import tpu as pltpu
from jax.sharding import PartitionSpec as P

F32, BF16 = jnp.float32, jnp.bfloat16


def split_const(mat):
    hi = mat.astype(np.float32).astype(jnp.bfloat16)
    lo = (mat - hi.astype(np.float64)).astype(np.float32).astype(jnp.bfloat16)
    return hi, lo


@functools.lru_cache(None)
def transform_tables(n_rows, n_lanes):
    n = n_rows * n_lanes
    t1 = np.concatenate([np.arange(0, n_rows, 2), np.arange(1, n_rows, 2)])
    k1 = np.arange(n_rows)
    ang = 2 * np.pi * np.outer(k1 + 0.25, t1) / n_rows
    f1 = np.concatenate([np.cos(ang), -np.sin(ang)], axis=0)
    g1 = f1.T / n
    t2 = np.arange(n_lanes)
    psi = 2 * np.pi * (np.outer(t2, t2) % n_lanes) / n_lanes
    cos2, sin2 = np.cos(psi), np.sin(psi)
    f2 = np.block([[cos2, -sin2], [sin2, cos2]])
    g2 = f2.T
    twist = 2 * np.pi * np.outer(k1 + 0.25, t2) / n
    twid = np.concatenate([np.cos(twist), -np.sin(twist)], axis=1).astype(np.float32)
    f1h, f1l = split_const(f1)
    g1h, g1l = split_const(g1)
    f2h, f2l = split_const(f2)
    g2h, g2l = split_const(g2)
    return (
        np.concatenate([f1h, f1l], axis=1),
        np.concatenate([f2h, f2l], axis=0),
        np.concatenate([g2h, g2l], axis=0),
        np.concatenate([g1h, g1l], axis=1),
        twid,
    )


def dot(a, b):
    return jnp.dot(a, b, preferred_element_type=F32)


def halves(val):
    hi = val.astype(BF16)
    lo = (val - hi.astype(F32)).astype(BF16)
    return hi, lo


RING = 4
PART_ORDERS = ((0, 1, 2), (1, 2, 0), (2, 0, 1))


def part_columns(total):
    tiles = total // 128
    ends = [0, (tiles + 2) // 3 * 128, ((tiles + 2) // 3 + (tiles + 1) // 3) * 128, total]
    return [(ends[i], ends[i + 1]) for i in range(3)]


def all_columns(width):
    return part_columns(2 * width) * 2


def result_kernel(*refs):
    for src, dst in zip(refs[:4], refs[5:9]):
        dst[...] = src[...]
    refs[9][...] = jnp.sum(refs[4][...].T, axis=0)


def results(*vals):
    vmem = pl.BlockSpec(memory_space=pltpu.VMEM)
    n_chans = vals[4].shape[0]
    return pl.pallas_call(
        result_kernel,
        out_shape=tuple(jax.ShapeDtypeStruct(val.shape, val.dtype) for val in vals[:4])
        + (jax.ShapeDtypeStruct((n_chans,), F32),),
        in_specs=[vmem] * 5,
        out_specs=(vmem,) * 5,
        cost_estimate=pl.CostEstimate(flops=10 ** 6, bytes_accessed=4 * 2 ** 20, transcendentals=0),
        name="results",
    )(*vals)


def hyena_kernel(x_ref, do_ref, filt_ref, skip_ref, win_hbm, wout_hbm, f1_hbm, f2_hbm, g2_hbm, g1_hbm, tw_hbm,
                 gx_ref, gwin_ref, gwout_ref, gfilt_ref, gskip_ref, *scratch):
    names = iter(scratch)

    def take(count):
        return [next(names) for _ in range(count)]

    u_out, dy_out, u_in, dy_in, y_in, du_in = take(6)
    y_out, du_out = u_in, dy_in
    u_f32, dy_f32, out_f32 = take(3)
    wide, flip, taps = take(3)
    u_spec, h_spec, d_spec = take(3)
    f1_ref, f2_ref, g2_ref, g1_ref, tw_ref, win_ref, wout_ref = take(7)
    qkv_ref, dz_ref = take(2)
    x_own, z_own, d_own, x_peer, z_peer, d_peer, do_peer = take(7)
    partial = take(6)
    vias, fins, reds = [], [], []
    for phase in range(3):
        vias.append(take(6))
        fins.append(take(6))
        if phase < 2:
            reds.append(take(6))
    load_sem, wide_sem, ex_send, ex_recv, swap_send, swap_recv, ring_send, ring_recv = take(8)

    n_dev, n_chans, n_tok = u_out.shape
    n_lanes = n_tok // 2
    n_rows = 2 * n_dev
    n_pairs = n_chans // 2
    width = n_dev * n_chans
    rank = lax.axis_index("cp")
    core = lax.rem(rank, 2)
    chip = lax.div(rank, 2)
    coords = (lax.div(chip, 16), lax.rem(lax.div(chip, 4), 4), lax.rem(chip, 4))
    strides = (32, 8, 2)
    peer = rank + 1 - 2 * core

    def remote(src, dst, send, recv, device):
        return pltpu.make_async_remote_copy(src_ref=src, dst_ref=dst, send_sem=send, recv_sem=recv,
                                            device_id={"cp": device}, device_id_type=pl.DeviceIdType.MESH)

    def others(body):
        body(lax.rem(rank + 1, n_dev))

        def step(i, carry):
            for k in range(7):
                body(lax.rem(rank + 2 + 7 * i + k, n_dev))
            return carry

        lax.fori_loop(0, (n_dev - 2) // 7, step, 0)

    barrier = pltpu.get_barrier_semaphore()
    others(lambda dev: pl.semaphore_signal(barrier, inc=1, device_id={"cp": dev}, device_id_type=pl.DeviceIdType.MESH))

    n_slot, per_slot = wide.shape[0], wide.shape[1]
    n_wide = filt_ref.shape[0] // per_slot
    first_lane = pl.multiple_of(lax.div(rank * n_chans, 128) * 128, 128)
    wides = [pltpu.make_async_copy(
        filt_ref.at[pl.ds(i * per_slot, per_slot), pl.ds(first_lane, 128)], wide.at[i % n_slot], wide_sem.at[i])
        for i in range(n_wide)]
    loads = [pltpu.make_async_copy(src, dst, load_sem.at[i]) for i, (src, dst) in enumerate(
        [(win_hbm.at[:, pl.ds(j * width, width)], win_ref.at[:, pl.ds(j * width, width)]) for j in range(3)]
        + [(wout_hbm, wout_ref), (f1_hbm, f1_ref), (f2_hbm, f2_ref), (g2_hbm, g2_ref), (g1_hbm, g1_ref), (tw_hbm, tw_ref)])]
    for copy in [loads[1], loads[2], loads[0]] + loads[3:] + wides[:n_slot]:
        copy.start()

    def act(i):
        return qkv_ref[i * width:(i + 1) * width]

    def project(i):
        loads[i].wait()
        for first in range(i * width, (i + 1) * width, 256):
            qkv_ref[first:first + 256] = dot(x_ref[...], win_ref[:, first:first + 256]).T.astype(BF16)

    project(1)
    project(2)
    u_out[...] = (act(1) * act(2)).reshape(u_out.shape)
    pl.semaphore_wait(barrier, n_dev - 1)

    def exchange(which, src, dst):
        others(lambda dev: remote(src.at[dev], dst.at[rank], ex_send.at[which], ex_recv.at[which], dev).start())
        dst[rank] = src[rank]

    def wait_all(sem, which, ref):
        part = ref.at[pl.ds(0, n_dev - 1)]
        pltpu.make_async_copy(part, part, sem.at[which]).wait()

    exchange(0, u_out, u_in)
    project(0)
    loads[3].wait()
    for first in range(0, width, 256):
        dz_ref[first:first + 256] = lax.dot_general(
            do_ref[...], wout_ref[first:first + 256], (((1,), (1,)), ((), ())), preferred_element_type=F32).T.astype(BF16)
    dy_out[...] = (dz_ref[...] * act(0)).reshape(dy_out.shape)
    exchange(1, dy_out, dy_in)
    n_group = 256 // (2 * n_chans)
    for i in range(width // 256):
        x_own[i * n_group:(i + 1) * n_group] = x_ref[:, i * 256:(i + 1) * 256].astype(F32).T.astype(BF16).reshape(
            n_group, 2, n_chans, n_tok)

    swaps = []

    def swap(src, dst):
        copy = remote(src, dst, swap_send.at[len(swaps)], swap_recv.at[len(swaps)], peer)
        copy.start()
        swaps.append(copy)
        return copy

    x_swap = swap(x_own.at[:, 1 - core], x_peer)
    do_swap = swap(do_ref, do_peer)

    own_row = pl.multiple_of(lax.rem(rank * n_chans, 128), n_chans)
    per_wide = per_slot // n_lanes

    for i in range(n_wide):
        wides[i].wait()

        def turn(j, carry):
            for k in range(4):
                tile = 4 * j + k
                flip[k] = wide[i % n_slot, pl.ds(pl.multiple_of(tile * n_lanes, n_lanes), n_lanes), :].T
                at = pl.multiple_of((i * per_wide + tile) * n_chans, n_chans)
                taps[pl.ds(at, n_chans), :] = flip[k, pl.ds(own_row, n_chans), :]
            return carry

        lax.fori_loop(0, per_wide // 4, turn, 0)
        if i + n_slot < n_wide:
            wides[i + n_slot].start()
    for copy in loads[4:]:
        copy.wait()

    def f1(i):
        return f1_ref[:, i * n_rows:(i + 1) * n_rows]

    def g1(i):
        return g1_ref[:, 2 * i * n_rows:2 * (i + 1) * n_rows]

    def f2(i):
        return f2_ref[2 * i * n_lanes:2 * (i + 1) * n_lanes]

    def g2(i):
        return g2_ref[2 * i * n_lanes:2 * (i + 1) * n_lanes]

    def twist():
        return tw_ref[:, :n_lanes], tw_ref[:, n_lanes:]

    def second(stage):
        wr, wi = twist()
        parts = []
        for i in range(2):
            ar = stage[:n_rows, i * n_lanes:(i + 1) * n_lanes]
            ai = stage[n_rows:, i * n_lanes:(i + 1) * n_lanes]
            parts.append(jnp.concatenate([ar * wr - ai * wi, ar * wi + ai * wr], axis=1))
        bh, bl = halves(jnp.concatenate(parts, axis=0))
        return dot(bh, f2(0)) + (dot(bh, f2(1)) + dot(bl, f2(0)))

    def inverse(pr, pi):
        wr, wi = twist()
        ph, pll = halves(jnp.concatenate([pr, pi], axis=1))
        mid = dot(ph, g2(0)) + (dot(ph, g2(1)) + dot(pll, g2(0)))
        tr, ti = [], []
        for i in range(2):
            gr = mid[i * n_rows:(i + 1) * n_rows, :n_lanes]
            gi = mid[i * n_rows:(i + 1) * n_rows, n_lanes:]
            tr.append(gr * wr + gi * wi)
            ti.append(gi * wr - gr * wi)
        th, tl = halves(jnp.concatenate([jnp.concatenate(tr, axis=1), jnp.concatenate(ti, axis=1)], axis=0))
        return dot(g1(0), th) + (dot(g1(0), tl) + dot(g1(1), th))

    def pairs(body, first=0, last=n_pairs):
        def step(p, carry):
            body(p)
            return carry

        lax.fori_loop(first, last, step, 0)

    def rows_of(ref, chan):
        return jnp.concatenate([ref[0, pl.ds(chan, n_dev, stride=n_chans), :],
                                ref[1, pl.ds(chan, n_dev, stride=n_chans), :]], axis=0)

    def both(ref, p):
        return jnp.concatenate([rows_of(ref, 2 * p), rows_of(ref, 2 * p + 1)], axis=1)

    def widen(src, dst):
        for half in range(2):
            dst[half] = src[:, :, half * n_lanes:(half + 1) * n_lanes].astype(F32).reshape(dst.shape[1:])

    def parts_of(ref, p):
        return ref[p, :, :n_lanes], ref[p, :, n_lanes:]

    def taps_spec(p):
        def one(chan):
            return jnp.concatenate([taps[pl.ds(chan, n_dev, stride=2 * n_chans), :],
                                    taps[pl.ds(n_chans + chan, n_dev, stride=2 * n_chans), :]], axis=0)

        h_hi, h_lo = halves(jnp.concatenate([one(2 * p), one(2 * p + 1)], axis=1))
        h_spec[p] = second(dot(f1(0), h_hi) + (dot(f1(0), h_lo) + dot(f1(1), h_hi)))

    pairs(taps_spec)

    def filtered(sig, spec, sign):
        def one(p):
            val = both(sig, p)
            low = val.astype(BF16)
            spec[p] = second(dot(f1(0), low) + dot(f1(1), low))
            sr, si = parts_of(spec, p)
            hr, hi = parts_of(h_spec, p)
            if sign > 0:
                lin = inverse(sr * hr - si * hi, sr * hi + si * hr)
            else:
                lin = inverse(sr * hr + si * hi, si * hr - sr * hi)
            for i in range(2):
                chan = 2 * p + i
                cols = slice(i * n_lanes, (i + 1) * n_lanes)
                res = lin[:, cols] + skip_ref[rank * n_chans + chan] * val[:, cols]
                for odd in range(2):
                    out_f32[odd, pl.ds(chan, n_dev, stride=n_chans), :] = res[odd * n_dev:(odd + 1) * n_dev]

        pairs(one)

    def narrow(dst):
        for half in range(2):
            dst[:, :, half * n_lanes:(half + 1) * n_lanes] = out_f32[half].astype(BF16).reshape(
                n_dev, n_chans, n_lanes)

    wait_all(ex_recv, 0, u_in)
    widen(u_in, u_f32)
    filtered(u_f32, u_spec, 1)
    narrow(y_out)
    exchange(2, y_out, y_in)
    wait_all(ex_recv, 1, dy_in)
    widen(dy_in, dy_f32)
    filtered(dy_f32, d_spec, -1)
    narrow(du_out)
    exchange(3, du_out, du_in)

    wait_all(ex_recv, 2, y_in)
    y_act = y_in[...].reshape(width, n_tok)
    z_own[...] = (act(0) * y_act).reshape(z_own.shape)
    d_own[0:width] = dz_ref[...] * y_act
    z_swap = swap(z_own.at[:, 1 - core], z_peer)
    d_swaps = [swap(d_own.at[pl.ds(0, width)], d_peer.at[pl.ds(0, width)])]

    def taps_grad(p):
        ur, ui = parts_of(u_spec, p)
        dr, di = parts_of(d_spec, p)
        lin = inverse(dr * ur + di * ui, di * ur - dr * ui)
        prod = both(u_f32, p) * both(dy_f32, p)
        for i in range(2):
            chan = 2 * p + i
            cols = slice(i * n_lanes, (i + 1) * n_lanes)
            gskip_ref[pl.ds(chan, 1), :] = jnp.sum(prod[:, cols], axis=0, keepdims=True)
            for odd in range(2):
                gfilt_ref[pl.ds(odd * n_chans + chan, n_dev, stride=2 * n_chans), :] = lin[
                    odd * n_dev:(odd + 1) * n_dev, cols]

    pairs(taps_grad, 0, n_pairs // 2)

    def at_offset(dim, step):
        pos = lax.rem(coords[dim] + step, RING)
        return pos, rank + (pos - coords[dim]) * strides[dim]

    nxt = [at_offset(dim, 1) for dim in range(3)]
    opp = [at_offset(dim, 2) for dim in range(3)]
    prv = [at_offset(dim, 3) for dim in range(3)]
    cols = all_columns(width)
    half_rows = width // 2

    def mm(a, b, cb):
        return lax.dot_general(a, b, (((1,), (cb,)), ((), ())), preferred_element_type=F32)

    def flat(val):
        return val.reshape(half_rows, n_tok)

    def segments(part):
        lo, hi = cols[part]
        runs = []
        for first, is_out, base in (((0, False, 0), (width, True, 0)) if part < 3 else ((0, False, width),)):
            last = first + width if part < 3 else 2 * width
            a, b = max(lo, first), min(hi, last)
            if a < b:
                runs.append((is_out, base + a - first, a - lo, b - a))
        return runs

    def products(part):
        for is_out, first, place, size in segments(part):
            for off in range(0, size, 512):
                step = min(512, size - off)
                at = first + off
                if is_out:
                    val = (mm(flat(z_own[:, core]), do_ref[:, at:at + step], 0)
                           + mm(flat(z_peer[...]), do_peer[:, at:at + step], 0))
                else:
                    val = (mm(flat(x_own[:, core]), d_own[at:at + step], 1)
                           + mm(flat(x_peer[...]), d_peer[at:at + step], 1))
                partial[part][:, :, :, :, place + off:place + off + step] = val.reshape(
                    RING, RING, RING, n_chans, step)

    def slab(ref, axis, pos, col=None):
        index = [slice(None)] * len(ref.shape)
        if axis is not None:
            index[axis] = pos
        if col is not None:
            index[-1] = pl.ds(*col)
        return ref.at[tuple(index)]

    copies = {}

    def send(part, phase, which, src, dst, device):
        slot = (phase * 6 + part) * 6 + which
        copy = remote(src, dst, ring_send.at[slot], ring_recv.at[slot], device)
        copy.start()
        copies[part, phase, which] = copy

    def setting(part, phase):
        order = PART_ORDERS[(part + part // 3) % 3]
        dim = order[phase]
        axis = sorted(order[phase:]).index(dim)
        src = partial[part] if phase == 0 else reds[phase - 1][part]
        size = src.shape[-1]
        first = (size // 128 + 1) // 2 * 128
        return dim, axis, src, vias[phase][part], fins[phase][part], (0, first), (first, size - first)

    def launch(part, phase):
        dim, axis, src, via, fin, a_cols, b_cols = setting(part, phase)
        send(part, phase, 0, slab(src, axis, opp[dim][0], a_cols), slab(via, None, None, a_cols), nxt[dim][1])
        send(part, phase, 1, slab(src, axis, opp[dim][0], b_cols), slab(via, None, None, b_cols), prv[dim][1])
        send(part, phase, 2, slab(src, axis, nxt[dim][0], b_cols), slab(fin, 0, 0, b_cols), nxt[dim][1])
        send(part, phase, 3, slab(src, axis, prv[dim][0], a_cols), slab(fin, 0, 1, a_cols), prv[dim][1])

    def each_block(shape, body):
        lead = shape[:-2]
        count = int(np.prod(lead)) if lead else 1
        if count == 1:
            body(tuple(0 for _ in lead))
            return

        def step(i, carry):
            index = []
            for size in reversed(lead):
                index.insert(0, lax.rem(i, size))
                i = lax.div(i, size)
            body(tuple(index))
            return carry

        lax.fori_loop(0, count, step, 0, unroll=min(count, 4))

    def relay(part, phase):
        dim, axis, src, via, fin, a_cols, b_cols = setting(part, phase)
        for which, col, spot, side in ((0, a_cols, nxt[dim], 0), (1, b_cols, prv[dim], 1)):
            copies[part, phase, which].wait_recv()
            span = pl.ds(*col)

            def add(index):
                at = index[:axis] + (spot[0],) + index[axis:]
                src[at + (slice(None), span)] = src[at + (slice(None), span)] + via[index + (slice(None), span)]

            each_block(via.shape, add)
            send(part, phase, 4 + which, slab(src, axis, spot[0], col), slab(fin, 0, side, col), spot[1])

    def finish(part, phase):
        dim, axis, src, via, fin, _, _ = setting(part, phase)
        for which in range(2, 6):
            copies[part, phase, which].wait_recv()

        def add(index):
            at = index[:axis] + (coords[dim],) + index[axis:]
            total = src[at] + fin[(0,) + index] + fin[(1,) + index]
            if phase < 2:
                reds[phase][part][index] = total
                return
            for is_out, first, place, size in segments(part):
                dst = gwout_ref if is_out else gwin_ref
                dst[:, first:first + size] = total[:, place:place + size].astype(dst.dtype)

        each_block(via.shape, add)
        if phase < 2:
            launch(part, phase + 1)

    early, late = (0, 1, 2), (3, 4, 5)
    for copy in (x_swap, do_swap, z_swap, d_swaps[0]):
        copy.wait_recv()
    for part in early:
        products(part)
        launch(part, 0)

    wait_all(ex_recv, 3, du_in)
    du_act = du_in[...].reshape(width, n_tok)
    for i in (1, 2):
        d_own[i * width:(i + 1) * width] = du_act * act(3 - i)
        span = pl.ds(i * width, width)
        d_swaps.append(swap(d_own.at[span], d_peer.at[span]))

    def run(step, parts, phase):
        for part in parts:
            step(part, phase)

    run(relay, early, 0)
    for copy in d_swaps[1:]:
        copy.wait_recv()
    for part in late:
        products(part)
        launch(part, 0)
    pairs(taps_grad, n_pairs // 2, n_pairs)

    def input_grad(first):
        gx_ref[:, first:first + 256] = dot(win_ref[first:first + 256], d_own[...]).T.astype(gx_ref.dtype)

    run(finish, early, 0)
    run(relay, late, 0)
    run(relay, early, 1)
    run(finish, early, 1)
    run(finish, late, 0)
    input_grad(0)
    input_grad(256)
    run(relay, early, 2)
    run(finish, early, 2)
    run(relay, late, 1)
    input_grad(512)
    run(finish, late, 1)
    input_grad(768)
    run(relay, late, 2)
    run(finish, late, 2)
    for which, ref in enumerate((u_out, dy_out, y_out, du_out)):
        wait_all(ex_send, which, ref)
    for copy in list(copies.values()) + swaps:
        copy.wait_send()


def hyena_grads(x_tok, d_out, filt_taps, skip_gain, w_in, w_out, n_dev):
    n_tok, width = x_tok.shape
    n_chans, n_chip = width // n_dev, n_dev // 2
    n_lanes, n_rows = n_tok // 2, 2 * n_dev
    n_taps = filt_taps.shape[0]
    n_wide, n_slot = 16, 8
    tables = [jnp.asarray(tab) for tab in transform_tables(n_rows, n_lanes)]
    vmem = pl.BlockSpec(memory_space=pltpu.VMEM)
    hbm = pl.BlockSpec(memory_space=pl.ANY)
    widths = [hi - lo for lo, hi in all_columns(width)]
    pairs = pltpu.VMEM((n_chip, 2, n_chans, n_tok), BF16)
    single = pltpu.VMEM((n_chip, n_chans, n_tok), BF16)
    stack = pltpu.VMEM((3 * width, n_tok), BF16)
    scratch = [pltpu.VMEM((n_dev, n_chans, n_tok), BF16)] * 6
    scratch += [pltpu.VMEM((2, width, n_lanes), F32)] * 3
    scratch += [pltpu.VMEM((n_slot, n_taps // n_wide, 128), F32), pltpu.VMEM((4, 128, n_lanes), F32),
                pltpu.VMEM((n_rows * n_chans, n_lanes), F32)]
    scratch += [pltpu.VMEM((n_chans // 2, 2 * n_rows, 2 * n_lanes), F32)] * 3
    scratch += [pltpu.VMEM(arr.shape, arr.dtype) for arr in tables + [w_in, w_out]]
    scratch += [stack, pltpu.VMEM((width, n_tok), BF16)]
    scratch += [pairs, pairs, stack, single, single, stack, pltpu.VMEM(d_out.shape, BF16)]
    scratch += [pltpu.VMEM((RING,) * 3 + (n_chans, w), F32) for w in widths]
    for n_lead in (2, 1, 0):
        lead = (RING,) * n_lead
        scratch += [pltpu.VMEM(lead + (n_chans, w), F32) for w in widths]
        scratch += [pltpu.VMEM((2,) + lead + (n_chans, w), F32) for w in widths]
        if n_lead:
            scratch += [pltpu.VMEM(lead + (n_chans, w), F32) for w in widths]
    scratch += [pltpu.SemaphoreType.DMA((n,)) for n in (len(tables) + 4, n_wide, 4, 4, 6, 6, 108, 108)]
    return pl.pallas_call(
        hyena_kernel,
        out_shape=(
            jax.ShapeDtypeStruct((n_tok, width), BF16),
            jax.ShapeDtypeStruct((n_chans, 3 * width), BF16),
            jax.ShapeDtypeStruct((n_chans, width), BF16),
            jax.ShapeDtypeStruct((n_rows * n_chans, n_lanes), F32),
            jax.ShapeDtypeStruct((n_chans, n_lanes), F32),
        ),
        in_specs=[vmem] * 2 + [hbm, pl.BlockSpec(memory_space=pltpu.SMEM)] + [hbm] * 7,
        out_specs=(vmem,) * 5,
        scratch_shapes=scratch,
        compiler_params=pltpu.CompilerParams(vmem_limit_bytes=62 * 2 ** 20, collective_id=0, has_side_effects=True),
        cost_estimate=pl.CostEstimate(flops=2 * 10 ** 10, bytes_accessed=32 * 2 ** 20, transcendentals=0),
        name="hyena_grads",
    )(x_tok, d_out, filt_taps, skip_gain, w_in, w_out, *tables)


def solution(mesh):
    ctx_size = mesh.shape["cp"]

    def local_step(x_seq, w_in, w_out, filt_taps, skip_gain, d_out):
        n_batch, n_tok, width = x_seq.shape
        n_chans = width // ctx_size
        seq_len = n_tok * ctx_size
        n_lanes = n_tok // 2
        x_tok, do_tok = x_seq[0], d_out[0]

        grad_x, grad_w_in, grad_w_out, gfilt, grad_skip = results(*hyena_grads(
            x_tok, do_tok, filt_taps, skip_gain, w_in, w_out, ctx_size))
        grad_filt = gfilt.reshape(seq_len // n_lanes, n_chans, n_lanes).transpose(0, 2, 1).reshape(seq_len, n_chans)
        return grad_x[None], grad_w_in, grad_w_out, grad_filt, grad_skip

    seq_spec = P("dp", "cp", None)
    row_spec = P(("dp", "cp"), None)
    return jax.shard_map(
        local_step,
        mesh=mesh,
        in_specs=(seq_spec, P(), P(), P(), P(), seq_spec),
        out_specs=(seq_spec, row_spec, row_spec, P("dp", "cp"), P(("dp", "cp"))),
        check_vma=False,
    )
```

```python
import functools

import jax
import jax.numpy as jnp
import numpy as np
from jax import lax
from jax.experimental import pallas as pl
from jax.experimental.pallas import tpu as pltpu
from jax.sharding import PartitionSpec as P

F32, BF16 = jnp.float32, jnp.bfloat16


def split_const(mat):
    hi = mat.astype(np.float32).astype(jnp.bfloat16)
    lo = (mat - hi.astype(np.float64)).astype(np.float32).astype(jnp.bfloat16)
    return hi, lo


@functools.lru_cache(None)
def transform_tables(n_rows, n_lanes):
    n = n_rows * n_lanes
    t1 = np.concatenate([np.arange(0, n_rows, 2), np.arange(1, n_rows, 2)])
    k1 = np.arange(n_rows)
    ang = 2 * np.pi * np.outer(k1 + 0.25, t1) / n_rows
    f1 = np.concatenate([np.cos(ang), -np.sin(ang)], axis=0)
    g1 = f1.T / n
    t2 = np.arange(n_lanes)
    psi = 2 * np.pi * (np.outer(t2, t2) % n_lanes) / n_lanes
    cos2, sin2 = np.cos(psi), np.sin(psi)
    f2 = np.block([[cos2, -sin2], [sin2, cos2]])
    g2 = f2.T
    twist = 2 * np.pi * np.outer(k1 + 0.25, t2) / n
    twid = np.concatenate([np.cos(twist), -np.sin(twist)], axis=1).astype(np.float32)
    f1h, f1l = split_const(f1)
    g1h, g1l = split_const(g1)
    f2h, f2l = split_const(f2)
    g2h, g2l = split_const(g2)
    return (
        np.concatenate([f1h, f1l], axis=1),
        np.concatenate([f2h, f2l], axis=0),
        np.concatenate([g2h, g2l], axis=0),
        np.concatenate([g1h, g1l], axis=1),
        twid,
    )


def dot(a, b):
    return jnp.dot(a, b, preferred_element_type=F32)


def halves(val):
    hi = val.astype(BF16)
    lo = (val - hi.astype(F32)).astype(BF16)
    return hi, lo


RING = 4
PART_ORDERS = ((0, 1, 2), (1, 2, 0), (2, 0, 1))


def part_columns(total):
    tiles = total // 128
    ends = [0, (tiles + 2) // 3 * 128, ((tiles + 2) // 3 + (tiles + 1) // 3) * 128, total]
    return [(ends[i], ends[i + 1]) for i in range(3)]


def all_columns(width):
    return part_columns(2 * width) * 2


def result_kernel(*refs):
    for src, dst in zip(refs[:4], refs[5:9]):
        dst[...] = src[...]
    refs[9][...] = jnp.sum(refs[4][...].T, axis=0)


def results(*vals):
    vmem = pl.BlockSpec(memory_space=pltpu.VMEM)
    n_chans = vals[4].shape[0]
    return pl.pallas_call(
        result_kernel,
        out_shape=tuple(jax.ShapeDtypeStruct(val.shape, val.dtype) for val in vals[:4])
        + (jax.ShapeDtypeStruct((n_chans,), F32),),
        in_specs=[vmem] * 5,
        out_specs=(vmem,) * 5,
        cost_estimate=pl.CostEstimate(flops=10 ** 6, bytes_accessed=4 * 2 ** 20, transcendentals=0),
        name="results",
    )(*vals)


def hyena_kernel(x_ref, do_ref, filt_ref, skip_ref, win_hbm, wout_hbm, f1_hbm, f2_hbm, g2_hbm, g1_hbm, tw_hbm,
                 gx_ref, gwin_ref, gwout_ref, gfilt_ref, gskip_ref, *scratch):
    names = iter(scratch)

    def take(count):
        return [next(names) for _ in range(count)]

    u_out, dy_out, u_in, dy_in, y_in, du_in = take(6)
    y_out, du_out = u_in, dy_in
    u_f32, dy_f32, out_f32 = take(3)
    wide, flip, taps = take(3)
    u_spec, h_spec, d_spec = take(3)
    f1_ref, f2_ref, g2_ref, g1_ref, tw_ref, win_ref, wout_ref = take(7)
    qkv_ref, dz_ref = take(2)
    x_own, z_own, d_own, x_peer, z_peer, d_peer, do_peer = take(7)
    partial = take(6)
    vias, fins, reds = [], [], []
    for phase in range(3):
        vias.append(take(6))
        fins.append(take(6))
        if phase < 2:
            reds.append(take(6))
    load_sem, wide_sem, ex_send, ex_recv, swap_send, swap_recv, ring_send, ring_recv = take(8)

    n_dev, n_chans, n_tok = u_out.shape
    n_lanes = n_tok // 2
    n_rows = 2 * n_dev
    n_pairs = n_chans // 2
    width = n_dev * n_chans
    rank = lax.axis_index("cp")
    core = lax.rem(rank, 2)
    chip = lax.div(rank, 2)
    coords = (lax.div(chip, 16), lax.rem(lax.div(chip, 4), 4), lax.rem(chip, 4))
    strides = (32, 8, 2)
    peer = rank + 1 - 2 * core

    def remote(src, dst, send, recv, device):
        return pltpu.make_async_remote_copy(src_ref=src, dst_ref=dst, send_sem=send, recv_sem=recv,
                                            device_id={"cp": device}, device_id_type=pl.DeviceIdType.MESH)

    def others(body):
        body(lax.rem(rank + 1, n_dev))

        def step(i, carry):
            for k in range(7):
                body(lax.rem(rank + 2 + 7 * i + k, n_dev))
            return carry

        lax.fori_loop(0, (n_dev - 2) // 7, step, 0)

    barrier = pltpu.get_barrier_semaphore()
    others(lambda dev: pl.semaphore_signal(barrier, inc=1, device_id={"cp": dev}, device_id_type=pl.DeviceIdType.MESH))

    n_slot, per_slot = wide.shape[0], wide.shape[1]
    n_wide = filt_ref.shape[0] // per_slot
    first_lane = pl.multiple_of(lax.div(rank * n_chans, 128) * 128, 128)
    wides = [pltpu.make_async_copy(
        filt_ref.at[pl.ds(i * per_slot, per_slot), pl.ds(first_lane, 128)], wide.at[i % n_slot], wide_sem.at[i])
        for i in range(n_wide)]
    loads = [pltpu.make_async_copy(src, dst, load_sem.at[i]) for i, (src, dst) in enumerate(
        [(win_hbm.at[:, pl.ds(j * width, width)], win_ref.at[:, pl.ds(j * width, width)]) for j in range(3)]
        + [(wout_hbm, wout_ref), (f1_hbm, f1_ref), (f2_hbm, f2_ref), (g2_hbm, g2_ref), (g1_hbm, g1_ref), (tw_hbm, tw_ref)])]
    for copy in [loads[1], loads[2], loads[0]] + loads[3:] + wides[:n_slot]:
        copy.start()

    def act(i):
        return qkv_ref[i * width:(i + 1) * width]

    def project(i):
        loads[i].wait()
        for first in range(i * width, (i + 1) * width, 256):
            qkv_ref[first:first + 256] = dot(x_ref[...], win_ref[:, first:first + 256]).T.astype(BF16)

    project(1)
    project(2)
    u_out[...] = (act(1) * act(2)).reshape(u_out.shape)
    pl.semaphore_wait(barrier, n_dev - 1)

    def exchange(which, src, dst):
        others(lambda dev: remote(src.at[dev], dst.at[rank], ex_send.at[which], ex_recv.at[which], dev).start())
        dst[rank] = src[rank]

    def wait_all(sem, which, ref):
        part = ref.at[pl.ds(0, n_dev - 1)]
        pltpu.make_async_copy(part, part, sem.at[which]).wait()

    exchange(0, u_out, u_in)
    project(0)
    loads[3].wait()
    for first in range(0, width, 256):
        dz_ref[first:first + 256] = lax.dot_general(
            do_ref[...], wout_ref[first:first + 256], (((1,), (1,)), ((), ())), preferred_element_type=F32).T.astype(BF16)
    dy_out[...] = (dz_ref[...] * act(0)).reshape(dy_out.shape)
    exchange(1, dy_out, dy_in)
    n_group = 256 // (2 * n_chans)
    for i in range(width // 256):
        x_own[i * n_group:(i + 1) * n_group] = x_ref[:, i * 256:(i + 1) * 256].astype(F32).T.astype(BF16).reshape(
            n_group, 2, n_chans, n_tok)

    swaps = []

    def swap(src, dst):
        copy = remote(src, dst, swap_send.at[len(swaps)], swap_recv.at[len(swaps)], peer)
        copy.start()
        swaps.append(copy)
        return copy

    x_swap = swap(x_own.at[:, 1 - core], x_peer)
    do_swap = swap(do_ref, do_peer)

    own_row = pl.multiple_of(lax.rem(rank * n_chans, 128), n_chans)
    per_wide = per_slot // n_lanes

    for i in range(n_wide):
        wides[i].wait()

        def turn(j, carry):
            for k in range(4):
                tile = 4 * j + k
                flip[k] = wide[i % n_slot, pl.ds(pl.multiple_of(tile * n_lanes, n_lanes), n_lanes), :].T
                at = pl.multiple_of((i * per_wide + tile) * n_chans, n_chans)
                taps[pl.ds(at, n_chans), :] = flip[k, pl.ds(own_row, n_chans), :]
            return carry

        lax.fori_loop(0, per_wide // 4, turn, 0)
        if i + n_slot < n_wide:
            wides[i + n_slot].start()
    for copy in loads[4:]:
        copy.wait()

    def f1(i):
        return f1_ref[:, i * n_rows:(i + 1) * n_rows]

    def g1(i):
        return g1_ref[:, 2 * i * n_rows:2 * (i + 1) * n_rows]

    def f2(i):
        return f2_ref[2 * i * n_lanes:2 * (i + 1) * n_lanes]

    def g2(i):
        return g2_ref[2 * i * n_lanes:2 * (i + 1) * n_lanes]

    def twist():
        return tw_ref[:, :n_lanes], tw_ref[:, n_lanes:]

    def second(stage):
        wr, wi = twist()
        parts = []
        for i in range(2):
            ar = stage[:n_rows, i * n_lanes:(i + 1) * n_lanes]
            ai = stage[n_rows:, i * n_lanes:(i + 1) * n_lanes]
            parts.append(jnp.concatenate([ar * wr - ai * wi, ar * wi + ai * wr], axis=1))
        bh, bl = halves(jnp.concatenate(parts, axis=0))
        return dot(bh, f2(0)) + (dot(bh, f2(1)) + dot(bl, f2(0)))

    def inverse(pr, pi):
        wr, wi = twist()
        ph, pll = halves(jnp.concatenate([pr, pi], axis=1))
        mid = dot(ph, g2(0)) + (dot(ph, g2(1)) + dot(pll, g2(0)))
        tr, ti = [], []
        for i in range(2):
            gr = mid[i * n_rows:(i + 1) * n_rows, :n_lanes]
            gi = mid[i * n_rows:(i + 1) * n_rows, n_lanes:]
            tr.append(gr * wr + gi * wi)
            ti.append(gi * wr - gr * wi)
        th, tl = halves(jnp.concatenate([jnp.concatenate(tr, axis=1), jnp.concatenate(ti, axis=1)], axis=0))
        return dot(g1(0), th) + (dot(g1(0), tl) + dot(g1(1), th))

    def pairs(body, first=0, last=n_pairs):
        def step(p, carry):
            body(p)
            return carry

        lax.fori_loop(first, last, step, 0)

    def rows_of(ref, chan):
        return jnp.concatenate([ref[0, pl.ds(chan, n_dev, stride=n_chans), :],
                                ref[1, pl.ds(chan, n_dev, stride=n_chans), :]], axis=0)

    def both(ref, p):
        return jnp.concatenate([rows_of(ref, 2 * p), rows_of(ref, 2 * p + 1)], axis=1)

    def widen(src, dst):
        for half in range(2):
            dst[half] = src[:, :, half * n_lanes:(half + 1) * n_lanes].astype(F32).reshape(dst.shape[1:])

    def parts_of(ref, p):
        return ref[p, :, :n_lanes], ref[p, :, n_lanes:]

    def taps_spec(p):
        def one(chan):
            return jnp.concatenate([taps[pl.ds(chan, n_dev, stride=2 * n_chans), :],
                                    taps[pl.ds(n_chans + chan, n_dev, stride=2 * n_chans), :]], axis=0)

        h_hi, h_lo = halves(jnp.concatenate([one(2 * p), one(2 * p + 1)], axis=1))
        h_spec[p] = second(dot(f1(0), h_hi) + (dot(f1(0), h_lo) + dot(f1(1), h_hi)))

    pairs(taps_spec)

    def filtered(sig, spec, sign):
        def one(p):
            val = both(sig, p)
            low = val.astype(BF16)
            spec[p] = second(dot(f1(0), low) + dot(f1(1), low))
            sr, si = parts_of(spec, p)
            hr, hi = parts_of(h_spec, p)
            if sign > 0:
                lin = inverse(sr * hr - si * hi, sr * hi + si * hr)
            else:
                lin = inverse(sr * hr + si * hi, si * hr - sr * hi)
            for i in range(2):
                chan = 2 * p + i
                cols = slice(i * n_lanes, (i + 1) * n_lanes)
                res = lin[:, cols] + skip_ref[rank * n_chans + chan] * val[:, cols]
                for odd in range(2):
                    out_f32[odd, pl.ds(chan, n_dev, stride=n_chans), :] = res[odd * n_dev:(odd + 1) * n_dev]

        pairs(one)

    def narrow(dst):
        for half in range(2):
            dst[:, :, half * n_lanes:(half + 1) * n_lanes] = out_f32[half].astype(BF16).reshape(
                n_dev, n_chans, n_lanes)

    wait_all(ex_recv, 0, u_in)
    widen(u_in, u_f32)
    filtered(u_f32, u_spec, 1)
    narrow(y_out)
    exchange(2, y_out, y_in)
    wait_all(ex_recv, 1, dy_in)
    widen(dy_in, dy_f32)
    filtered(dy_f32, d_spec, -1)
    narrow(du_out)
    exchange(3, du_out, du_in)

    wait_all(ex_recv, 2, y_in)
    y_act = y_in[...].reshape(width, n_tok)
    z_own[...] = (act(0) * y_act).reshape(z_own.shape)
    d_own[0:width] = dz_ref[...] * y_act
    z_swap = swap(z_own.at[:, 1 - core], z_peer)
    d_swaps = [swap(d_own.at[pl.ds(0, width)], d_peer.at[pl.ds(0, width)])]

    def taps_grad(p):
        ur, ui = parts_of(u_spec, p)
        dr, di = parts_of(d_spec, p)
        lin = inverse(dr * ur + di * ui, di * ur - dr * ui)
        prod = both(u_f32, p) * both(dy_f32, p)
        for i in range(2):
            chan = 2 * p + i
            cols = slice(i * n_lanes, (i + 1) * n_lanes)
            gskip_ref[pl.ds(chan, 1), :] = jnp.sum(prod[:, cols], axis=0, keepdims=True)
            for odd in range(2):
                gfilt_ref[pl.ds(odd * n_chans + chan, n_dev, stride=2 * n_chans), :] = lin[
                    odd * n_dev:(odd + 1) * n_dev, cols]

    pairs(taps_grad, 0, n_pairs // 2)

    def at_offset(dim, step):
        pos = lax.rem(coords[dim] + step, RING)
        return pos, rank + (pos - coords[dim]) * strides[dim]

    nxt = [at_offset(dim, 1) for dim in range(3)]
    opp = [at_offset(dim, 2) for dim in range(3)]
    prv = [at_offset(dim, 3) for dim in range(3)]
    cols = all_columns(width)
    half_rows = width // 2

    def mm(a, b, cb):
        return lax.dot_general(a, b, (((1,), (cb,)), ((), ())), preferred_element_type=F32)

    def flat(val):
        return val.reshape(half_rows, n_tok)

    def segments(part):
        lo, hi = cols[part]
        runs = []
        for first, is_out, base in (((0, False, 0), (width, True, 0)) if part < 3 else ((0, False, width),)):
            last = first + width if part < 3 else 2 * width
            a, b = max(lo, first), min(hi, last)
            if a < b:
                runs.append((is_out, base + a - first, a - lo, b - a))
        return runs

    def products(part):
        for is_out, first, place, size in segments(part):
            for off in range(0, size, 512):
                step = min(512, size - off)
                at = first + off
                if is_out:
                    val = (mm(flat(z_own[:, core]), do_ref[:, at:at + step], 0)
                           + mm(flat(z_peer[...]), do_peer[:, at:at + step], 0))
                else:
                    val = (mm(flat(x_own[:, core]), d_own[at:at + step], 1)
                           + mm(flat(x_peer[...]), d_peer[at:at + step], 1))
                partial[part][:, :, :, :, place + off:place + off + step] = val.reshape(
                    RING, RING, RING, n_chans, step)

    def slab(ref, axis, pos, col=None):
        index = [slice(None)] * len(ref.shape)
        if axis is not None:
            index[axis] = pos
        if col is not None:
            index[-1] = pl.ds(*col)
        return ref.at[tuple(index)]

    copies = {}

    def send(part, phase, which, src, dst, device):
        slot = (phase * 6 + part) * 6 + which
        copy = remote(src, dst, ring_send.at[slot], ring_recv.at[slot], device)
        copy.start()
        copies[part, phase, which] = copy

    def setting(part, phase):
        order = PART_ORDERS[(part + part // 3) % 3]
        dim = order[phase]
        axis = sorted(order[phase:]).index(dim)
        src = partial[part] if phase == 0 else reds[phase - 1][part]
        size = src.shape[-1]
        first = (size // 128 + 1) // 2 * 128
        return dim, axis, src, vias[phase][part], fins[phase][part], (0, first), (first, size - first)

    def launch(part, phase):
        dim, axis, src, via, fin, a_cols, b_cols = setting(part, phase)
        send(part, phase, 0, slab(src, axis, opp[dim][0], a_cols), slab(via, None, None, a_cols), nxt[dim][1])
        send(part, phase, 1, slab(src, axis, opp[dim][0], b_cols), slab(via, None, None, b_cols), prv[dim][1])
        send(part, phase, 2, slab(src, axis, nxt[dim][0], b_cols), slab(fin, 0, 0, b_cols), nxt[dim][1])
        send(part, phase, 3, slab(src, axis, prv[dim][0], a_cols), slab(fin, 0, 1, a_cols), prv[dim][1])

    def each_block(shape, body):
        lead = shape[:-2]
        count = int(np.prod(lead)) if lead else 1
        if count == 1:
            body(tuple(0 for _ in lead))
            return

        def step(i, carry):
            index = []
            for size in reversed(lead):
                index.insert(0, lax.rem(i, size))
                i = lax.div(i, size)
            body(tuple(index))
            return carry

        lax.fori_loop(0, count, step, 0, unroll=min(count, 4))

    def relay(part, phase):
        dim, axis, src, via, fin, a_cols, b_cols = setting(part, phase)
        for which, col, spot, side in ((0, a_cols, nxt[dim], 0), (1, b_cols, prv[dim], 1)):
            copies[part, phase, which].wait_recv()
            span = pl.ds(*col)

            def add(index):
                at = index[:axis] + (spot[0],) + index[axis:]
                src[at + (slice(None), span)] = src[at + (slice(None), span)] + via[index + (slice(None), span)]

            each_block(via.shape, add)
            send(part, phase, 4 + which, slab(src, axis, spot[0], col), slab(fin, 0, side, col), spot[1])

    def finish(part, phase):
        dim, axis, src, via, fin, _, _ = setting(part, phase)
        for which in range(2, 6):
            copies[part, phase, which].wait_recv()

        def add(index):
            at = index[:axis] + (coords[dim],) + index[axis:]
            total = src[at] + fin[(0,) + index] + fin[(1,) + index]
            if phase < 2:
                reds[phase][part][index] = total
                return
            for is_out, first, place, size in segments(part):
                dst = gwout_ref if is_out else gwin_ref
                dst[:, first:first + size] = total[:, place:place + size].astype(dst.dtype)

        each_block(via.shape, add)
        if phase < 2:
            launch(part, phase + 1)

    early, late = (0, 1, 2), (3, 4, 5)
    for copy in (x_swap, do_swap, z_swap, d_swaps[0]):
        copy.wait_recv()
    for part in early:
        products(part)
        launch(part, 0)

    wait_all(ex_recv, 3, du_in)
    du_act = du_in[...].reshape(width, n_tok)
    for i in (1, 2):
        d_own[i * width:(i + 1) * width] = du_act * act(3 - i)
        span = pl.ds(i * width, width)
        d_swaps.append(swap(d_own.at[span], d_peer.at[span]))

    def run(step, parts, phase):
        for part in parts:
            step(part, phase)

    run(relay, early, 0)
    for copy in d_swaps[1:]:
        copy.wait_recv()
    for part in late:
        products(part)
        launch(part, 0)
    pairs(taps_grad, n_pairs // 2, n_pairs)

    def input_grad(first):
        gx_ref[:, first:first + 256] = dot(win_ref[first:first + 256], d_own[...]).T.astype(gx_ref.dtype)

    run(finish, early, 0)
    run(relay, late, 0)
    run(relay, early, 1)
    run(finish, early, 1)
    run(finish, late, 0)
    run(relay, early, 2)
    input_grad(0)
    input_grad(256)
    run(relay, late, 1)
    run(finish, early, 2)
    input_grad(512)
    run(finish, late, 1)
    input_grad(768)
    run(relay, late, 2)
    run(finish, late, 2)
    for which, ref in enumerate((u_out, dy_out, y_out, du_out)):
        wait_all(ex_send, which, ref)
    for copy in list(copies.values()) + swaps:
        copy.wait_send()


def hyena_grads(x_tok, d_out, filt_taps, skip_gain, w_in, w_out, n_dev):
    n_tok, width = x_tok.shape
    n_chans, n_chip = width // n_dev, n_dev // 2
    n_lanes, n_rows = n_tok // 2, 2 * n_dev
    n_taps = filt_taps.shape[0]
    n_wide, n_slot = 16, 8
    tables = [jnp.asarray(tab) for tab in transform_tables(n_rows, n_lanes)]
    vmem = pl.BlockSpec(memory_space=pltpu.VMEM)
    hbm = pl.BlockSpec(memory_space=pl.ANY)
    widths = [hi - lo for lo, hi in all_columns(width)]
    pairs = pltpu.VMEM((n_chip, 2, n_chans, n_tok), BF16)
    single = pltpu.VMEM((n_chip, n_chans, n_tok), BF16)
    stack = pltpu.VMEM((3 * width, n_tok), BF16)
    scratch = [pltpu.VMEM((n_dev, n_chans, n_tok), BF16)] * 6
    scratch += [pltpu.VMEM((2, width, n_lanes), F32)] * 3
    scratch += [pltpu.VMEM((n_slot, n_taps // n_wide, 128), F32), pltpu.VMEM((4, 128, n_lanes), F32),
                pltpu.VMEM((n_rows * n_chans, n_lanes), F32)]
    scratch += [pltpu.VMEM((n_chans // 2, 2 * n_rows, 2 * n_lanes), F32)] * 3
    scratch += [pltpu.VMEM(arr.shape, arr.dtype) for arr in tables + [w_in, w_out]]
    scratch += [stack, pltpu.VMEM((width, n_tok), BF16)]
    scratch += [pairs, pairs, stack, single, single, stack, pltpu.VMEM(d_out.shape, BF16)]
    scratch += [pltpu.VMEM((RING,) * 3 + (n_chans, w), F32) for w in widths]
    for n_lead in (2, 1, 0):
        lead = (RING,) * n_lead
        scratch += [pltpu.VMEM(lead + (n_chans, w), F32) for w in widths]
        scratch += [pltpu.VMEM((2,) + lead + (n_chans, w), F32) for w in widths]
        if n_lead:
            scratch += [pltpu.VMEM(lead + (n_chans, w), F32) for w in widths]
    scratch += [pltpu.SemaphoreType.DMA((n,)) for n in (len(tables) + 4, n_wide, 4, 4, 6, 6, 108, 108)]
    return pl.pallas_call(
        hyena_kernel,
        out_shape=(
            jax.ShapeDtypeStruct((n_tok, width), BF16),
            jax.ShapeDtypeStruct((n_chans, 3 * width), BF16),
            jax.ShapeDtypeStruct((n_chans, width), BF16),
            jax.ShapeDtypeStruct((n_rows * n_chans, n_lanes), F32),
            jax.ShapeDtypeStruct((n_chans, n_lanes), F32),
        ),
        in_specs=[vmem] * 2 + [hbm, pl.BlockSpec(memory_space=pltpu.SMEM)] + [hbm] * 7,
        out_specs=(vmem,) * 5,
        scratch_shapes=scratch,
        compiler_params=pltpu.CompilerParams(vmem_limit_bytes=62 * 2 ** 20, collective_id=0, has_side_effects=True),
        cost_estimate=pl.CostEstimate(flops=2 * 10 ** 10, bytes_accessed=32 * 2 ** 20, transcendentals=0),
        name="hyena_grads",
    )(x_tok, d_out, filt_taps, skip_gain, w_in, w_out, *tables)


def solution(mesh):
    ctx_size = mesh.shape["cp"]

    def local_step(x_seq, w_in, w_out, filt_taps, skip_gain, d_out):
        n_batch, n_tok, width = x_seq.shape
        n_chans = width // ctx_size
        seq_len = n_tok * ctx_size
        n_lanes = n_tok // 2
        x_tok, do_tok = x_seq[0], d_out[0]

        grad_x, grad_w_in, grad_w_out, gfilt, grad_skip = results(*hyena_grads(
            x_tok, do_tok, filt_taps, skip_gain, w_in, w_out, ctx_size))
        grad_filt = gfilt.reshape(seq_len // n_lanes, n_chans, n_lanes).transpose(0, 2, 1).reshape(seq_len, n_chans)
        return grad_x[None], grad_w_in, grad_w_out, grad_filt, grad_skip

    seq_spec = P("dp", "cp", None)
    row_spec = P(("dp", "cp"), None)
    return jax.shard_map(
        local_step,
        mesh=mesh,
        in_specs=(seq_spec, P(), P(), P(), P(), seq_spec),
        out_specs=(seq_spec, row_spec, row_spec, P("dp", "cp"), P(("dp", "cp"))),
        check_vma=False,
    )
```
